32 devices in a mesh: yy: 4 (over z), zz: 2 (over y), t: 4 (over x, core).
Axes of the slice: x: 2, y: 2, z: 4, core: 2. Of those that a mesh axis runs over, the one named last changes fastest.
Arguments:
- fat_links: float32 [4, 24, 12, 192, 20, 3, 3, 2], P(None, 't', 'zz', 'yy')
- long_links: float32 [4, 24, 12, 192, 20, 3, 3, 2], P(None, 't', 'zz', 'yy')
- source: float32 [24, 12, 192, 10, 3, 2], P('t', 'zz', 'yy')
- quark_mass: float32 [1], replicated
Outputs:
- output 1: float32 [24, 12, 192, 10, 3, 2], P('t', 'zz', 'yy')
- output 2: float32 [8], replicated
All inputs are finite; a program needn't handle non-finite values.
Results may differ from the reference program's by a relative error of at most 0.001.
Values are sent between devices in bfloat16 or wider.
A program may use at most 1 GiB of HBM per device.

```python
import jax
import jax.numpy as jnp
from jax import lax

T_DIM = 24
Z_DIM = 12
Y_DIM = 192
X_DIM = 20
ITERS = 8
XH_DIM = X_DIM // 2


def random_su3(base_key, site_shape):
    key_re, key_im = jax.random.split(base_key)
    raw_mat = lax.complex(jax.random.normal(key_re, site_shape + (2, 3), jnp.float32), jax.random.normal(key_im, site_shape + (2, 3), jnp.float32))
    row_one = raw_mat[..., 0, :]
    row_one = row_one / jnp.sqrt(jnp.sum(jnp.real(row_one * jnp.conj(row_one)), axis=-1, keepdims=True))
    row_two = raw_mat[..., 1, :]
    row_two = row_two - jnp.sum(jnp.conj(row_one) * row_two, axis=-1, keepdims=True) * row_one
    row_two = row_two / jnp.sqrt(jnp.sum(jnp.real(row_two * jnp.conj(row_two)), axis=-1, keepdims=True))
    row_three = jnp.conj(jnp.stack([row_one[..., 1] * row_two[..., 2] - row_one[..., 2] * row_two[..., 1], row_one[..., 2] * row_two[..., 0] - row_one[..., 0] * row_two[..., 2], row_one[..., 0] * row_two[..., 1] - row_one[..., 1] * row_two[..., 0]], axis=-1))
    su_mat = jnp.stack([row_one, row_two, row_three], axis=-2)
    return jnp.stack([jnp.real(su_mat), jnp.imag(su_mat)], axis=-1)


def setup_inputs(seed: int = 0) -> dict:
    base_key = jax.random.key(seed)
    key_fat, key_long, key_src, key_mass = jax.random.split(base_key, 4)
    site_shape = (T_DIM, Z_DIM, Y_DIM, X_DIM)
    fat_links = lax.map(lambda dir_key: random_su3(dir_key, site_shape), jax.random.split(key_fat, 4))
    long_links = 0.5 * lax.map(lambda dir_key: random_su3(dir_key, site_shape), jax.random.split(key_long, 4))
    source = jax.random.normal(key_src, (T_DIM, Z_DIM, Y_DIM, XH_DIM, 3, 2), jnp.float32)
    quark_mass = jax.random.uniform(key_mass, (1,), jnp.float32, 0.5, 1.0)
    return {'fat_links': fat_links, 'long_links': long_links, 'source': source, 'quark_mass': quark_mass}


def mat_vec(link_mat, colour_vec):
    link_re = link_mat[..., 0]
    link_im = link_mat[..., 1]
    vec_re = colour_vec[..., None, :, 0]
    vec_im = colour_vec[..., None, :, 1]
    return jnp.stack([jnp.sum(link_re * vec_re - link_im * vec_im, axis=-1), jnp.sum(link_re * vec_im + link_im * vec_re, axis=-1)], axis=-1)


def adj_vec(link_mat, colour_vec):
    link_re = link_mat[..., 0]
    link_im = link_mat[..., 1]
    vec_re = colour_vec[..., :, None, 0]
    vec_im = colour_vec[..., :, None, 1]
    return jnp.stack([jnp.sum(link_re * vec_re + link_im * vec_im, axis=-2), jnp.sum(link_re * vec_im - link_im * vec_re, axis=-2)], axis=-1)


def split_links(link_full, par_grid):
    n_dir, t_len, z_len, y_len, x_len = link_full.shape[:5]
    paired = link_full.reshape(n_dir, t_len, z_len, y_len, x_len // 2, 2, 3, 3, 2)
    par_links = par_grid[None, :, :, :, None, None, None, None]
    first_half = paired[:, :, :, :, :, 0]
    second_half = paired[:, :, :, :, :, 1]
    return jnp.where(par_links == 0, first_half, second_half), jnp.where(par_links == 0, second_half, first_half)


def xhat_shift(field_in, step_len, out_par, par_field):
    if out_par == 0:
        base_off = (step_len - 1) // 2
        odd_off = base_off + 1
    else:
        base_off = (step_len + 1) // 2
        odd_off = base_off - 1
    return jnp.where(par_field == 1, jnp.roll(field_in, -odd_off, axis=3), jnp.roll(field_in, -base_off, axis=3))


def apply_hop(psi_in, out_par, fat_out, fat_in, long_out, long_in, par_field):
    total = jnp.zeros_like(psi_in)
    for direction in range(3):
        chi_one = adj_vec(fat_in[direction], psi_in)
        chi_three = adj_vec(long_in[direction], psi_in)
        total = total + mat_vec(fat_out[direction], jnp.roll(psi_in, -1, axis=direction)) + mat_vec(long_out[direction], jnp.roll(psi_in, -3, axis=direction)) - jnp.roll(chi_one, 1, axis=direction) - jnp.roll(chi_three, 3, axis=direction)
    chi_one = adj_vec(fat_in[3], psi_in)
    chi_three = adj_vec(long_in[3], psi_in)
    total = total + mat_vec(fat_out[3], xhat_shift(psi_in, 1, out_par, par_field)) + mat_vec(long_out[3], xhat_shift(psi_in, 3, out_par, par_field)) - xhat_shift(chi_one, -1, out_par, par_field) - xhat_shift(chi_three, -3, out_par, par_field)
    return total


def reference(fat_links, long_links, source, quark_mass):
    par_grid = (jnp.arange(T_DIM)[:, None, None] + jnp.arange(Z_DIM)[None, :, None] + jnp.arange(Y_DIM)[None, None, :]) % 2
    par_field = par_grid[:, :, :, None, None, None]
    fat_even, fat_odd = split_links(fat_links, par_grid)
    long_even, long_odd = split_links(long_links, par_grid)
    mass_sq = quark_mass[0] * quark_mass[0]

    def normal_apply(vec_even):
        odd_part = apply_hop(vec_even, 1, fat_odd, fat_even, long_odd, long_even, par_field)
        return mass_sq * vec_even - apply_hop(odd_part, 0, fat_even, fat_odd, long_even, long_odd, par_field)

    src_norm = jnp.sum(source * source)

    def cg_step(carry, unused):
        sol_vec, res_vec, search_dir, res_norm = carry
        applied = normal_apply(search_dir)
        step_size = res_norm / jnp.sum(search_dir * applied)
        sol_vec = sol_vec + step_size * search_dir
        res_vec = res_vec - step_size * applied
        new_norm = jnp.sum(res_vec * res_vec)
        search_dir = res_vec + (new_norm / res_norm) * search_dir
        return (sol_vec, res_vec, search_dir, new_norm), new_norm / src_norm

    init_state = (jnp.zeros_like(source), source, source, src_norm)
    final_state, history = lax.scan(cg_step, init_state, None, length=ITERS)
    return final_state[0], history
```

```python
import jax
import jax.numpy as jnp
from jax import lax
from jax.experimental import pallas as pl
from jax.experimental.pallas import tpu as pltpu
from jax.sharding import PartitionSpec as P

ITERS = 8
MESH = pl.DeviceIdType.MESH
F32 = jnp.float32
TL, ZL, YL, XH = 6, 6, 48, 10
R0 = 16
ROWS, LANES, HALF, VALID = 32, 128, 64, 30
XL = 5
NSTG = 4
COMPS, LINKS = range(6), range(18)
C0 = 3
STEPS = ((0, 1), (1, 3))
SITE = VALID * 2 * 6


def vec(*shape):
    return pltpu.VMEM(shape + (LANES,), F32)


def plane():
    return vec(ZL, 6, ROWS)


def sems(*shape):
    return pltpu.SemaphoreType.DMA(shape)


def halo_t():
    return vec(2, ZL, 6, R0)


def halo_y():
    return vec(2, ZL, ROWS)


SCRATCH = dict(
    lkt=vec(24, 18, 56), lko=vec(72, 18, ROWS), stg=pltpu.VMEM((2 * NSTG, 2304, YL), F32),
    f=vec(18, 6, 64), acc=plane(), cb=vec(2, 6, ROWS), xs=vec(2, 6, YL),
    r=plane(), p=plane(), s=plane(), z=plane(), x=plane(), zs=vec(2, 6, 136), zr=vec(2, 6, 136),
    tsf=halo_t(), trf=halo_t(), tsc=halo_t(), trc=halo_t(), ysf=halo_y(), yrf=halo_y(), ysc=halo_y(), yrc=halo_y(),
    rt=vec(2, 4, 6, 8), rz=vec(2, 2, 6, 8), ry=vec(2, 4, 6, 8), gd=vec(6, 8), cf=vec(8, 8),
    stg_sem=sems(NSTG, 12), io_sem=sems(36), z_ss=sems(2, 6), z_rs=sems(2, 6), h_ss=sems(2, 3, 4), h_rs=sems(2, 3, 4),
    a_ss=sems(2, 7), a_rs=sems(2, 7),
)


def mat(acc, link, psi):
    for i in range(3):
        for j in range(3):
            a, b = link(6 * i + 2 * j), link(6 * i + 2 * j + 1)
            c, d = psi[2 * j], psi[2 * j + 1]
            acc[2 * i] = acc[2 * i] + (a * c - b * d)
            acc[2 * i + 1] = acc[2 * i + 1] + (a * d + b * c)


def adj(acc, link, psi):
    for j in range(3):
        for i in range(3):
            a, b = link(6 * j + 2 * i), link(6 * j + 2 * i + 1)
            c, d = psi[2 * j], psi[2 * j + 1]
            acc[2 * i] = acc[2 * i] - (a * c + b * d)
            acc[2 * i + 1] = acc[2 * i + 1] + (b * c - a * d)


def rot(v, n):
    n %= LANES
    return pltpu.roll(v, n, 1) if n else v


def kernel(fat, lng, src, mass, out, res, *scratch):
    k = type('Refs', (), {})()
    for name, ref in zip(SCRATCH, scratch):
        setattr(k, name, ref)
    iy, iz, it = lax.axis_index('yy'), lax.axis_index('zz'), lax.axis_index('t')

    def at_t(d):
        return (iy, iz, lax.rem(it + d, 4))

    def at_z():
        return (iy, 1 - iz, it)

    def at_y(d):
        return (lax.rem(iy + d, 4), iz, it)

    def remote(src_ref, dst_ref, send, recv, dev):
        return pltpu.make_async_remote_copy(src_ref=src_ref, dst_ref=dst_ref, send_sem=send, recv_sem=recv, device_id=dev, device_id_type=MESH)

    others = range(1, 4)
    barrier = pltpu.get_barrier_semaphore()
    for dev in [at_t(d) for d in others] + [at_z()] + [at_y(d) for d in others]:
        pl.semaphore_signal(barrier, inc=1, device_id=dev, device_id_type=MESH)
    pl.semaphore_wait(barrier, 7)

    lane8, row8 = (lax.broadcasted_iota(jnp.int32, (8, LANES), d) for d in (1, 0))
    ylane8 = lane8 % HALF
    lane, row = (lax.broadcasted_iota(jnp.int32, (ROWS, LANES), d) for d in (1, 0))
    ylane, x5 = lane % HALF, lax.rem(row, XL)
    parity = row // XL + lane
    real = row < VALID
    good = real & (ylane < YL)
    seg0 = lane < HALF
    zero8 = jnp.zeros((8, LANES), F32)
    zeros = jnp.zeros((ROWS, LANES), F32)

    def lt(n, o, zi):
        return (n * 2 + o) * ZL + zi

    def lo(di, n, o, zi):
        return (((di - 1) * 2 + n) * 2 + o) * ZL + zi

    def field(i, j, c, off=0):
        return k.f[9 * i + j, c, pl.ds(R0 + off, ROWS), :]

    def psi_of(i, j, off=0):
        return [field(i, j, c, off) for c in COMPS]

    def each_src(act):
        for q in range(36):
            zi, ti = q // TL, q % TL
            act(q, pl.ds(zi * SITE + ti * 60, 60), ti, pl.ds(zi * 60, 60))

    def src_copy(q, here, ti, there):
        return pltpu.make_async_copy(src.at[ti, there], k.stg.at[0, here], k.io_sem.at[q])

    def out_copy(q, here, ti, there):
        return pltpu.make_async_copy(k.stg.at[0, here], out.at[ti, there], k.io_sem.at[q])

    def stg_copies(g):
        slot, di, zi = lax.rem(g, NSTG), g // ZL, lax.rem(g, ZL)
        return [pltpu.make_async_copy(ref.at[di, t, zi], k.stg.at[2 * slot + n, pl.ds(SITE * t, SITE)], k.stg_sem.at[slot, TL * n + t])
                for n, ref in enumerate((fat, lng)) for t in range(TL)]

    z16 = jnp.zeros((ROWS, R0), F32)

    def both(half):
        return jnp.where(real, jnp.concatenate([half[0], z16, half[1], z16], axis=1), 0.0)

    each_src(lambda *a: src_copy(*a).start())
    k.f[...] = jnp.zeros_like(k.f)
    for ref in (k.p, k.s, k.z, k.x):
        ref[...] = jnp.zeros_like(ref)
    k.lkt[:, :, 0:R0, :] = jnp.zeros((24, 18, R0, LANES), F32)
    k.lkt[:, :, R0 + ROWS:, :] = jnp.zeros((24, 18, 8, LANES), F32)
    each_src(lambda *a: src_copy(*a).wait())

    def src_plane(zi, _):
        for c in COMPS:
            v = both([k.stg[0, pl.ds(zi * SITE + 6 * s + c, ROWS, 12), :] for s in range(2)])
            k.f[zi, c, pl.ds(R0, ROWS), :] = v
            k.r[zi, c] = v
        return 0

    lax.fori_loop(0, ZL, src_plane, 0)

    def convert(g, ref, base, lead):
        slot, zi = lax.rem(g, NSTG), lax.rem(g, ZL)
        even = (((parity + zi) & 1) == 0)[:, 0:YL]

        def some_comps(q, _):
            for n in range(2):
                for u in range(3):
                    c = 3 * q + u
                    v = [[k.stg[2 * slot + n, pl.ds(c + (2 * s + h) * 18, ROWS, 72), :] for h in range(2)] for s in range(2)]
                    for o in range(2):
                        ref[lead(n, o, zi), c, pl.ds(base, ROWS), :] = both([jnp.where(even, v[s][o], v[s][1 - o]) for s in range(2)])
            return 0
        lax.fori_loop(0, 6, some_comps, 0)

    def load_step(g, ref, base, lead):
        for cp in stg_copies(g):
            cp.wait()
        convert(g, ref, base, lead)

        @pl.when(g + NSTG < 24)
        def _():
            for cp in stg_copies(g + NSTG):
                cp.start()

    for g in range(NSTG):
        for cp in stg_copies(jnp.int32(g)):
            cp.start()

    def load_t(g, _):
        load_step(g, k.lkt, R0, lt)
        return 0

    def load_o(g, _):
        load_step(g, k.lko, 0, lambda n, o, zi: lo(g // ZL, n, o, zi))
        return 0

    lax.fori_loop(0, ZL, load_t, 0)
    lax.fori_loop(ZL, 24, load_o, 0)

    def z_copy(i, m):
        return remote(k.zs.at[i, m], k.zr.at[i, m], k.z_ss.at[i, m], k.z_rs.at[i, m], at_z())

    def h_copies(i, t):
        pairs = ((k.tsf, k.trf, at_t(3)), (k.tsc, k.trc, at_t(1)), (k.ysf, k.yrf, at_y(3)), (k.ysc, k.yrc, at_y(1)))
        two = pl.ds(2 * t, 2)
        return [remote(a.at[i, two], b.at[i, two], k.h_ss.at[i, t, n], k.h_rs.at[i, t, n], dev) for n, (a, b, dev) in enumerate(pairs)]

    def plane_of(t, n2):
        first = jnp.where(t == 0, 1, jnp.where(t == 1, 0, 3))
        return first + n2 * jnp.where(t == 0, 3, 2)

    gap = ylane8 >= YL

    def rows_of(u, part, off=0):
        return pl.ds(off + 15 * (u % 2) + part, 8)

    def wire(host, part):
        return pl.ds(15 * host + part, 8)

    def pack(load, i, m):
        for u in range(3):
            for part in (0, 7):
                guest = load(9 + u, part)
                for q in range(3):
                    k.zs[i, m, wire(3 * q + u, part), :] = jnp.where(gap, rot(guest, YL - R0 * q), load(3 * q + u, part))

    def unpack(i, m, store):
        for u in range(3):
            for part in (0, 7):
                guest = zero8
                for q in range(3):
                    h = k.zr[i, m, wire(3 * q + u, part), :]
                    store(3 * q + u, part, jnp.where(gap, 0.0, h))
                    guest = jnp.where(ylane8 // R0 == q, rot(h, R0 * q - YL), guest)
                store(9 + u, part, guest)

    def start(i, *ms):
        for m in ms:
            z_copy(i, m).start()

    def arrive(i, *ms):
        for m in ms:
            z_copy(i, m).wait_recv()

    def pack_psi(i, m):
        pack(lambda u, part: k.f[9 * i + m, u // 2, rows_of(u, part, R0), :], i, m)

    def pack_c(i, m, b, *terms):
        acc = [zeros] * 6
        for n, j in terms:
            adj(acc, lambda c: k.lko[lo(1, n, i, j), c], psi_of(i, j))
        for c in COMPS:
            k.cb[b, c] = acc[c]
        pack(lambda u, part: k.cb[b, u // 2, rows_of(u, part), :], i, C0 + m)

    def unpack_psi(i, m):
        def store(u, part, v):
            k.f[9 * i + 6 + m, u // 2, rows_of(u, part, R0), :] = v
        unpack(i, m, store)

    def unpack_c(i, m):
        def store(u, part, v):
            w = jnp.where(row8 == 0, 0.0, v) if part else v
            k.acc[m, u // 2, rows_of(u, part), :] = k.acc[m, u // 2, rows_of(u, part), :] + w
        unpack(i, C0 + m, store)

    def send(i, t):
        @pl.when(t == 0)
        def _():
            pack_psi(i, 1)
            pack_c(i, 1, 0, (1, 4))
            start(i, 1, C0 + 1)

        @pl.when(t == 1)
        def _():
            pack_psi(i, 0)
            pack_psi(i, 2)
            start(i, 0, 2)

        @pl.when(t == 2)
        def _():
            pack_c(i, 0, 0, (0, 5), (1, 3))
            pack_c(i, 2, 1, (1, 5))
            start(i, C0, C0 + 2)

    def receive(i, t):
        @pl.when(t == 0)
        def _():
            arrive(i, 1, C0 + 1)
            unpack_psi(i, 1)
            unpack_c(i, 1)

        @pl.when(t == 1)
        def _():
            arrive(i, C0, C0 + 2)
            unpack_c(i, 0)
            unpack_c(i, 2)

        @pl.when(t == 2)
        def _():
            arrive(i, 0, 2)
            unpack_psi(i, 0)
            unpack_psi(i, 2)

    def post(i, t):
        o = 1 - i

        def one_plane(n2, _):
            j = plane_of(t, n2)
            slot = 2 * t + n2
            psi = psi_of(i, j)
            back = [zeros] * 6
            for n, off in STEPS:
                chi = [zeros] * 6
                adj(chi, lambda c: k.lko[lo(2, n, i, j), c], psi)
                back = [back[c] + rot(chi[c], off) for c in COMPS]
            fwd, bwd = psi[0], rot(back[0], -YL)
            for c in COMPS[1:]:
                here = ylane // 4 == c
                fwd = jnp.where(here, rot(psi[c], 4 * c), fwd)
                bwd = jnp.where(here, rot(back[c], 4 * c - YL), bwd)
            k.ysf[i, slot] = fwd
            k.ysc[i, slot] = bwd
            e = ((parity + (j + o)) & 1) == 1
            for n, _ in STEPS:
                chi = [zeros] * 6
                adj(chi, lambda c: k.lko[lo(3, n, i, j), c], psi)
                for c in COMPS:
                    k.xs[n, c, pl.ds(8, ROWS), :] = chi[c]
                    far = jnp.where(x5 > 0, k.xs[n, c, pl.ds(7, ROWS), :], k.xs[n, c, pl.ds(12, ROWS), :])
                    near = rot(jnp.where(seg0, chi[c], far), HALF)
                    back[c] = back[c] + (jnp.where(e, near, far) if n else jnp.where(e, chi[c], near))
            acc = back
            far = [jnp.where(x5 < 4, field(i, j, c, 1), field(i, j, c, -4)) for c in COMPS]
            near = [rot(jnp.where(seg0, far[c], psi[c]), HALF) for c in COMPS]
            mat(acc, lambda c: k.lko[lo(3, 0, o, j), c], [jnp.where(e, near[c], psi[c]) for c in COMPS])
            mat(acc, lambda c: k.lko[lo(3, 1, o, j), c], [jnp.where(e, far[c], near[c]) for c in COMPS])
            for n, off in STEPS:
                off *= XL
                adj(acc, lambda c: k.lkt[lt(n, i, j), c, pl.ds(R0 - off, ROWS), :], psi_of(i, j, -off))
            for c in COMPS:
                k.acc[j, c] = acc[c]
            for h in range(2):
                acc = [zero8] * 6
                for n, first in ((0, R0 + 25), (1, R0 + 15 + 8 * h)):
                    if n or not h:
                        adj(acc, lambda c: k.lkt[lt(n, i, j), c, pl.ds(first, 8), :], [k.f[9 * i + j, c, pl.ds(first, 8), :] for c in COMPS])
                for c in COMPS:
                    k.tsc[i, slot, c, pl.ds(8 * h, 8), :] = acc[c]
                    k.tsf[i, slot, c, pl.ds(8 * h, 8), :] = k.f[9 * i + j, c, pl.ds(R0 + 8 * h, 8), :]
            return 0

        lax.fori_loop(0, 2, one_plane, 0)
        for cp in h_copies(i, t):
            cp.start()

    m2 = mass[0] * mass[0]
    inside = pl.ds(R0, ROWS)

    def store_odd(j, acc):
        for c in COMPS:
            k.f[9 + j, c, inside, :] = acc[c]

    def update_even(j, acc):
        cw, aw, ax, beta = (jnp.broadcast_to(k.cf[v, 0:1], (ROWS, LANES)) for v in range(4))
        gg, dd = zeros, zeros
        for c in COMPS:
            w = jnp.where(real, k.f[j, c, inside, :], 0.0)
            n = m2 * w - acc[c]
            zv = n + beta * k.z[j, c]
            sv = w + beta * k.s[j, c]
            r = k.r[j, c]
            pv = r + beta * k.p[j, c]
            k.x[j, c] = k.x[j, c] + ax * pv
            r = r - ax * sv
            w = cw * w - aw * zv
            k.z[j, c], k.s[j, c], k.p[j, c], k.r[j, c], k.f[j, c, inside, :] = zv, sv, pv, r, w
            gg = gg + r * r
            dd = dd + w * r
        for v, t in enumerate((gg, dd)):
            k.gd[v] = k.gd[v] + sum(t[8 * b:8 * b + 8] for b in range(4))

    def finish(i, t, update):
        o = 1 - i
        for cp in h_copies(i, t):
            cp.wait_recv()

        def one_plane(n2, _):
            j = plane_of(t, n2)
            slot = 2 * t + n2
            for c in COMPS:
                k.f[9 * i + j, c, pl.ds(R0 + VALID, R0), :] = k.trf[i, slot, c]
            yf, yc = k.yrf[i, slot], k.yrc[i, slot]
            top = (ylane >= YL) & (ylane < YL + 3)
            psi = [jnp.where(top, rot(yf, YL - 4 * c), field(i, j, c)) for c in COMPS]
            low = [jnp.where(ylane < 3, rot(yc, -4 * c), 0.0) for c in COMPS]
            acc = [k.acc[j, c] + low[c] for c in COMPS]
            for n, off in STEPS:
                mat(acc, lambda c: k.lkt[lt(n, o, j), c, inside, :], psi_of(i, j, XL * off))
            for n, off in STEPS:
                mat(acc, lambda c: k.lko[lo(1, n, o, j), c], psi_of(i, j + off))
                jb, on = jnp.maximum(j - off, 0), jnp.where(j >= off, 1.0, 0.0)
                adj(acc, lambda c: k.lko[lo(1, n, i, jb), c], [on * v for v in psi_of(i, jb)])
            for n, off in STEPS:
                mat(acc, lambda c: k.lko[lo(2, n, o, j), c], [rot(psi[c], -off) for c in COMPS])
            extra = [jnp.concatenate([k.trc[i, slot, c], zeros[:R0]], axis=0) for c in COMPS]
            update(j, [jnp.where(good, acc[c] + extra[c], 0.0) for c in COMPS])
            return 0

        lax.fori_loop(0, 2, one_plane, 0)

    def a_copies(stage, b, n):
        buf, me, first = ((k.rt, it, -1), (k.rz, iz, 3), (k.ry, iy, 3))[stage]
        to = ([at_t(d) for d in others], [at_z()], [at_y(d) for d in others])[stage]
        mine = buf.at[b, me, pl.ds(0, n)]
        first = (0, 3, 4)[stage]
        return [remote(mine, mine, k.a_ss.at[b, first + d], k.a_rs.at[b, first + d], dev) for d, dev in enumerate(to)]

    def sum_start(b, n):
        for v in range(n):
            k.rt[b, it, v] = k.gd[v]
        for cp in a_copies(0, b, n):
            cp.start()

    def sum_next(stage, b, n):
        for cp in a_copies(stage, b, n):
            cp.wait()
        frm = (k.rt, k.rz, k.ry)[stage]
        for v in range(n):
            tot = frm[b, 0, v] + frm[b, 1, v]
            if stage != 1:
                tot = tot + frm[b, 2, v] + frm[b, 3, v]
            if stage == 0:
                k.rz[b, iz, v] = tot
            elif stage == 1:
                k.ry[b, iy, v] = tot
            else:
                k.gd[v] = jnp.broadcast_to(jnp.sum(jnp.sum(tot, axis=0, keepdims=True), axis=1, keepdims=True), (8, LANES))
        if stage < 2:
            for cp in a_copies(stage + 1, b, n):
                cp.start()

    CW, AW, AX, BETA, GAMMA, ALPHA, FIRST = range(7)
    one = jnp.ones((8, LANES), F32)
    for v, t in ((CW, zero8), (AW, -one), (AX, zero8), (BETA, zero8), (GAMMA, one), (ALPHA, one)):
        k.cf[v] = t

    def scalars(step):
        gamma, delta = k.gd[0], k.gd[1]

        @pl.when(step == 1)
        def _():
            k.cf[ALPHA] = gamma / delta
            k.cf[FIRST] = gamma

        @pl.when(step > 1)
        def _():
            beta = gamma / k.cf[GAMMA]
            k.cf[BETA] = beta
            k.cf[ALPHA] = gamma / (delta - beta * gamma / k.cf[ALPHA])
            res[step - 2] = (gamma / k.cf[FIRST])[0, 0]
        k.cf[CW], k.cf[AW], k.cf[AX], k.cf[GAMMA] = one, k.cf[ALPHA], k.cf[ALPHA], gamma

    def phase(u, _):
        n, ph = u // 3 - 1, lax.rem(u, 3)
        i = lax.rem(n + 2, 2)
        step = n // 2
        b = lax.rem(jnp.maximum(step, 0), 2)
        t = jnp.where(ph == 0, 0, jnp.where((ph == 1) == (i == 0), 1, 2))
        live = n >= 0
        summing = (step > 0) & live

        @pl.when(summing & (i == 0) & (ph == 1))
        def _():
            sum_next(0, b, 2)

        @pl.when(summing & (i == 0) & (ph == 2))
        def _():
            sum_next(1, b, 2)

        @pl.when(live & (i == 1) & (ph == 0))
        def _():
            @pl.when(step > 0)
            def _():
                sum_next(2, b, 2)
                scalars(step)
            k.gd[0], k.gd[1] = zero8, zero8

        @pl.when(live)
        def _():
            receive(i, t)

            @pl.when(i == 0)
            def _():
                finish(0, t, store_odd)

            @pl.when(i == 1)
            def _():
                finish(1, t, update_even)

        @pl.when(n < 2 * ITERS - 1)
        def _():
            send(1 - i, t)
            post(1 - i, t)

        @pl.when(live & (ph == 2))
        def _():
            for m in range(6):
                z_copy(i, m).wait_send()
            for g in range(3):
                for cp in h_copies(i, g):
                    cp.wait_send()

            @pl.when((i == 1) & (step < ITERS - 1))
            def _():
                sum_start(1 - b, 2)
        return 0

    lax.fori_loop(0, 3 * (2 * ITERS + 1), phase, 0)

    def dots(j, carry):
        for c in COMPS:
            w, r, s = k.f[j, c, inside, :], k.r[j, c], k.s[j, c]
            carry = tuple(t + u * v for t, (u, v) in zip(carry, ((r, r), (w, r), (w, w), (r, s), (w, s), (s, s))))
        return carry

    for v, t in enumerate(lax.fori_loop(0, ZL, dots, (zeros,) * 6)):
        k.gd[v] = sum(t[8 * b:8 * b + 8] for b in range(4))
    sum_start(0, 6)
    for stage in range(3):
        sum_next(stage, 0, 6)
    rr, wr, ww, rs, ws, ss = (k.gd[v] for v in range(6))
    beta = rr / k.cf[GAMMA]
    alpha = rr / (wr - beta * rr / k.cf[ALPHA])
    last = rr - 2.0 * alpha * (wr + beta * rs) + alpha * alpha * (ww + 2.0 * beta * ws + beta * beta * ss)
    for v, t in ((ITERS - 2, rr), (ITERS - 1, last)):
        res[v] = (t / k.cf[FIRST])[0, 0]
    alpha, beta = (jnp.broadcast_to(v[0:1], (ROWS, LANES)) for v in (alpha, beta))

    def out_plane(j, _):
        for c in COMPS:
            v = k.x[j, c] + alpha * (k.r[j, c] + beta * k.p[j, c])
            for s in range(2):
                k.stg[0, pl.ds(j * SITE + 6 * s + c, VALID, 12), :] = rot(v, HALF * s)[0:VALID, 0:YL]
        return 0

    lax.fori_loop(0, ZL, out_plane, 0)
    each_src(lambda *a: out_copy(*a).start())
    each_src(lambda *a: out_copy(*a).wait())


def solution(mesh):
    link_spec = P(None, 't', 'zz', 'yy', None, None, None, None)
    field_spec = P('t', 'zz', 'yy', None, None, None)

    def local_solve(fat_links, long_links, source, quark_mass):
        fat, lng = (jnp.transpose(v, (0, 1, 2, 4, 5, 6, 7, 3)).reshape(4, TL, ZL, SITE, YL) for v in (fat_links, long_links))
        src = jnp.transpose(source, (0, 1, 3, 4, 5, 2)).reshape(TL, SITE, YL)
        anywhere, scalar = (pl.BlockSpec(memory_space=space) for space in (pl.ANY, pltpu.SMEM))
        sol, res = pl.pallas_call(
            kernel,
            out_shape=tuple(jax.ShapeDtypeStruct(shape, F32) for shape in ((TL, SITE, YL), (8,))),
            in_specs=[anywhere] * 3 + [scalar],
            out_specs=(anywhere, scalar),
            scratch_shapes=list(SCRATCH.values()),
            compiler_params=pltpu.CompilerParams(collective_id=0, has_side_effects=True, vmem_limit_bytes=67043328),
            name='cg',
        )(fat, lng, src, quark_mass)
        return jnp.transpose(sol.reshape(TL, ZL, XH, 3, 2, YL), (0, 1, 5, 2, 3, 4)), res

    return jax.shard_map(local_solve, mesh=mesh, in_specs=(link_spec, link_spec, field_spec, P(None)), out_specs=(field_spec, P()), check_vma=False)
```

```python
import jax
import jax.numpy as jnp
from jax import lax
from jax.experimental import pallas as pl
from jax.experimental.pallas import tpu as pltpu
from jax.sharding import PartitionSpec as P

ITERS = 8
MESH = pl.DeviceIdType.MESH
F32 = jnp.float32
TL, ZL, YL, XH = 6, 6, 48, 10
R0 = 16
ROWS, LANES, HALF, VALID = 32, 128, 64, 30
XL = 5
NSTG = 4
COMPS, LINKS = range(6), range(18)
C0 = 3
STEPS = ((0, 1), (1, 3))
SITE = VALID * 2 * 6
LOADS = 4 * ZL
BLK = 16
BLOCKS = range(0, ROWS, BLK)


def vec(*shape):
    return pltpu.VMEM(shape + (LANES,), F32)


def plane():
    return vec(ZL, 6, ROWS)


def sems(*shape):
    return pltpu.SemaphoreType.DMA(shape)


def halo_t():
    return vec(2, ZL, 6, R0)


def halo_y():
    return vec(2, ZL, BLK)


SCRATCH = dict(
    lkt=vec(24, 18, 56), lko=vec(72, 18, ROWS), stg=pltpu.VMEM((2 * NSTG, 2304, YL), F32), sst=pltpu.VMEM((2304, YL), F32),
    f=vec(18, 6, 64), acc=plane(), cb=vec(2, 6, ROWS), xs=vec(2, 6, YL),
    r=plane(), p=plane(), s=plane(), z=plane(), x=plane(), zs=vec(2, 6, 136), zr=vec(2, 6, 136),
    tsf=halo_t(), trf=halo_t(), tsc=halo_t(), trc=halo_t(), ysf=halo_y(), yrf=halo_y(), ysc=halo_y(), yrc=halo_y(),
    ra=vec(2, 8, 8), rb=vec(2, 4, 8), gd=vec(6, 8), cf=vec(8, 8),
    stg_sem=sems(NSTG, 12), io_sem=sems(36), z_ss=sems(2, 6), z_rs=sems(2, 6), h_ss=sems(2, 3, 4), h_rs=sems(2, 3, 4),
    a_ss=sems(2, 10), a_rs=sems(2, 10),
)


def mat(acc, link, psi):
    for i in range(3):
        for j in range(3):
            a, b = link(6 * i + 2 * j), link(6 * i + 2 * j + 1)
            c, d = psi[2 * j], psi[2 * j + 1]
            acc[2 * i] = acc[2 * i] + (a * c - b * d)
            acc[2 * i + 1] = acc[2 * i + 1] + (a * d + b * c)


def adj(acc, link, psi):
    for j in range(3):
        for i in range(3):
            a, b = link(6 * j + 2 * i), link(6 * j + 2 * i + 1)
            c, d = psi[2 * j], psi[2 * j + 1]
            acc[2 * i] = acc[2 * i] - (a * c + b * d)
            acc[2 * i + 1] = acc[2 * i + 1] + (b * c - a * d)


def rot(v, n):
    n %= LANES
    return pltpu.roll(v, n, 1) if n else v


def kernel(fat, lng, src, mass, out, res, *scratch):
    k = type('Refs', (), {})()
    for name, ref in zip(SCRATCH, scratch):
        setattr(k, name, ref)
    iy, iz, it = lax.axis_index('yy'), lax.axis_index('zz'), lax.axis_index('t')

    def at_t(d):
        return (iy, iz, lax.rem(it + d, 4))

    def at_z(d=0):
        return (iy, 1 - iz, lax.rem(it + d, 4))

    def at_y(d):
        return (lax.rem(iy + d, 4), iz, it)

    def remote(src_ref, dst_ref, send, recv, dev):
        return pltpu.make_async_remote_copy(src_ref=src_ref, dst_ref=dst_ref, send_sem=send, recv_sem=recv, device_id=dev, device_id_type=MESH)

    others = range(1, 4)
    near = [at_t(d) for d in others] + [at_z(d) for d in range(4)]
    ring = [at_y(d) for d in others]

    def plane_of(t, n2):
        first = jnp.where(t == 0, 1, jnp.where(t == 1, 0, 3))
        return first + n2 * jnp.where(t == 0, 3, 2)

    def what(g):
        q = jnp.maximum(g - ZL, 0)
        d = lax.rem(q, 3)
        p = q // 3
        early = g < ZL
        return jnp.where(early, 1, jnp.where(d == 0, 0, d + 1)), jnp.where(early, g, plane_of(p // 2, lax.rem(p, 2)))

    def stg_copies(g):
        slot = lax.rem(g, NSTG)
        di, zi = what(g)
        return [pltpu.make_async_copy(ref.at[di, t, zi], k.stg.at[2 * slot + n, pl.ds(SITE * t, SITE)], k.stg_sem.at[slot, TL * n + t])
                for n, ref in enumerate((fat, lng)) for t in range(TL)]

    def each_src(act):
        for q in range(TL * ZL):
            zi, ti = q // TL, q % TL
            act(q, pl.ds(zi * SITE + ti * 60, 60), ti, pl.ds(zi * 60, 60))

    def src_copy(q, here, ti, there):
        return pltpu.make_async_copy(src.at[ti, there], k.sst.at[here], k.io_sem.at[q])

    def out_copy(q, here, ti, there):
        return pltpu.make_async_copy(k.sst.at[here], out.at[ti, there], k.io_sem.at[q])

    barrier = pltpu.get_barrier_semaphore()
    for dev in near + ring:
        pl.semaphore_signal(barrier, inc=1, device_id=dev, device_id_type=MESH)
    each_src(lambda *a: src_copy(*a).start())
    for g in range(NSTG):
        for cp in stg_copies(jnp.int32(g)):
            cp.start()

    lane8, row8 = (lax.broadcasted_iota(jnp.int32, (8, LANES), d) for d in (1, 0))
    ylane8 = lane8 % HALF
    lane, row = (lax.broadcasted_iota(jnp.int32, (ROWS, LANES), d) for d in (1, 0))
    lane_b, row_b = lane[:BLK], row[:BLK]
    ylane = lane_b % HALF
    seg0 = lane_b < HALF
    zero8 = jnp.zeros((8, LANES), F32)
    zeros = jnp.zeros((BLK, LANES), F32)

    def lt(n, o, zi):
        return (n * 2 + o) * ZL + zi

    def lo(di, n, o, zi):
        return (((di - 1) * 2 + n) * 2 + o) * ZL + zi

    def at(h, off=0):
        return pl.ds(off + h, BLK)

    def psi_of(i, j, h, off=0):
        return [k.f[9 * i + j, c, at(h, R0 + off), :] for c in COMPS]

    k.f[...] = jnp.zeros_like(k.f)
    for ref in (k.p, k.s, k.z, k.x):
        ref[...] = jnp.zeros_like(ref)
    k.lkt[:, :, 0:R0, :] = jnp.zeros((24, 18, R0, LANES), F32)
    k.lkt[:, :, R0 + ROWS:, :] = jnp.zeros((24, 18, 8, LANES), F32)

    z16 = jnp.zeros((ROWS, R0), F32)

    def both(half):
        return jnp.where(row < VALID, jnp.concatenate([half[0], z16, half[1], z16], axis=1), 0.0)

    def src_plane(zi, _):
        for c in COMPS:
            v = both([k.sst[pl.ds(zi * SITE + 6 * s + c, ROWS, 12), :] for s in range(2)])
            k.f[zi, c, pl.ds(R0, ROWS), :] = v
            k.r[zi, c] = v
        return 0

    each_src(lambda *a: src_copy(*a).wait())
    lax.fori_loop(0, ZL, src_plane, 0)
    pl.semaphore_wait(barrier, len(near + ring))

    def convert(g, zi, ref, base, lead):
        slot = lax.rem(g, NSTG)
        even = (((row // XL + lane + zi) & 1) == 0)[:, 0:YL]

        def some_comps(q, _):
            for n in range(2):
                for u in range(3):
                    c = 3 * q + u
                    v = [[k.stg[2 * slot + n, pl.ds(c + (2 * s + h) * 18, ROWS, 72), :] for h in range(2)] for s in range(2)]
                    for o in range(2):
                        ref[lead(n, o, zi), c, pl.ds(base, ROWS), :] = both([jnp.where(even, v[s][o], v[s][1 - o]) for s in range(2)])
            return 0
        lax.fori_loop(0, 6, some_comps, 0)

    def load_step(g, _):
        di, zi = what(g)
        for cp in stg_copies(g):
            cp.wait()

        @pl.when(di == 0)
        def _():
            convert(g, zi, k.lkt, R0, lt)

        @pl.when(di > 0)
        def _():
            convert(g, zi, k.lko, 0, lambda n, o, zi: lo(di, n, o, zi))

        @pl.when(g + NSTG < LOADS)
        def _():
            for cp in stg_copies(g + NSTG):
                cp.start()
        return 0

    def z_copy(i, m):
        return remote(k.zs.at[i, m], k.zr.at[i, m], k.z_ss.at[i, m], k.z_rs.at[i, m], at_z())

    def h_copies(i, t):
        pairs = ((k.tsf, k.trf, at_t(3)), (k.tsc, k.trc, at_t(1)), (k.ysf, k.yrf, at_y(3)), (k.ysc, k.yrc, at_y(1)))
        two = pl.ds(2 * t, 2)
        return [remote(a.at[i, two], b.at[i, two], k.h_ss.at[i, t, n], k.h_rs.at[i, t, n], dev) for n, (a, b, dev) in enumerate(pairs)]

    gap = ylane8 >= YL

    def rows_of(u, part, off=0):
        return pl.ds(off + 15 * (u % 2) + part, 8)

    def wire(host, part):
        return pl.ds(15 * host + part, 8)

    def pack(load, i, m):
        for u in range(3):
            for part in (0, 7):
                guest = load(9 + u, part)
                for q in range(3):
                    k.zs[i, m, wire(3 * q + u, part), :] = jnp.where(gap, rot(guest, YL - R0 * q), load(3 * q + u, part))

    def unpack(i, m, store):
        for u in range(3):
            for part in (0, 7):
                guest = zero8
                for q in range(3):
                    h = k.zr[i, m, wire(3 * q + u, part), :]
                    store(3 * q + u, part, jnp.where(gap, 0.0, h))
                    guest = jnp.where(ylane8 // R0 == q, rot(h, R0 * q - YL), guest)
                store(9 + u, part, guest)

    def start(i, *ms):
        for m in ms:
            z_copy(i, m).start()

    def arrive(i, *ms):
        for m in ms:
            z_copy(i, m).wait_recv()

    def pack_psi(i, m):
        pack(lambda u, part: k.f[9 * i + m, u // 2, rows_of(u, part, R0), :], i, m)

    def pack_c(i, m, b, *terms):
        for h in BLOCKS:
            acc = [zeros] * 6
            for n, j in terms:
                adj(acc, lambda c: k.lko[lo(1, n, i, j), c, at(h), :], psi_of(i, j, h))
            for c in COMPS:
                k.cb[b, c, at(h), :] = acc[c]
        pack(lambda u, part: k.cb[b, u // 2, rows_of(u, part), :], i, C0 + m)

    def unpack_psi(i, m):
        def store(u, part, v):
            k.f[9 * i + 6 + m, u // 2, rows_of(u, part, R0), :] = v
        unpack(i, m, store)

    def unpack_c(i, m):
        def store(u, part, v):
            w = jnp.where(row8 == 0, 0.0, v) if part else v
            k.acc[m, u // 2, rows_of(u, part), :] = k.acc[m, u // 2, rows_of(u, part), :] + w
        unpack(i, C0 + m, store)

    def send(i, t):
        @pl.when(t == 0)
        def _():
            pack_psi(i, 1)
            pack_c(i, 1, 0, (1, 4))
            start(i, 1, C0 + 1)

        @pl.when(t == 1)
        def _():
            pack_psi(i, 0)
            pack_psi(i, 2)
            start(i, 0, 2)

        @pl.when(t == 2)
        def _():
            pack_c(i, 0, 0, (0, 5), (1, 3))
            pack_c(i, 2, 1, (1, 5))
            start(i, C0, C0 + 2)

    def receive(i, t):
        @pl.when(t == 0)
        def _():
            arrive(i, 1, C0 + 1)
            unpack_psi(i, 1)
            unpack_c(i, 1)

        @pl.when(t == 1)
        def _():
            arrive(i, C0, C0 + 2)
            unpack_c(i, 0)
            unpack_c(i, 2)

        @pl.when(t == 2)
        def _():
            arrive(i, 0, 2)
            unpack_psi(i, 0)
            unpack_psi(i, 2)

    def tell(i, t):
        def one_plane(n2, _):
            j = plane_of(t, n2)
            slot = 2 * t + n2
            fwd, bwd = zeros, zeros
            for h in BLOCKS:
                psi = psi_of(i, j, h)
                back = [zeros] * 6
                for n, off in STEPS:
                    chi = [zeros] * 6
                    adj(chi, lambda c: k.lko[lo(2, n, i, j), c, at(h), :], psi)
                    back = [back[c] + rot(chi[c], off) for c in COMPS]
                for c in COMPS:
                    k.acc[j, c, at(h), :] = back[c]
                    to = 4 * c + 24 * (h // BLK)
                    here = ylane // 4 == to // 4
                    fwd = jnp.where(here, rot(psi[c], to), fwd)
                    bwd = jnp.where(here, rot(back[c], to - YL), bwd)
            k.ysf[i, slot] = fwd
            k.ysc[i, slot] = bwd
            for h in range(2):
                acc = [zero8] * 6
                for n, first in ((0, R0 + 25), (1, R0 + 15 + 8 * h)):
                    if n or not h:
                        adj(acc, lambda c: k.lkt[lt(n, i, j), c, pl.ds(first, 8), :], [k.f[9 * i + j, c, pl.ds(first, 8), :] for c in COMPS])
                for c in COMPS:
                    k.tsc[i, slot, c, pl.ds(8 * h, 8), :] = acc[c]
                    k.tsf[i, slot, c, pl.ds(8 * h, 8), :] = k.f[9 * i + j, c, pl.ds(R0 + 8 * h, 8), :]
            return 0

        lax.fori_loop(0, 2, one_plane, 0)
        for cp in h_copies(i, t):
            cp.start()

    def post(i, t):
        o = 1 - i

        def one_plane(n2, _):
            j = plane_of(t, n2)
            for h in BLOCKS:
                psi = psi_of(i, j, h)
                for n, _ in STEPS:
                    chi = [zeros] * 6
                    adj(chi, lambda c: k.lko[lo(3, n, i, j), c, at(h), :], psi)
                    for c in COMPS:
                        k.xs[n, c, at(h, 8), :] = chi[c]
            for h in BLOCKS:
                x5 = lax.rem(row_b + h, XL)
                e = (((row_b + h) // XL + lane_b + (j + o)) & 1) == 1
                acc = [k.acc[j, c, at(h), :] for c in COMPS]
                for n, _ in STEPS:
                    for c in COMPS:
                        own = k.xs[n, c, at(h, 8), :]
                        far = jnp.where(x5 > 0, k.xs[n, c, at(h, 7), :], k.xs[n, c, at(h, 12), :])
                        close = rot(jnp.where(seg0, own, far), HALF)
                        acc[c] = acc[c] + (jnp.where(e, close, far) if n else jnp.where(e, own, close))
                for n, off in STEPS:
                    off *= XL
                    adj(acc, lambda c: k.lkt[lt(n, i, j), c, at(h, R0 - off), :], psi_of(i, j, h, -off))
                psi = psi_of(i, j, h)
                far = [jnp.where(x5 < 4, u, v) for u, v in zip(psi_of(i, j, h, 1), psi_of(i, j, h, -4))]
                close = [rot(jnp.where(seg0, far[c], psi[c]), HALF) for c in COMPS]
                mat(acc, lambda c: k.lko[lo(3, 0, o, j), c, at(h), :], [jnp.where(e, close[c], psi[c]) for c in COMPS])
                mat(acc, lambda c: k.lko[lo(3, 1, o, j), c, at(h), :], [jnp.where(e, far[c], close[c]) for c in COMPS])
                for c in COMPS:
                    k.acc[j, c, at(h), :] = acc[c]
            return 0

        lax.fori_loop(0, 2, one_plane, 0)

    m2 = mass[0] * mass[0]

    def store_odd(j, h, real, acc):
        for c in COMPS:
            k.f[9 + j, c, at(h, R0), :] = acc[c]

    def update_even(j, h, real, acc):
        cw, aw, ax, beta = (jnp.broadcast_to(k.cf[v, 0:1], (BLK, LANES)) for v in range(4))
        gg, dd = zeros, zeros
        for c in COMPS:
            sl, fl = (j, c, at(h), slice(None)), (j, c, at(h, R0), slice(None))
            w = jnp.where(real, k.f[fl], 0.0)
            n = m2 * w - acc[c]
            zv = n + beta * k.z[sl]
            sv = w + beta * k.s[sl]
            r = k.r[sl]
            pv = r + beta * k.p[sl]
            k.x[sl] = k.x[sl] + ax * pv
            r = r - ax * sv
            w = cw * w - aw * zv
            k.z[sl], k.s[sl], k.p[sl], k.r[sl], k.f[fl] = zv, sv, pv, r, w
            gg = gg + r * r
            dd = dd + w * r
        for v, t in enumerate((gg, dd)):
            k.gd[v] = k.gd[v] + (t[:8] + t[8:])

    def finish(i, t, update):
        o = 1 - i
        for cp in h_copies(i, t):
            cp.wait_recv()

        def one_plane(n2, _):
            j = plane_of(t, n2)
            slot = 2 * t + n2
            for c in COMPS:
                k.f[9 * i + j, c, pl.ds(R0 + VALID, R0), :] = k.trf[i, slot, c]
            yf, yc = k.yrf[i, slot], k.yrc[i, slot]
            for h in BLOCKS:
                frm = [4 * c + 24 * (h // BLK) for c in COMPS]
                top = (ylane >= YL) & (ylane < YL + 3)
                psi = [jnp.where(top, rot(yf, YL - frm[c]), v) for c, v in enumerate(psi_of(i, j, h))]
                acc = [k.acc[j, c, at(h), :] + jnp.where(ylane < 3, rot(yc, -frm[c]), 0.0) for c in COMPS]
                if h == 0:
                    acc = [acc[c] + k.trc[i, slot, c] for c in COMPS]
                for n, off in STEPS:
                    mat(acc, lambda c: k.lkt[lt(n, o, j), c, at(h, R0), :], psi_of(i, j, h, XL * off))
                for n, off in STEPS:
                    mat(acc, lambda c: k.lko[lo(1, n, o, j), c, at(h), :], psi_of(i, j + off, h))
                    jb, on = jnp.maximum(j - off, 0), jnp.where(j >= off, 1.0, 0.0)
                    adj(acc, lambda c: k.lko[lo(1, n, i, jb), c, at(h), :], [on * v for v in psi_of(i, jb, h)])
                for n, off in STEPS:
                    mat(acc, lambda c: k.lko[lo(2, n, o, j), c, at(h), :], [rot(psi[c], -off) for c in COMPS])
                real = row_b + h < VALID
                good = real & (ylane < YL)
                update(j, h, real, [jnp.where(good, acc[c], 0.0) for c in COMPS])
            return 0

        lax.fori_loop(0, 2, one_plane, 0)

    def a_copies(stage, b):
        mine = k.rb.at[b, iy] if stage else k.ra.at[b, 4 * iz + it]
        return [remote(mine, mine, k.a_ss.at[b, d], k.a_rs.at[b, d], dev) for d, dev in enumerate(near + ring) if (d >= len(near)) == bool(stage)]

    def sum_start(b, n):
        tile = zero8
        for v in range(n):
            tile = jnp.where(row8 == v, jnp.sum(k.gd[v], axis=0, keepdims=True), tile)
        k.ra[b, 4 * iz + it] = tile
        for cp in a_copies(0, b):
            cp.start()

    def sum_next(b):
        for cp in a_copies(0, b):
            cp.wait()
        k.rb[b, iy] = sum(k.ra[b, d] for d in range(1, 8)) + k.ra[b, 0]
        for cp in a_copies(1, b):
            cp.start()

    def sum_end(b, n):
        for cp in a_copies(1, b):
            cp.wait()
        tile = sum(k.rb[b, d] for d in others) + k.rb[b, 0]
        tile = jnp.broadcast_to(jnp.sum(tile, axis=1, keepdims=True), (8, LANES))
        return [jnp.broadcast_to(tile[v:v + 1], (8, LANES)) for v in range(n)]

    CW, AW, AX, BETA, GAMMA, ALPHA, FIRST = range(7)
    one = jnp.ones((8, LANES), F32)
    for v, t in ((CW, zero8), (AW, -one), (AX, zero8), (BETA, zero8), (GAMMA, one), (ALPHA, one)):
        k.cf[v] = t

    def scalars(step, gamma, delta):
        @pl.when(step == 1)
        def _():
            k.cf[ALPHA] = gamma / delta
            k.cf[FIRST] = gamma

        @pl.when(step > 1)
        def _():
            beta = gamma / k.cf[GAMMA]
            k.cf[BETA] = beta
            k.cf[ALPHA] = gamma / (delta - beta * gamma / k.cf[ALPHA])
            res[step - 2] = (gamma / k.cf[FIRST])[0, 0]
        k.cf[CW], k.cf[AW], k.cf[AX], k.cf[GAMMA] = one, k.cf[ALPHA], k.cf[ALPHA], gamma

    def phase(u, _):
        begin = u < 4
        n, ph = jnp.maximum(u - 4, 0) // 3, lax.rem(u + 2, 3)
        i = lax.rem(n, 2)
        step = n // 2
        b = lax.rem(step, 2)
        t = jnp.where(ph == 0, 0, jnp.where((ph == 1) == (i == 0), 1, 2))
        live = u >= 4
        more = n < 2 * ITERS - 1

        @pl.when(begin)
        def _():
            lax.fori_loop(ZL * u, ZL * (u + 1), load_step, 0)

        @pl.when(live & (i == 0) & (ph == 2) & (step > 0))
        def _():
            sum_next(b)

        @pl.when(live & (i == 1) & (ph == 0))
        def _():
            @pl.when(step > 0)
            def _():
                scalars(step, *sum_end(b, 2))
            k.gd[0], k.gd[1] = zero8, zero8

        @pl.when(live)
        def _():
            receive(i, t)

            @pl.when(i == 0)
            def _():
                finish(0, t, store_odd)

            @pl.when(i == 1)
            def _():
                finish(1, t, update_even)

        o = jnp.where(begin, 0, 1 - i)

        def send_one(g, _):
            send(o, g)
            return 0

        lax.fori_loop(jnp.where(begin, 0, t), jnp.where(begin, jnp.where(u == 0, 3, 0), jnp.where(more, t + 1, t)), send_one, 0)

        @pl.when((begin & (u > 0)) | (live & more))
        def _():
            tell(o, jnp.where(begin, u - 1, t))

        def post_one(e, _):
            late = begin | (e == 2)
            post(jnp.where(late, o, i), jnp.where(begin, u - 1, jnp.where(late, 0, e + 1)))
            return 0

        first = jnp.where(begin | (n == 0), 2, 0)
        busy = jnp.where(begin, u > 0, ph == 0)
        lax.fori_loop(first, jnp.where(busy, jnp.where(more, 3, 2), first), post_one, 0)

        @pl.when(live & (ph == 2))
        def _():
            for m in range(6):
                z_copy(i, m).wait_send()
            for g in range(3):
                for cp in h_copies(i, g):
                    cp.wait_send()

            @pl.when((i == 1) & more)
            def _():
                sum_start(1 - b, 2)
        return 0

    lax.fori_loop(0, 4 + 3 * 2 * ITERS, phase, 0)

    def dots(j, carry):
        for c in COMPS:
            w, r, s = k.f[j, c, pl.ds(R0, ROWS), :], k.r[j, c], k.s[j, c]
            carry = tuple(t + u * v for t, (u, v) in zip(carry, ((r, r), (w, r), (w, w), (r, s), (w, s), (s, s))))
        return carry

    for v, t in enumerate(lax.fori_loop(0, ZL, dots, (jnp.zeros((ROWS, LANES), F32),) * 6)):
        k.gd[v] = sum(t[8 * b:8 * b + 8] for b in range(4))
    sum_start(0, 6)
    sum_next(0)
    rr, wr, ww, rs, ws, ss = sum_end(0, 6)
    beta = rr / k.cf[GAMMA]
    alpha = rr / (wr - beta * rr / k.cf[ALPHA])
    last = rr - 2.0 * alpha * (wr + beta * rs) + alpha * alpha * (ww + 2.0 * beta * ws + beta * beta * ss)
    for v, t in ((ITERS - 2, rr), (ITERS - 1, last)):
        res[v] = (t / k.cf[FIRST])[0, 0]
    alpha, beta = (jnp.broadcast_to(v[0:1], (ROWS, LANES)) for v in (alpha, beta))

    def out_plane(j, _):
        for c in COMPS:
            v = k.x[j, c] + alpha * (k.r[j, c] + beta * k.p[j, c])
            for s in range(2):
                k.sst[pl.ds(j * SITE + 6 * s + c, VALID, 12), :] = rot(v, HALF * s)[0:VALID, 0:YL]
        return 0

    lax.fori_loop(0, ZL, out_plane, 0)
    each_src(lambda *a: out_copy(*a).start())
    each_src(lambda *a: out_copy(*a).wait())


def solution(mesh):
    link_spec = P(None, 't', 'zz', 'yy', None, None, None, None)
    field_spec = P('t', 'zz', 'yy', None, None, None)

    def local_solve(fat_links, long_links, source, quark_mass):
        fat, lng = (jnp.transpose(v, (0, 1, 2, 4, 5, 6, 7, 3)).reshape(4, TL, ZL, SITE, YL) for v in (fat_links, long_links))
        src = jnp.transpose(source, (0, 1, 3, 4, 5, 2)).reshape(TL, SITE, YL)
        anywhere, scalar = (pl.BlockSpec(memory_space=space) for space in (pl.ANY, pltpu.SMEM))
        sol, res = pl.pallas_call(
            kernel,
            out_shape=tuple(jax.ShapeDtypeStruct(shape, F32) for shape in ((TL, SITE, YL), (8,))),
            in_specs=[anywhere] * 3 + [scalar],
            out_specs=(anywhere, scalar),
            scratch_shapes=list(SCRATCH.values()),
            compiler_params=pltpu.CompilerParams(collective_id=0, has_side_effects=True, vmem_limit_bytes=67043328),
            name='cg',
        )(fat, lng, src, quark_mass)
        return jnp.transpose(sol.reshape(TL, ZL, XH, 3, 2, YL), (0, 1, 5, 2, 3, 4)), res

    return jax.shard_map(local_solve, mesh=mesh, in_specs=(link_spec, link_spec, field_spec, P(None)), out_specs=(field_spec, P()), check_vma=False)
```

```python
import jax
import jax.numpy as jnp
from jax import lax
from jax.experimental import pallas as pl
from jax.experimental.pallas import tpu as pltpu
from jax.sharding import PartitionSpec as P

ITERS = 8
MESH = pl.DeviceIdType.MESH
F32 = jnp.float32
TL, ZL, YL, XH = 6, 6, 48, 10
R0 = 16
ROWS, LANES, HALF, VALID = 32, 128, 64, 30
XL = 5
NSTG = 4
COMPS, LINKS = range(6), range(18)
C0 = 3
STEPS = ((0, 1), (1, 3))
SITE = VALID * 2 * 6
LOADS = 4 * ZL
BLK = 16
BLOCKS = range(0, ROWS, BLK)


def vec(*shape):
    return pltpu.VMEM(shape + (LANES,), F32)


def plane():
    return vec(ZL, 6, ROWS)


def sems(*shape):
    return pltpu.SemaphoreType.DMA(shape)


def halo_t():
    return vec(2, ZL, 6, R0)


def halo_y():
    return vec(2, ZL, BLK)


SCRATCH = dict(
    lkt=vec(24, 18, 56), lko=vec(72, 18, ROWS), stg=pltpu.VMEM((2 * NSTG, 2304, YL), F32), sst=pltpu.VMEM((2304, YL), F32),
    f=vec(18, 6, 64), acc=plane(), cb=vec(2, 6, ROWS), xs=vec(2, 6, YL),
    r=plane(), p=plane(), s=plane(), z=plane(), x=plane(), zs=vec(2, 6, 136), zr=vec(2, 6, 136),
    tsf=halo_t(), trf=halo_t(), tsc=halo_t(), trc=halo_t(), ysf=halo_y(), yrf=halo_y(), ysc=halo_y(), yrc=halo_y(),
    ra=vec(2, 8, 8), rb=vec(2, 4, 8), gd=vec(6, 8), cf=vec(8, 8),
    stg_sem=sems(NSTG, 12), io_sem=sems(36), z_ss=sems(2, 6), z_rs=sems(2, 6), h_ss=sems(2, 3, 4), h_rs=sems(2, 3, 4),
    a_ss=sems(2, 10), a_rs=sems(2, 10),
)


def mat(acc, link, psi):
    for i in range(3):
        for j in range(3):
            a, b = link(6 * i + 2 * j), link(6 * i + 2 * j + 1)
            c, d = psi[2 * j], psi[2 * j + 1]
            acc[2 * i] = acc[2 * i] + (a * c - b * d)
            acc[2 * i + 1] = acc[2 * i + 1] + (a * d + b * c)


def adj(acc, link, psi):
    for j in range(3):
        for i in range(3):
            a, b = link(6 * j + 2 * i), link(6 * j + 2 * i + 1)
            c, d = psi[2 * j], psi[2 * j + 1]
            acc[2 * i] = acc[2 * i] - (a * c + b * d)
            acc[2 * i + 1] = acc[2 * i + 1] + (b * c - a * d)


def rot(v, n):
    n %= LANES
    return pltpu.roll(v, n, 1) if n else v


def kernel(fat, lng, src, mass, out, res, *scratch):
    k = type('Refs', (), {})()
    for name, ref in zip(SCRATCH, scratch):
        setattr(k, name, ref)
    iy, iz, it = lax.axis_index('yy'), lax.axis_index('zz'), lax.axis_index('t')

    def at_t(d):
        return (iy, iz, lax.rem(it + d, 4))

    def at_z(d=0):
        return (iy, 1 - iz, lax.rem(it + d, 4))

    def at_y(d):
        return (lax.rem(iy + d, 4), iz, it)

    def remote(src_ref, dst_ref, send, recv, dev):
        return pltpu.make_async_remote_copy(src_ref=src_ref, dst_ref=dst_ref, send_sem=send, recv_sem=recv, device_id=dev, device_id_type=MESH)

    others = range(1, 4)
    near = [at_t(d) for d in others] + [at_z(d) for d in range(4)]
    ring = [at_y(d) for d in others]

    def plane_of(t, n2):
        first = jnp.where(t == 0, 1, jnp.where(t == 1, 0, 3))
        return first + n2 * jnp.where(t == 0, 3, 2)

    def what(g):
        q = jnp.maximum(g - ZL, 0)
        d = lax.rem(q, 3)
        p = q // 3
        early = g < ZL
        return jnp.where(early, 1, jnp.where(d == 0, 0, d + 1)), jnp.where(early, g, plane_of(p // 2, lax.rem(p, 2)))

    def stg_copies(g):
        slot = lax.rem(g, NSTG)
        di, zi = what(g)
        return [pltpu.make_async_copy(ref.at[di, t, zi], k.stg.at[2 * slot + n, pl.ds(SITE * t, SITE)], k.stg_sem.at[slot, TL * n + t])
                for n, ref in enumerate((fat, lng)) for t in range(TL)]

    def each_src(act):
        for q in range(TL * ZL):
            zi, ti = q // TL, q % TL
            act(q, pl.ds(zi * SITE + ti * 60, 60), ti, pl.ds(zi * 60, 60))

    def src_copy(q, here, ti, there):
        return pltpu.make_async_copy(src.at[ti, there], k.sst.at[here], k.io_sem.at[q])

    def out_copy(q, here, ti, there):
        return pltpu.make_async_copy(k.sst.at[here], out.at[ti, there], k.io_sem.at[q])

    barrier = pltpu.get_barrier_semaphore()
    for dev in near + ring:
        pl.semaphore_signal(barrier, inc=1, device_id=dev, device_id_type=MESH)
    each_src(lambda *a: src_copy(*a).start())
    for g in range(NSTG):
        for cp in stg_copies(jnp.int32(g)):
            cp.start()

    lane8, row8 = (lax.broadcasted_iota(jnp.int32, (8, LANES), d) for d in (1, 0))
    ylane8 = lane8 % HALF
    lane, row = (lax.broadcasted_iota(jnp.int32, (ROWS, LANES), d) for d in (1, 0))
    lane_b, row_b = lane[:BLK], row[:BLK]
    ylane = lane_b % HALF
    seg0 = lane_b < HALF
    zero8 = jnp.zeros((8, LANES), F32)
    zeros = jnp.zeros((BLK, LANES), F32)

    def lt(n, o, zi):
        return (n * 2 + o) * ZL + zi

    def lo(di, n, o, zi):
        return (((di - 1) * 2 + n) * 2 + o) * ZL + zi

    def at(h, off=0):
        return pl.ds(off + h, BLK)

    def psi_of(i, j, h, off=0):
        return [k.f[9 * i + j, c, at(h, R0 + off), :] for c in COMPS]

    k.f[...] = jnp.zeros_like(k.f)
    for ref in (k.p, k.s, k.z, k.x):
        ref[...] = jnp.zeros_like(ref)
    k.lkt[:, :, 0:R0, :] = jnp.zeros((24, 18, R0, LANES), F32)
    k.lkt[:, :, R0 + ROWS:, :] = jnp.zeros((24, 18, 8, LANES), F32)

    k.stg[:, SITE * TL:, :] = jnp.zeros((2 * NSTG, 144, YL), F32)
    z16 = jnp.zeros((ROWS, R0), F32)

    def both(half):
        return jnp.where(row < VALID, jnp.concatenate([half[0], z16, half[1], z16], axis=1), 0.0)

    def src_plane(zi, _):
        for c in COMPS:
            v = both([k.sst[pl.ds(zi * SITE + 6 * s + c, ROWS, 12), :] for s in range(2)])
            k.f[zi, c, pl.ds(R0, ROWS), :] = v
            k.r[zi, c] = v
        return 0

    each_src(lambda *a: src_copy(*a).wait())
    lax.fori_loop(0, ZL, src_plane, 0)
    pl.semaphore_wait(barrier, len(near + ring))

    def convert(g, zi, ref, base, lead):
        slot = lax.rem(g, NSTG)
        even = ((row // XL + lane + zi) & 1) == 0
        rest = jnp.zeros((ROWS, LANES - YL), F32)

        def whole(n, c, h):
            v = [jnp.concatenate([k.stg[2 * slot + n, pl.ds(c + (2 * s + h) * 18, ROWS, 72), :], rest], axis=1) for s in range(2)]
            return v[0] + rot(v[1], HALF)

        for n in range(2):
            for c in LINKS:
                v = [whole(n, c, h) for h in range(2)]
                for o in range(2):
                    ref[lead(n, o, zi), c, pl.ds(base, ROWS), :] = jnp.where(even, v[o], v[1 - o])

    def load_step(g, _):
        di, zi = what(g)
        for cp in stg_copies(g):
            cp.wait()

        @pl.when(di == 0)
        def _():
            convert(g, zi, k.lkt, R0, lt)

        @pl.when(di > 0)
        def _():
            convert(g, zi, k.lko, 0, lambda n, o, zi: lo(di, n, o, zi))

        @pl.when(g + NSTG < LOADS)
        def _():
            for cp in stg_copies(g + NSTG):
                cp.start()
        return 0

    def z_copy(i, m):
        return remote(k.zs.at[i, m, used], k.zr.at[i, m, used], k.z_ss.at[i, m], k.z_rs.at[i, m], at_z())

    def h_copies(i, t):
        pairs = ((k.tsf, k.trf, at_t(3)), (k.tsc, k.trc, at_t(1)), (k.ysf, k.yrf, at_y(3)), (k.ysc, k.yrc, at_y(1)))
        two = pl.ds(2 * t, 2)
        return [remote(a.at[i, two], b.at[i, two], k.h_ss.at[i, t, n], k.h_rs.at[i, t, n], dev) for n, (a, b, dev) in enumerate(pairs)]

    gap = ylane8 >= YL
    used = pl.ds(0, 135)

    def rows_of(u, part, off=0):
        return pl.ds(off + 15 * (u % 2) + part, 8)

    def wire(host, part):
        return pl.ds(15 * host + part, 8)

    def pack(load, i, m):
        for u in range(3):
            for part in (0, 7):
                guest = load(9 + u, part)
                for q in range(3):
                    k.zs[i, m, wire(3 * q + u, part), :] = jnp.where(gap, rot(guest, YL - R0 * q), load(3 * q + u, part))

    def unpack(i, m, store):
        for u in range(3):
            for part in (0, 7):
                guest = zero8
                for q in range(3):
                    h = k.zr[i, m, wire(3 * q + u, part), :]
                    store(3 * q + u, part, jnp.where(gap, 0.0, h))
                    guest = jnp.where(ylane8 // R0 == q, rot(h, R0 * q - YL), guest)
                store(9 + u, part, guest)

    def start(i, *ms):
        for m in ms:
            z_copy(i, m).start()

    def arrive(i, *ms):
        for m in ms:
            z_copy(i, m).wait_recv()

    def pack_psi(i, m):
        pack(lambda u, part: k.f[9 * i + m, u // 2, rows_of(u, part, R0), :], i, m)

    def pack_c(i, m, b, *terms):
        for h in BLOCKS:
            acc = [zeros] * 6
            for n, j in terms:
                adj(acc, lambda c: k.lko[lo(1, n, i, j), c, at(h), :], psi_of(i, j, h))
            for c in COMPS:
                k.cb[b, c, at(h), :] = acc[c]
        pack(lambda u, part: k.cb[b, u // 2, rows_of(u, part), :], i, C0 + m)

    def unpack_psi(i, m):
        def store(u, part, v):
            k.f[9 * i + 6 + m, u // 2, rows_of(u, part, R0), :] = v
        unpack(i, m, store)

    def unpack_c(i, m):
        def store(u, part, v):
            w = jnp.where(row8 == 0, 0.0, v) if part else v
            k.acc[m, u // 2, rows_of(u, part), :] = k.acc[m, u // 2, rows_of(u, part), :] + w
        unpack(i, C0 + m, store)

    def send(i, t):
        @pl.when(t == 0)
        def _():
            pack_psi(i, 1)
            pack_c(i, 1, 0, (1, 4))
            start(i, 1, C0 + 1)

        @pl.when(t == 1)
        def _():
            pack_psi(i, 0)
            pack_psi(i, 2)
            start(i, 0, 2)

        @pl.when(t == 2)
        def _():
            pack_c(i, 0, 0, (0, 5), (1, 3))
            pack_c(i, 2, 1, (1, 5))
            start(i, C0, C0 + 2)

    def receive(i, t):
        @pl.when(t == 0)
        def _():
            arrive(i, 1, C0 + 1)
            unpack_psi(i, 1)
            unpack_c(i, 1)

        @pl.when(t == 1)
        def _():
            arrive(i, C0, C0 + 2)
            unpack_c(i, 0)
            unpack_c(i, 2)

        @pl.when(t == 2)
        def _():
            arrive(i, 0, 2)
            unpack_psi(i, 0)
            unpack_psi(i, 2)

    def tell(i, t):
        def one_plane(n2, _):
            j = plane_of(t, n2)
            slot = 2 * t + n2
            fwd, bwd = zeros, zeros
            for h in BLOCKS:
                psi = psi_of(i, j, h)
                back = [zeros] * 6
                for n, off in STEPS:
                    chi = [zeros] * 6
                    adj(chi, lambda c: k.lko[lo(2, n, i, j), c, at(h), :], psi)
                    back = [back[c] + rot(chi[c], off) for c in COMPS]
                for c in COMPS:
                    k.acc[j, c, at(h), :] = back[c]
                    to = 4 * c + 24 * (h // BLK)
                    here = ylane // 4 == to // 4
                    fwd = jnp.where(here, rot(psi[c], to), fwd)
                    bwd = jnp.where(here, rot(back[c], to - YL), bwd)
            k.ysf[i, slot] = fwd
            k.ysc[i, slot] = bwd
            for h in range(2):
                acc = [zero8] * 6
                for n, first in ((0, R0 + 25), (1, R0 + 15 + 8 * h)):
                    if n or not h:
                        adj(acc, lambda c: k.lkt[lt(n, i, j), c, pl.ds(first, 8), :], [k.f[9 * i + j, c, pl.ds(first, 8), :] for c in COMPS])
                for c in COMPS:
                    k.tsc[i, slot, c, pl.ds(8 * h, 8), :] = acc[c]
                    k.tsf[i, slot, c, pl.ds(8 * h, 8), :] = k.f[9 * i + j, c, pl.ds(R0 + 8 * h, 8), :]
            return 0

        lax.fori_loop(0, 2, one_plane, 0)
        for cp in h_copies(i, t):
            cp.start()

    def post(i, t):
        o = 1 - i

        def one_plane(n2, _):
            j = plane_of(t, n2)
            for h in BLOCKS:
                psi = psi_of(i, j, h)
                for n, _ in STEPS:
                    chi = [zeros] * 6
                    adj(chi, lambda c: k.lko[lo(3, n, i, j), c, at(h), :], psi)
                    for c in COMPS:
                        k.xs[n, c, at(h, 8), :] = chi[c]
            for h in BLOCKS:
                x5 = lax.rem(row_b + h, XL)
                e = (((row_b + h) // XL + lane_b + (j + o)) & 1) == 1
                acc = [k.acc[j, c, at(h), :] for c in COMPS]
                for n, _ in STEPS:
                    for c in COMPS:
                        own = k.xs[n, c, at(h, 8), :]
                        far = jnp.where(x5 > 0, k.xs[n, c, at(h, 7), :], k.xs[n, c, at(h, 12), :])
                        close = rot(jnp.where(seg0, own, far), HALF)
                        acc[c] = acc[c] + (jnp.where(e, close, far) if n else jnp.where(e, own, close))
                for n, off in STEPS:
                    off *= XL
                    adj(acc, lambda c: k.lkt[lt(n, i, j), c, at(h, R0 - off), :], psi_of(i, j, h, -off))
                psi = psi_of(i, j, h)
                far = [jnp.where(x5 < 4, u, v) for u, v in zip(psi_of(i, j, h, 1), psi_of(i, j, h, -4))]
                close = [rot(jnp.where(seg0, far[c], psi[c]), HALF) for c in COMPS]
                mat(acc, lambda c: k.lko[lo(3, 0, o, j), c, at(h), :], [jnp.where(e, close[c], psi[c]) for c in COMPS])
                mat(acc, lambda c: k.lko[lo(3, 1, o, j), c, at(h), :], [jnp.where(e, far[c], close[c]) for c in COMPS])
                for c in COMPS:
                    k.acc[j, c, at(h), :] = acc[c]
            return 0

        lax.fori_loop(0, 2, one_plane, 0)

    m2 = mass[0] * mass[0]

    def store_odd(j, h, real, acc):
        for c in COMPS:
            k.f[9 + j, c, at(h, R0), :] = acc[c]

    def update_even(j, h, real, acc):
        cw, aw, ax, beta = (jnp.broadcast_to(k.cf[v, 0:1], (BLK, LANES)) for v in range(4))
        gg, dd = zeros, zeros
        for c in COMPS:
            sl, fl = (j, c, at(h), slice(None)), (j, c, at(h, R0), slice(None))
            w = jnp.where(real, k.f[fl], 0.0)
            n = m2 * w - acc[c]
            zv = n + beta * k.z[sl]
            sv = w + beta * k.s[sl]
            r = k.r[sl]
            pv = r + beta * k.p[sl]
            k.x[sl] = k.x[sl] + ax * pv
            r = r - ax * sv
            w = cw * w - aw * zv
            k.z[sl], k.s[sl], k.p[sl], k.r[sl], k.f[fl] = zv, sv, pv, r, w
            gg = gg + r * r
            dd = dd + w * r
        for v, t in enumerate((gg, dd)):
            k.gd[v] = k.gd[v] + (t[:8] + t[8:])

    def finish(i, t, update):
        o = 1 - i
        for cp in h_copies(i, t):
            cp.wait_recv()

        def one_plane(n2, _):
            j = plane_of(t, n2)
            slot = 2 * t + n2
            for c in COMPS:
                k.f[9 * i + j, c, pl.ds(R0 + VALID, R0), :] = k.trf[i, slot, c]
            yf, yc = k.yrf[i, slot], k.yrc[i, slot]
            for h in BLOCKS:
                frm = [4 * c + 24 * (h // BLK) for c in COMPS]
                top = (ylane >= YL) & (ylane < YL + 3)
                psi = [jnp.where(top, rot(yf, YL - frm[c]), v) for c, v in enumerate(psi_of(i, j, h))]
                acc = [k.acc[j, c, at(h), :] + jnp.where(ylane < 3, rot(yc, -frm[c]), 0.0) for c in COMPS]
                if h == 0:
                    acc = [acc[c] + k.trc[i, slot, c] for c in COMPS]
                for n, off in STEPS:
                    mat(acc, lambda c: k.lkt[lt(n, o, j), c, at(h, R0), :], psi_of(i, j, h, XL * off))
                for n, off in STEPS:
                    mat(acc, lambda c: k.lko[lo(1, n, o, j), c, at(h), :], psi_of(i, j + off, h))
                    jb, on = jnp.maximum(j - off, 0), jnp.where(j >= off, 1.0, 0.0)
                    adj(acc, lambda c: k.lko[lo(1, n, i, jb), c, at(h), :], [on * v for v in psi_of(i, jb, h)])
                for n, off in STEPS:
                    mat(acc, lambda c: k.lko[lo(2, n, o, j), c, at(h), :], [rot(psi[c], -off) for c in COMPS])
                real = row_b + h < VALID
                good = real & (ylane < YL)
                update(j, h, real, [jnp.where(good, acc[c], 0.0) for c in COMPS])
            return 0

        lax.fori_loop(0, 2, one_plane, 0)

    def a_copies(stage, b):
        mine = k.rb.at[b, iy] if stage else k.ra.at[b, 4 * iz + it]
        return [remote(mine, mine, k.a_ss.at[b, d], k.a_rs.at[b, d], dev) for d, dev in enumerate(near + ring) if (d >= len(near)) == bool(stage)]

    def sum_start(b, n):
        tile = zero8
        for v in range(n):
            tile = jnp.where(row8 == v, jnp.sum(k.gd[v], axis=0, keepdims=True), tile)
        k.ra[b, 4 * iz + it] = tile
        for cp in a_copies(0, b):
            cp.start()

    def sum_next(b):
        for cp in a_copies(0, b):
            cp.wait()
        k.rb[b, iy] = sum(k.ra[b, d] for d in range(1, 8)) + k.ra[b, 0]
        for cp in a_copies(1, b):
            cp.start()

    def sum_end(b, n):
        for cp in a_copies(1, b):
            cp.wait()
        tile = sum(k.rb[b, d] for d in others) + k.rb[b, 0]
        tile = jnp.broadcast_to(jnp.sum(tile, axis=1, keepdims=True), (8, LANES))
        return [jnp.broadcast_to(tile[v:v + 1], (8, LANES)) for v in range(n)]

    CW, AW, AX, BETA, GAMMA, ALPHA, FIRST = range(7)
    one = jnp.ones((8, LANES), F32)
    for v, t in ((CW, zero8), (AW, -one), (AX, zero8), (BETA, zero8), (GAMMA, one), (ALPHA, one)):
        k.cf[v] = t

    def scalars(step, gamma, delta):
        @pl.when(step == 1)
        def _():
            k.cf[ALPHA] = gamma / delta
            k.cf[FIRST] = gamma

        @pl.when(step > 1)
        def _():
            beta = gamma / k.cf[GAMMA]
            k.cf[BETA] = beta
            k.cf[ALPHA] = gamma / (delta - beta * gamma / k.cf[ALPHA])
            res[step - 2] = (gamma / k.cf[FIRST])[0, 0]
        k.cf[CW], k.cf[AW], k.cf[AX], k.cf[GAMMA] = one, k.cf[ALPHA], k.cf[ALPHA], gamma

    def phase(u, _):
        last = u == 4
        begin = (u < 3) | last
        load = jnp.where(last, 3, u)
        v = jnp.where(u == 3, 0, jnp.maximum(u - 4, 0))
        n, ph = v // 3, lax.rem(v, 3)
        i = lax.rem(n, 2)
        step = n // 2
        b = lax.rem(step, 2)
        t = jnp.where(ph == 0, 0, jnp.where((ph == 1) == (i == 0), 1, 2))
        live = jnp.logical_not(begin)
        more = n < 2 * ITERS - 1

        @pl.when(begin)
        def _():
            lax.fori_loop(ZL * load, ZL * (load + 1), load_step, 0)

        @pl.when(live & (i == 0) & (ph == 2) & (step > 0))
        def _():
            sum_next(b)

        @pl.when(live & (i == 1) & (ph == 0))
        def _():
            @pl.when(step > 0)
            def _():
                scalars(step, *sum_end(b, 2))
            k.gd[0], k.gd[1] = zero8, zero8

        @pl.when(live)
        def _():
            receive(i, t)

            @pl.when(i == 0)
            def _():
                finish(0, t, store_odd)

            @pl.when(i == 1)
            def _():
                finish(1, t, update_even)

        o = jnp.where(begin, 0, 1 - i)

        def send_one(g, _):
            send(o, g)
            return 0

        lax.fori_loop(jnp.where(begin, 0, t), jnp.where(begin, jnp.where(u == 0, 3, 0), jnp.where(more, t + 1, t)), send_one, 0)

        @pl.when((begin & (u > 0)) | (live & more))
        def _():
            tell(o, jnp.where(begin, load - 1, t))

        def post_one(e, _):
            late = begin | (e == 2)
            post(jnp.where(late, o, i), jnp.where(begin, load - 1, jnp.where(late, 0, e + 1)))
            return 0

        first = jnp.where(begin | (n == 0), 2, 0)
        busy = jnp.where(begin, u > 0, ph == 0)
        lax.fori_loop(first, jnp.where(busy, jnp.where(more, 3, 2), first), post_one, 0)

        @pl.when(live & (ph == 2))
        def _():
            for m in range(6):
                z_copy(i, m).wait_send()
            for g in range(3):
                for cp in h_copies(i, g):
                    cp.wait_send()

            @pl.when((i == 1) & more)
            def _():
                sum_start(1 - b, 2)
        return 0

    lax.fori_loop(0, 4 + 3 * 2 * ITERS, phase, 0)

    def dots(j, carry):
        for c in COMPS:
            w, r, s = k.f[j, c, pl.ds(R0, ROWS), :], k.r[j, c], k.s[j, c]
            carry = tuple(t + u * v for t, (u, v) in zip(carry, ((r, r), (w, r), (w, w), (r, s), (w, s), (s, s))))
        return carry

    for v, t in enumerate(lax.fori_loop(0, ZL, dots, (jnp.zeros((ROWS, LANES), F32),) * 6)):
        k.gd[v] = sum(t[8 * b:8 * b + 8] for b in range(4))
    sum_start(0, 6)
    sum_next(0)
    parts = (k.sst, k.stg.at[0], k.stg.at[1])

    def out_plane(j, _):
        for to, frm in zip(parts, (k.x, k.r, k.p)):
            for c in COMPS:
                for s in range(2):
                    to[pl.ds(j * SITE + 6 * s + c, VALID, 12), :] = rot(frm[j, c], HALF * s)[0:VALID, 0:YL]
        return 0

    lax.fori_loop(0, ZL, out_plane, 0)
    rr, wr, ww, rs, ws, ss = sum_end(0, 6)
    beta = rr / k.cf[GAMMA]
    alpha = rr / (wr - beta * rr / k.cf[ALPHA])
    last = rr - 2.0 * alpha * (wr + beta * rs) + alpha * alpha * (ww + 2.0 * beta * ws + beta * beta * ss)
    for v, t in ((ITERS - 2, rr), (ITERS - 1, last)):
        res[v] = (t / k.cf[FIRST])[0, 0]
    alpha, beta = (jnp.broadcast_to(v[0:1, 0:YL], (SITE, YL)) for v in (alpha, beta))

    def out_rows(j, _):
        here = pl.ds(j * SITE, SITE)
        x, r, p = (ref[here, :] for ref in parts)
        k.sst[here, :] = x + alpha * (r + beta * p)
        return 0

    lax.fori_loop(0, ZL, out_rows, 0)
    each_src(lambda *a: out_copy(*a).start())
    each_src(lambda *a: out_copy(*a).wait())


def solution(mesh):
    link_spec = P(None, 't', 'zz', 'yy')
    field_spec = P('t', 'zz', 'yy')

    def local_solve(fat_links, long_links, source, quark_mass):
        fat, lng = (jnp.transpose(v, (0, 1, 2, 4, 5, 6, 7, 3)).reshape(4, TL, ZL, SITE, YL) for v in (fat_links, long_links))
        src = jnp.transpose(source, (0, 1, 3, 4, 5, 2)).reshape(TL, SITE, YL)
        anywhere, scalar = (pl.BlockSpec(memory_space=space) for space in (pl.ANY, pltpu.SMEM))
        sol, res = pl.pallas_call(
            kernel,
            out_shape=tuple(jax.ShapeDtypeStruct(shape, F32) for shape in ((TL, SITE, YL), (8,))),
            in_specs=[anywhere] * 3 + [scalar],
            out_specs=(anywhere, scalar),
            scratch_shapes=list(SCRATCH.values()),
            compiler_params=pltpu.CompilerParams(collective_id=0, has_side_effects=True, vmem_limit_bytes=67043328),
            name='cg',
        )(fat, lng, src, quark_mass)
        return jnp.transpose(sol.reshape(TL, ZL, XH, 3, 2, YL), (0, 1, 5, 2, 3, 4)), res

    return jax.shard_map(local_solve, mesh=mesh, in_specs=(link_spec, link_spec, field_spec, P()), out_specs=(field_spec, P()), check_vma=False)
```

```python
import jax
import jax.numpy as jnp
from jax import lax
from jax.experimental import pallas as pl
from jax.experimental.pallas import tpu as pltpu
from jax.sharding import PartitionSpec as P

ITERS = 8
MESH = pl.DeviceIdType.MESH
F32 = jnp.float32
TL, ZL, YL, XH = 6, 6, 48, 10
R0 = 16
ROWS, LANES, HALF, VALID = 32, 128, 64, 30
XL = 5
NSTG = 4
COMPS, LINKS = range(6), range(18)
C0 = 3
STEPS = ((0, 1), (1, 3))
SITE = VALID * 2 * 6
ORDER = 'z3z4z5t1y1t4y4z0z1x1x4t0y0t2y2t3y3t5y5x0x2z2x3x5'
FIRST_STEP = 'aadhlpptwwyy'
LOADS = 4 * ZL
PITCH, QUAD = 76, 72
BLK = 16
BLOCKS = range(0, ROWS, BLK)


def packed(values):
    return [sum(v << 5 * q for q, v in enumerate(values[w:w + 6])) for w in range(0, len(values), 6)]


def pick(words, q):
    word = words[-1]
    for w, value in enumerate(words[:-1]):
        word = jnp.where(q // 6 == w, value, word)
    return (word >> 5 * lax.rem(q, 6)) & 31


STEP_WORDS = packed(['tzyx'.index(ORDER[q]) * 8 + int(ORDER[q + 1]) for q in range(0, 2 * LOADS, 2)])
PHASE_WORDS = packed([ord(q) - ord('a') for q in FIRST_STEP])


def loop(first, last, act):
    def body(q, carry):
        act(q)
        return carry
    lax.fori_loop(first, last, body, 0)


def vec(*shape):
    return pltpu.VMEM(shape + (LANES,), F32)


def plane():
    return vec(ZL, 6, ROWS)


def sems(*shape):
    return pltpu.SemaphoreType.DMA(shape)


def halo_t():
    return vec(2, ZL, 6, R0)


def halo_y():
    return vec(2, ZL, BLK)


SCRATCH = dict(
    lkt=vec(24, 18, 56), lko=vec(72, 18, ROWS), stg=pltpu.VMEM((2 * NSTG, ROWS * PITCH, YL), F32), sst=pltpu.VMEM((2304, YL), F32),
    f=vec(18, 6, 64), acc=plane(), cb=vec(2, 6, ROWS), xs=vec(2, 6, YL),
    r=plane(), p=plane(), s=plane(), z=plane(), x=plane(), zs=vec(2, 6, 136), zr=vec(2, 6, 136),
    tsf=halo_t(), trf=halo_t(), tsc=halo_t(), trc=halo_t(), ysf=halo_y(), yrf=halo_y(), ysc=halo_y(), yrc=halo_y(),
    ra=vec(2, 32), gd=vec(6, 8), cf=vec(8, 8),
    stg_sem=sems(NSTG, 2), io_sem=sems(ZL), m_sem=sems(1), ms=pltpu.VMEM((1, 1), F32), z_ss=sems(2), z_rs=sems(2, 6), h_ss=sems(2, 4), h_rs=sems(2, 3, 4),
    a_ss=sems(2), a_rs=sems(2),
)


def terms(link, psi):
    for i in range(3):
        for j in range(3):
            at = 2 * (3 * i + j)
            yield i, j, link(at), link(at + 1), psi


def mat(acc, link, psi):
    for i, j, a, b, v in terms(link, psi):
        c, d = v[2 * j:2 * j + 2]
        acc[2 * i] = acc[2 * i] + (a * c - b * d)
        acc[2 * i + 1] = acc[2 * i + 1] + (a * d + b * c)


def adj(acc, link, psi):
    for j, i, a, b, v in terms(link, psi):
        c, d = v[2 * j:2 * j + 2]
        acc[2 * i] = acc[2 * i] - (a * c + b * d)
        acc[2 * i + 1] = acc[2 * i + 1] + (b * c - a * d)


def rot(v, n):
    n %= LANES
    return pltpu.roll(v, n, 1) if n else v


def kernel(fat, lng, src, mass, out, res, *scratch):
    k = type('Refs', (), {})()
    for name, ref in zip(SCRATCH, scratch):
        setattr(k, name, ref)
    iy, iz, it = lax.axis_index('yy'), lax.axis_index('zz'), lax.axis_index('t')

    def at_t(d):
        return (iy, iz, lax.rem(it + d, 4))

    def at_z():
        return (iy, 1 - iz, it)

    def at_y(d):
        return (lax.rem(iy + d, 4), iz, it)

    def remote(src_ref, dst_ref, send, recv, dev):
        return pltpu.make_async_remote_copy(src_ref=src_ref, dst_ref=dst_ref, send_sem=send, recv_sem=recv, device_id=dev, device_id_type=MESH)

    def at_any(d):
        return (iy + d // 8) & 3, (iz + d // 4) & 1, (it + d) & 3

    def each_other(act):
        for d in range(1, 32):
            act(d)

    def plane_of(t, n2):
        first = jnp.where(t == 0, 1, jnp.where(t == 1, 0, 3))
        return first + n2 * jnp.where(t == 0, 3, 2)

    def what(g):
        code = pick(STEP_WORDS, g)
        return code // 8, code & 7

    def stg_copies(g):
        slot = lax.rem(g, NSTG)
        di, zi = what(g)

        def to(n):
            return k.stg.at[2 * slot + n, pl.ds(0, VALID * PITCH)].reshape(TL, XL, PITCH, YL).at[:, :, pl.ds(0, QUAD)]
        return [pltpu.make_async_copy(ref.at[di, :, zi], to(n), k.stg_sem.at[slot, n]) for n, ref in enumerate((fat, lng))]

    def src_copy(zi):
        return pltpu.make_async_copy(src.at[:, pl.ds(60 * zi, 60)], k.sst.at[pl.ds(SITE * zi, SITE)].reshape(TL, 60, YL), k.io_sem.at[zi])

    mass_copy = pltpu.make_async_copy(mass, k.ms, k.m_sem.at[0])
    mass_copy.start()
    for zi in range(ZL):
        src_copy(zi).start()
    for g in range(NSTG):
        for cp in stg_copies(jnp.int32(g)):
            cp.start()
    barrier = pltpu.get_barrier_semaphore()
    each_other(lambda d: pl.semaphore_signal(barrier, inc=1, device_id=at_any(d), device_id_type=MESH))

    lane8, row8 = (lax.broadcasted_iota(jnp.int32, (8, LANES), d) for d in (1, 0))
    ylane8 = lane8 % HALF
    lane, row = (lax.broadcasted_iota(jnp.int32, (ROWS, LANES), d) for d in (1, 0))
    lane_b, row_b = lane[:BLK], row[:BLK]
    ylane = lane_b % HALF
    seg0 = lane_b < HALF
    zero8 = jnp.zeros((8, LANES), F32)
    zeros = jnp.zeros((BLK, LANES), F32)

    def lt(n, o, zi):
        return (n * 2 + o) * ZL + zi

    def lo(di, n, o, zi):
        return (((di - 1) * 2 + n) * 2 + o) * ZL + zi

    def at(h, off=0):
        return pl.ds(off + h, BLK)

    def psi_of(i, j, h, off=0):
        return [k.f[9 * i + j, c, at(h, R0 + off), :] for c in COMPS]

    k.f[...] = jnp.zeros_like(k.f)
    for ref in (k.p, k.s, k.z, k.x):
        ref[...] = jnp.zeros_like(ref)
    k.lkt[:, :, 0:R0, :] = jnp.zeros((24, 18, R0, LANES), F32)
    k.lkt[:, :, R0 + ROWS:, :] = jnp.zeros((24, 18, 8, LANES), F32)

    k.stg[:, VALID * PITCH:, :] = jnp.zeros((2 * NSTG, 2 * PITCH, YL), F32)
    z16 = jnp.zeros((ROWS, R0), F32)

    def both(half):
        return jnp.where(row < VALID, jnp.concatenate([half[0], z16, half[1], z16], axis=1), 0.0)

    def src_plane(zi):
        for c in COMPS:
            v = both([k.sst[pl.ds(zi * SITE + 6 * s + c, ROWS, 12), :] for s in range(2)])
            k.f[zi, c, pl.ds(R0, ROWS), :] = v
            k.r[zi, c] = v

    def convert(g, zi, ref, base, lead):
        slot = lax.rem(g, NSTG)
        even = ((row // XL + lane + zi) & 1) == 0
        rest = jnp.zeros((ROWS, LANES - YL), F32)

        def whole(n, c, h):
            v = [jnp.concatenate([k.stg[2 * slot + n, pl.ds(c + (2 * s + h) * 18, ROWS, PITCH), :], rest], axis=1) for s in range(2)]
            return v[0] + rot(v[1], HALF)

        for n in range(2):
            for c in LINKS:
                v = [whole(n, c, h) for h in range(2)]
                for o in range(2):
                    ref[lead(n, o, zi), c, pl.ds(base, ROWS), :] = jnp.where(even, v[o], v[1 - o])

    def load_step(g):
        di, zi = what(g)
        for cp in stg_copies(g):
            cp.wait()

        @pl.when(di == 0)
        def _():
            convert(g, zi, k.lkt, R0, lt)

        @pl.when(di > 0)
        def _():
            convert(g, zi, k.lko, 0, lambda n, o, zi: lo(di, n, o, zi))

        @pl.when(g + NSTG < LOADS)
        def _():
            for cp in stg_copies(g + NSTG):
                cp.start()

    def z_copy(i, m):
        return remote(k.zs.at[i, m, used], k.zr.at[i, m, used], k.z_ss.at[i], k.z_rs.at[i, m], at_z())

    def h_copies(i, t, whole=False):
        pairs = ((k.tsf, k.trf, at_t(3)), (k.tsc, k.trc, at_t(1)), (k.ysf, k.yrf, at_y(3)), (k.ysc, k.yrc, at_y(1)))
        some = pl.ds(0, ZL) if whole else pl.ds(2 * t, 2)
        return [remote(a.at[i, some], b.at[i, some], k.h_ss.at[i, n], k.h_rs.at[i, t, n], dev) for n, (a, b, dev) in enumerate(pairs)]

    def sent(i):
        remote(k.zs.at[i, :, used], k.zr.at[i, :, used], k.z_ss.at[i], k.z_rs.at[i, 0], at_z()).wait_send()
        for cp in h_copies(i, 0, True):
            cp.wait_send()

    gap = ylane8 >= YL
    used = pl.ds(0, 135)

    def rows_of(u, part, off=0):
        return pl.ds(off + 15 * (u % 2) + part, 8)

    def wire(host, part):
        return pl.ds(15 * host + part, 8)

    def pack(load, i, m):
        for u in range(3):
            for part in (0, 7):
                guest = load(9 + u, part)
                for q in range(3):
                    k.zs[i, m, wire(3 * q + u, part), :] = jnp.where(gap, rot(guest, YL - R0 * q), load(3 * q + u, part))

    def unpack(i, m, store):
        for u in range(3):
            for part in (0, 7):
                guest = zero8
                for q in range(3):
                    h = k.zr[i, m, wire(3 * q + u, part), :]
                    store(3 * q + u, part, jnp.where(gap, 0.0, h))
                    guest = jnp.where(ylane8 // R0 == q, rot(h, R0 * q - YL), guest)
                store(9 + u, part, guest)

    def start(i, *ms):
        for m in ms:
            z_copy(i, m).start()

    def arrive(i, *ms):
        for m in ms:
            z_copy(i, m).wait_recv()

    def pack_psi(i, m):
        pack(lambda u, part: k.f[9 * i + m, u // 2, rows_of(u, part, R0), :], i, m)

    def pack_c(i, m, b, *terms):
        for h in BLOCKS:
            acc = [zeros] * 6
            for n, j in terms:
                adj(acc, lambda c: k.lko[lo(1, n, i, j), c, at(h), :], psi_of(i, j, h))
            for c in COMPS:
                k.cb[b, c, at(h), :] = acc[c]
        pack(lambda u, part: k.cb[b, u // 2, rows_of(u, part), :], i, C0 + m)

    def unpack_psi(i, m):
        def store(u, part, v):
            k.f[9 * i + 6 + m, u // 2, rows_of(u, part, R0), :] = v
        unpack(i, m, store)

    def unpack_c(i, m):
        def store(u, part, v):
            w = jnp.where(row8 == 0, 0.0, v) if part else v
            k.acc[m, u // 2, rows_of(u, part), :] = k.acc[m, u // 2, rows_of(u, part), :] + w
        unpack(i, C0 + m, store)

    def send(i, t):
        @pl.when(t == 0)
        def _():
            pack_psi(i, 1)
            pack_c(i, 1, 0, (1, 4))
            start(i, 1, C0 + 1)

        @pl.when(t == 1)
        def _():
            pack_psi(i, 0)
            pack_psi(i, 2)
            start(i, 0, 2)

        @pl.when(t == 2)
        def _():
            pack_c(i, 0, 0, (0, 5), (1, 3))
            pack_c(i, 2, 1, (1, 5))
            start(i, C0, C0 + 2)

    def receive(i, t):
        @pl.when(t == 0)
        def _():
            arrive(i, 1, C0 + 1)
            unpack_psi(i, 1)
            unpack_c(i, 1)

        @pl.when(t == 1)
        def _():
            arrive(i, C0, C0 + 2)
            unpack_c(i, 0)
            unpack_c(i, 2)

        @pl.when(t == 2)
        def _():
            arrive(i, 0, 2)
            unpack_psi(i, 0)
            unpack_psi(i, 2)

    def tell(i, t):
        def one_plane(n2):
            j = plane_of(t, n2)
            slot = 2 * t + n2
            fwd, bwd = zeros, zeros
            for h in BLOCKS:
                psi = psi_of(i, j, h)
                back = [zeros] * 6
                for n, off in STEPS:
                    chi = [zeros] * 6
                    adj(chi, lambda c: k.lko[lo(2, n, i, j), c, at(h), :], psi)
                    back = [back[c] + rot(chi[c], off) for c in COMPS]
                for c in COMPS:
                    k.acc[j, c, at(h), :] = back[c]
                    to = 4 * c + 24 * (h // BLK)
                    here = ylane // 4 == to // 4
                    fwd = jnp.where(here, rot(psi[c], to), fwd)
                    bwd = jnp.where(here, rot(back[c], to - YL), bwd)
            k.ysf[i, slot] = fwd
            k.ysc[i, slot] = bwd
            for h in range(2):
                acc = [zero8] * 6
                for n, first in ((0, R0 + 25), (1, R0 + 15 + 8 * h)):
                    if n or not h:
                        adj(acc, lambda c: k.lkt[lt(n, i, j), c, pl.ds(first, 8), :], [k.f[9 * i + j, c, pl.ds(first, 8), :] for c in COMPS])
                for c in COMPS:
                    k.tsc[i, slot, c, pl.ds(8 * h, 8), :] = acc[c]
                    k.tsf[i, slot, c, pl.ds(8 * h, 8), :] = k.f[9 * i + j, c, pl.ds(R0 + 8 * h, 8), :]

        loop(0, 2, one_plane)
        for cp in h_copies(i, t):
            cp.start()

    def post(i, t):
        o = 1 - i

        def one_plane(n2):
            j = plane_of(t, n2)
            for h in BLOCKS:
                psi = psi_of(i, j, h)
                for n, _ in STEPS:
                    chi = [zeros] * 6
                    adj(chi, lambda c: k.lko[lo(3, n, i, j), c, at(h), :], psi)
                    for c in COMPS:
                        k.xs[n, c, at(h, 8), :] = chi[c]
            for h in BLOCKS:
                x5 = lax.rem(row_b + h, XL)
                e = (((row_b + h) // XL + lane_b + (j + o)) & 1) == 1
                acc = [k.acc[j, c, at(h), :] for c in COMPS]
                for n, _ in STEPS:
                    for c in COMPS:
                        own = k.xs[n, c, at(h, 8), :]
                        far = jnp.where(x5 > 0, k.xs[n, c, at(h, 7), :], k.xs[n, c, at(h, 12), :])
                        close = rot(jnp.where(seg0, own, far), HALF)
                        acc[c] = acc[c] + (jnp.where(e, close, far) if n else jnp.where(e, own, close))
                for n, off in STEPS:
                    off *= XL
                    adj(acc, lambda c: k.lkt[lt(n, i, j), c, at(h, R0 - off), :], psi_of(i, j, h, -off))
                psi = psi_of(i, j, h)
                far = [jnp.where(x5 < 4, u, v) for u, v in zip(psi_of(i, j, h, 1), psi_of(i, j, h, -4))]
                close = [rot(jnp.where(seg0, far[c], psi[c]), HALF) for c in COMPS]
                mat(acc, lambda c: k.lko[lo(3, 0, o, j), c, at(h), :], [jnp.where(e, close[c], psi[c]) for c in COMPS])
                mat(acc, lambda c: k.lko[lo(3, 1, o, j), c, at(h), :], [jnp.where(e, far[c], close[c]) for c in COMPS])
                for c in COMPS:
                    k.acc[j, c, at(h), :] = acc[c]

        loop(0, 2, one_plane)

    mass_copy.wait()
    m2 = k.ms[0, 0] * k.ms[0, 0]

    def store_odd(j, h, real, acc):
        for c in COMPS:
            k.f[9 + j, c, at(h, R0), :] = acc[c]

    def update_even(j, h, real, acc):
        cw, aw, ax, beta = (jnp.broadcast_to(k.cf[v, 0:1], (BLK, LANES)) for v in range(4))
        gg, dd = zeros, zeros
        for c in COMPS:
            sl, fl = (j, c, at(h), slice(None)), (j, c, at(h, R0), slice(None))
            w = jnp.where(real, k.f[fl], 0.0)
            n = m2 * w - acc[c]
            zv = n + beta * k.z[sl]
            sv = w + beta * k.s[sl]
            r = k.r[sl]
            pv = r + beta * k.p[sl]
            k.x[sl] = k.x[sl] + ax * pv
            r = r - ax * sv
            w = cw * w - aw * zv
            k.z[sl], k.s[sl], k.p[sl], k.r[sl], k.f[fl] = zv, sv, pv, r, w
            gg = gg + r * r
            dd = dd + w * r
        for v, t in enumerate((gg, dd)):
            k.gd[v] = k.gd[v] + (t[:8] + t[8:])

    def finish(i, t, update):
        o = 1 - i
        for cp in h_copies(i, t):
            cp.wait_recv()

        def one_plane(n2):
            j = plane_of(t, n2)
            slot = 2 * t + n2
            for c in COMPS:
                k.f[9 * i + j, c, pl.ds(R0 + VALID, R0), :] = k.trf[i, slot, c]
            yf, yc = k.yrf[i, slot], k.yrc[i, slot]
            for h in BLOCKS:
                frm = [4 * c + 24 * (h // BLK) for c in COMPS]
                top = (ylane >= YL) & (ylane < YL + 3)
                psi = [jnp.where(top, rot(yf, YL - frm[c]), v) for c, v in enumerate(psi_of(i, j, h))]
                acc = [k.acc[j, c, at(h), :] + jnp.where(ylane < 3, rot(yc, -frm[c]), 0.0) for c in COMPS]
                if h == 0:
                    acc = [acc[c] + k.trc[i, slot, c] for c in COMPS]
                for n, off in STEPS:
                    mat(acc, lambda c: k.lkt[lt(n, o, j), c, at(h, R0), :], psi_of(i, j, h, XL * off))
                for n, off in STEPS:
                    mat(acc, lambda c: k.lko[lo(1, n, o, j), c, at(h), :], psi_of(i, j + off, h))
                    jb, on = jnp.maximum(j - off, 0), jnp.where(j >= off, 1.0, 0.0)
                    adj(acc, lambda c: k.lko[lo(1, n, i, jb), c, at(h), :], [on * v for v in psi_of(i, jb, h)])
                for n, off in STEPS:
                    mat(acc, lambda c: k.lko[lo(2, n, o, j), c, at(h), :], [rot(psi[c], -off) for c in COMPS])
                real = row_b + h < VALID
                good = real & (ylane < YL)
                update(j, h, real, [jnp.where(good, acc[c], 0.0) for c in COMPS])

        loop(0, 2, one_plane)

    me = 8 * iy + 4 * iz + it

    def a_copy(b, first, rows, dev):
        here = k.ra.at[b, pl.ds(first, rows)]
        return remote(here, here, k.a_ss.at[b], k.a_rs.at[b], dev)

    def sum_start(b, n):
        mine = zeros[:1]
        for v in range(n):
            total = jnp.sum(jnp.sum(k.gd[v], axis=0, keepdims=True), axis=1, keepdims=True)
            mine = jnp.where(lane[:1] == v, total, mine)
        k.ra[b, pl.ds(me, 1), :] = mine
        each_other(lambda d: a_copy(b, me, 1, at_any(d)).start())

    def sum_end(b, n):
        a_copy(b, 0, 31, at_z()).wait()
        tile = jnp.sum(k.ra[b], axis=0, keepdims=True)
        return [jnp.broadcast_to(tile[:, v:v + 1], (8, LANES)) for v in range(n)]

    CW, AW, AX, BETA, GAMMA, ALPHA, FIRST = range(7)
    one = jnp.ones((8, LANES), F32)
    for v, t in ((CW, zero8), (AW, -one), (AX, zero8), (BETA, zero8), (GAMMA, one), (ALPHA, one)):
        k.cf[v] = t

    def scalars(step, gamma, delta):
        @pl.when(step == 1)
        def _():
            k.cf[ALPHA] = gamma / delta
            k.cf[FIRST] = gamma

        @pl.when(step > 1)
        def _():
            beta = gamma / k.cf[GAMMA]
            k.cf[BETA] = beta
            k.cf[ALPHA] = gamma / (delta - beta * gamma / k.cf[ALPHA])
            res[step - 2] = (gamma / k.cf[FIRST])[0, 0]
        k.cf[CW], k.cf[AW], k.cf[AX], k.cf[GAMMA] = one, k.cf[ALPHA], k.cf[ALPHA], gamma

    def phase(u):
        begin = (u < 5) | (u == 6) | (u == 7) | (u == 9)
        v = jnp.where(u > 9, u - 8, jnp.where(u > 6, 1, 0))
        n, ph = v // 3, lax.rem(v, 3)
        i = lax.rem(n, 2)
        step = n // 2
        b = lax.rem(step, 2)
        t = jnp.where(ph == 0, 0, jnp.where((ph == 1) == (i == 0), 1, 2))
        live = jnp.logical_not(begin)
        more = n < 2 * ITERS - 1

        @pl.when(begin)
        def _():
            loop(pick(PHASE_WORDS, jnp.minimum(u, 10)), pick(PHASE_WORDS, jnp.minimum(u + 1, 10)), load_step)

        @pl.when(u == 0)
        def _():
            for zi in range(ZL):
                src_copy(zi).wait()
            loop(0, ZL, src_plane)
            pl.semaphore_wait(barrier, 31)

        @pl.when(live & (i == 1) & (ph == 0))
        def _():
            @pl.when(step > 0)
            def _():
                scalars(step, *sum_end(b, 2))
            k.gd[0], k.gd[1] = zero8, zero8

        @pl.when(live)
        def _():
            receive(i, t)

            @pl.when(i == 0)
            def _():
                finish(0, t, store_odd)

            @pl.when(i == 1)
            def _():
                finish(1, t, update_even)

        @pl.when(live & (ph == 2) & (i == 1) & more)
        def _():
            sum_start(1 - b, 2)

        o = jnp.where(begin, 0, 1 - i)

        loop(0, jnp.where(begin, jnp.where(u < 2, u + 1, 0), jnp.where(more, 1, 0)), lambda e: send(o, jnp.where(begin, jnp.where(u == 0, 1, 2 * e), t)))

        @pl.when((begin & ((u == 2) | (u == 4) | (u == 6))) | (live & more))
        def _():
            tell(o, jnp.where(begin, u // 2 - 1, t))

        def post_one(e):
            late = begin | (e == 2)
            post(jnp.where(late, o, i), jnp.where(begin, u // 3 - 1, jnp.where(late, 0, e + 1)))

        first = jnp.where(begin | (n == 0), 2, 0)
        busy = jnp.where(begin, (u == 3) | (u == 7) | (u == 9), ph == 0)
        loop(first, jnp.where(busy, jnp.where(more, 3, 2), first), post_one)

        @pl.when(live & (ph == 2))
        def _():
            sent(i)

    loop(0, 8 + 3 * 2 * ITERS, phase)

    def dots(j, carry):
        for c in COMPS:
            w, r, s = k.f[j, c, pl.ds(R0, ROWS), :], k.r[j, c], k.s[j, c]
            carry = tuple(t + u * v for t, (u, v) in zip(carry, ((r, r), (w, r), (w, w), (r, s), (w, s), (s, s))))
        return carry

    for v, t in enumerate(lax.fori_loop(0, ZL, dots, (jnp.zeros((ROWS, LANES), F32),) * 6)):
        k.gd[v] = sum(t[8 * b:8 * b + 8] for b in range(4))
    sum_start(0, 6)
    parts = (k.sst, k.stg.at[0], k.stg.at[1])

    def out_plane(j):
        for to, frm in zip(parts, (k.x, k.r, k.p)):
            for c in COMPS:
                for s in range(2):
                    to[pl.ds(j * SITE + 6 * s + c, VALID, 12), :] = rot(frm[j, c], HALF * s)[0:VALID, 0:YL]

    loop(0, ZL, out_plane)
    rr, wr, ww, rs, ws, ss = sum_end(0, 6)
    beta = rr / k.cf[GAMMA]
    alpha = rr / (wr - beta * rr / k.cf[ALPHA])
    last = rr - 2.0 * alpha * (wr + beta * rs) + alpha * alpha * (ww + 2.0 * beta * ws + beta * beta * ss)
    for v, t in ((ITERS - 2, rr), (ITERS - 1, last)):
        res[v] = (t / k.cf[FIRST])[0, 0]
    alpha, beta = (jnp.broadcast_to(v[0:1, 0:YL], (SITE, YL)) for v in (alpha, beta))

    def out_rows(j):
        here = pl.ds(j * SITE, SITE)
        x, r, p = (ref[here, :] for ref in parts)
        v = x + alpha * (r + beta * p)
        for t in range(TL):
            out[t, pl.ds(j * 60, 60), :] = v[60 * t:60 * (t + 1)]

    loop(0, ZL, out_rows)


def solution(mesh):
    link_spec = P(None, 't', 'zz', 'yy')
    field_spec = P('t', 'zz', 'yy')

    def local_solve(fat_links, long_links, source, quark_mass):
        fat, lng = (jnp.transpose(v, (0, 1, 2, 4, 5, 6, 7, 3)).reshape(4, TL, ZL, XL, QUAD, YL) for v in (fat_links, long_links))
        src = jnp.transpose(source, (0, 1, 3, 4, 5, 2)).reshape(TL, SITE, YL)
        anywhere, local, scalar = (pl.BlockSpec(memory_space=space) for space in (pl.ANY, pltpu.VMEM, pltpu.SMEM))
        sol, res = pl.pallas_call(
            kernel,
            out_shape=(pltpu.VMEM((TL, SITE, YL), F32), pltpu.SMEM((8,), F32)),
            in_specs=[anywhere] * 4,
            out_specs=(local, scalar),
            scratch_shapes=list(SCRATCH.values()),
            compiler_params=pltpu.CompilerParams(collective_id=0, has_side_effects=True, vmem_limit_bytes=60000000),
            name='cg',
        )(fat, lng, src, quark_mass.reshape(1, 1))
        return jnp.transpose(sol.reshape(TL, ZL, XH, 3, 2, YL), (0, 1, 5, 2, 3, 4)), res

    return jax.shard_map(local_solve, mesh=mesh, in_specs=(link_spec, link_spec, field_spec, P()), out_specs=(field_spec, P()), check_vma=False)
```

```python
import jax
import jax.numpy as jnp
from jax import lax
from jax.experimental import pallas as pl
from jax.experimental.pallas import tpu as pltpu
from jax.sharding import PartitionSpec as P

ITERS = 8
MESH = pl.DeviceIdType.MESH
F32 = jnp.float32
TL, ZL, YL, XH = 6, 6, 48, 10
R0 = 16
ROWS, LANES, HALF, VALID = 32, 128, 64, 30
XL = 5
NSTG = 6
COMPS, LINKS = range(6), range(18)
C0 = 3
STEPS = ((0, 1), (1, 3))
SITE = VALID * 2 * 6
ORDER = 'z3z4z5t1y1t4y4z0z1x1x4t0y0t2y2t3y3t5y5x0x2z2x3x5'
FIRST_STEP = 'aadhlpptwwyy'
LOADS = 4 * ZL
PITCH, QUAD = 76, 72
BLK = 16
BLOCKS = range(0, ROWS, BLK)


def packed(values):
    return [sum(v << 5 * q for q, v in enumerate(values[w:w + 6])) for w in range(0, len(values), 6)]


def pick(words, q):
    word = words[-1]
    for w, value in enumerate(words[:-1]):
        word = jnp.where(q // 6 == w, value, word)
    return (word >> 5 * lax.rem(q, 6)) & 31


STEP_WORDS = packed(['tzyx'.index(ORDER[q]) * 8 + int(ORDER[q + 1]) for q in range(0, 2 * LOADS, 2)])
PHASE_WORDS = packed([ord(q) - ord('a') for q in FIRST_STEP])


def loop(first, last, act):
    def body(q, carry):
        act(q)
        return carry
    lax.fori_loop(first, last, body, 0)


def vec(*shape):
    return pltpu.VMEM(shape + (LANES,), F32)


def plane():
    return vec(ZL, 6, ROWS)


def sems(*shape):
    return pltpu.SemaphoreType.DMA(shape)


def halo_t():
    return vec(2, ZL, 6, R0)


def wires():
    return vec(2, 6, 136)


def halo_y():
    return vec(2, ZL, BLK)


SCRATCH = dict(
    lkt=vec(24, 18, 56), lko=vec(72, 18, ROWS), stg=pltpu.VMEM((2 * NSTG, ROWS * PITCH, YL), F32), sst=pltpu.VMEM((2304, YL), F32),
    f=vec(18, 6, 64), acc=plane(), cb=vec(2, 6, ROWS), xs=vec(2, 6, YL),
    r=plane(), p=plane(), s=plane(), z=plane(), x=plane(), zs=wires(), zr=wires(),
    tsf=halo_t(), trf=halo_t(), tsc=halo_t(), trc=halo_t(), ysf=halo_y(), yrf=halo_y(), ysc=halo_y(), yrc=halo_y(),
    ra=vec(2, 32), gd=vec(6, 8), cf=vec(8, 8),
    stg_sem=sems(NSTG, 2), io_sem=sems(ZL), z_ss=sems(2), z_rs=sems(2, 6), h_ss=sems(2, 4), h_rs=sems(2, 3, 4),
    a_ss=sems(2, 2), a_rs=sems(2, 2),
)


def terms(link, psi):
    for i in range(3):
        for j in range(3):
            at = 2 * (3 * i + j)
            yield i, j, link(at), link(at + 1), psi


def mat(acc, link, psi):
    for i, j, a, b, v in terms(link, psi):
        c, d = v[2 * j:2 * j + 2]
        acc[2 * i] = acc[2 * i] + (a * c - b * d)
        acc[2 * i + 1] = acc[2 * i + 1] + (a * d + b * c)


def adj(acc, link, psi):
    for j, i, a, b, v in terms(link, psi):
        c, d = v[2 * j:2 * j + 2]
        acc[2 * i] = acc[2 * i] - (a * c + b * d)
        acc[2 * i + 1] = acc[2 * i + 1] + (b * c - a * d)


def rot(v, n):
    n %= LANES
    return pltpu.roll(v, n, 1) if n else v


def kernel(fat, lng, src, mass, out, res, *scratch):
    k = type('Refs', (), {})()
    for name, ref in zip(SCRATCH, scratch):
        setattr(k, name, ref)
    iy, iz, it = lax.axis_index('yy'), lax.axis_index('zz'), lax.axis_index('t')

    def at_t(d):
        return (iy, iz, lax.rem(it + d, 4))

    def at_z():
        return (iy, 1 - iz, it)

    def at_y(d):
        return (lax.rem(iy + d, 4), iz, it)

    def remote(src_ref, dst_ref, send, recv, dev):
        return pltpu.make_async_remote_copy(src_ref=src_ref, dst_ref=dst_ref, send_sem=send, recv_sem=recv, device_id=dev, device_id_type=MESH)

    slab = [((iy + d // 4) & 3, iz, (it + d) & 3) for d in range(1, R0)]

    def plane_of(t, n2):
        first = jnp.where(t == 0, 1, jnp.where(t == 1, 0, 3))
        return first + n2 * jnp.where(t == 0, 3, 2)

    def what(g):
        code = pick(STEP_WORDS, g)
        return code // 8, code & 7

    def stg_copies(g):
        slot = lax.rem(g, NSTG)
        di, zi = what(g)

        def to(n):
            return k.stg.at[2 * slot + n, pl.ds(0, VALID * PITCH)].reshape(TL, XL, PITCH, YL).at[:, :, pl.ds(0, QUAD)]
        return [pltpu.make_async_copy(ref.at[di, :, zi], to(n), k.stg_sem.at[slot, n]) for n, ref in enumerate((fat, lng))]

    def src_copy(zi):
        return pltpu.make_async_copy(src.at[:, pl.ds(60 * zi, 60)], k.sst.at[pl.ds(SITE * zi, SITE)].reshape(TL, 60, YL), k.io_sem.at[zi])

    for zi in range(ZL):
        src_copy(zi).start()
    for g in range(NSTG):
        for cp in stg_copies(jnp.int32(g)):
            cp.start()
    barrier = pltpu.get_barrier_semaphore()
    for dev in slab + [at_z()]:
        pl.semaphore_signal(barrier, inc=1, device_id=dev, device_id_type=MESH)

    lane8, row8 = (lax.broadcasted_iota(jnp.int32, (8, LANES), d) for d in (1, 0))
    ylane8 = lane8 % HALF
    lane, row = (lax.broadcasted_iota(jnp.int32, (ROWS, LANES), d) for d in (1, 0))
    lane_b, row_b = lane[:BLK], row[:BLK]
    ylane = lane_b % HALF
    seg0 = lane_b < HALF
    zero8 = jnp.zeros((8, LANES), F32)
    zeros = jnp.zeros((BLK, LANES), F32)

    def lt(n, o, zi):
        return (n * 2 + o) * ZL + zi

    def lo(di, n, o, zi):
        return (((di - 1) * 2 + n) * 2 + o) * ZL + zi

    def at(h, off=0):
        return pl.ds(off + h, BLK)

    def psi_of(i, j, h, off=0):
        return [k.f[9 * i + j, c, at(h, R0 + off), :] for c in COMPS]

    k.f[...] = jnp.zeros_like(k.f)
    for ref in (k.p, k.s, k.z, k.x):
        ref[...] = jnp.zeros_like(ref)
    k.lkt[:, :, 0:R0, :] = jnp.zeros((24, 18, R0, LANES), F32)
    k.lkt[:, :, R0 + ROWS:, :] = jnp.zeros((24, 18, 8, LANES), F32)

    k.stg[:, VALID * PITCH:, :] = jnp.zeros((2 * NSTG, 2 * PITCH, YL), F32)
    def whole(half):
        rest = jnp.zeros((ROWS, LANES - YL), F32)
        first, second = (jnp.concatenate([v, rest], axis=1) for v in half)
        return first + rot(second, HALF)

    def src_plane(zi):
        for c in COMPS:
            v = jnp.where(row < VALID, whole([k.sst[pl.ds(zi * SITE + 6 * s + c, ROWS, 12), :] for s in range(2)]), 0.0)
            k.f[zi, c, pl.ds(R0, ROWS), :] = v
            k.r[zi, c] = v

    def convert(g, zi, ref, base, lead):
        slot = lax.rem(g, NSTG)
        even = ((row // XL + lane + zi) & 1) == 0
        for n in range(2):
            for c in LINKS:
                v = [whole([k.stg[2 * slot + n, pl.ds(c + (2 * s + h) * 18, ROWS, PITCH), :] for s in range(2)]) for h in range(2)]
                for o in range(2):
                    ref[lead(n, o, zi), c, pl.ds(base, ROWS), :] = jnp.where(even, v[o], v[1 - o])

    def load_step(g):
        di, zi = what(g)
        for cp in stg_copies(g):
            cp.wait()

        @pl.when(di == 0)
        def _():
            convert(g, zi, k.lkt, R0, lt)

        @pl.when(di > 0)
        def _():
            convert(g, zi, k.lko, 0, lambda n, o, zi: lo(di, n, o, zi))

        @pl.when(g + NSTG < LOADS)
        def _():
            for cp in stg_copies(g + NSTG):
                cp.start()

    def z_copy(i, m):
        return remote(k.zs.at[i, m, used], k.zr.at[i, m, used], k.z_ss.at[i], k.z_rs.at[i, m], at_z())

    def h_copies(i, t, whole=False):
        pairs = ((k.tsf, k.trf, at_t(3)), (k.tsc, k.trc, at_t(1)), (k.ysf, k.yrf, at_y(3)), (k.ysc, k.yrc, at_y(1)))
        some = pl.ds(0, ZL) if whole else pl.ds(2 * t, 2)
        return [remote(a.at[i, some], b.at[i, some], k.h_ss.at[i, n], k.h_rs.at[i, t, n], dev) for n, (a, b, dev) in enumerate(pairs)]

    def sent(i):
        remote(k.zs.at[i, :, used], k.zr.at[i, :, used], k.z_ss.at[i], k.z_rs.at[i, 0], at_z()).wait_send()
        for cp in h_copies(i, 0, True):
            cp.wait_send()

    gap = ylane8 >= YL
    used = pl.ds(0, 135)

    def rows_of(u, part, off=0):
        return pl.ds(off + 15 * (u % 2) + part, 8)

    def wire(host, part):
        return pl.ds(15 * host + part, 8)

    def pack(load, i, m):
        for u in range(3):
            for part in (0, 7):
                guest = load(9 + u, part)
                for q in range(3):
                    k.zs[i, m, wire(3 * q + u, part), :] = jnp.where(gap, rot(guest, YL - R0 * q), load(3 * q + u, part))

    def unpack(i, m, store):
        for u in range(3):
            for part in (0, 7):
                guest = zero8
                for q in range(3):
                    h = k.zr[i, m, wire(3 * q + u, part), :]
                    store(3 * q + u, part, jnp.where(gap, 0.0, h))
                    guest = jnp.where(ylane8 // R0 == q, rot(h, R0 * q - YL), guest)
                store(9 + u, part, guest)

    def start(i, *ms):
        for m in ms:
            z_copy(i, m).start()

    def arrive(i, *ms):
        for m in ms:
            z_copy(i, m).wait_recv()

    def pack_psi(i, m):
        pack(lambda u, part: k.f[9 * i + m, u // 2, rows_of(u, part, R0), :], i, m)

    def pack_c(i, m, b, *terms):
        for h in BLOCKS:
            acc = [zeros] * 6
            for n, j in terms:
                adj(acc, lambda c: k.lko[lo(1, n, i, j), c, at(h), :], psi_of(i, j, h))
            for c in COMPS:
                k.cb[b, c, at(h), :] = acc[c]
        pack(lambda u, part: k.cb[b, u // 2, rows_of(u, part), :], i, C0 + m)

    def unpack_psi(i, m):
        def store(u, part, v):
            k.f[9 * i + 6 + m, u // 2, rows_of(u, part, R0), :] = v
        unpack(i, m, store)

    def unpack_c(i, m):
        def store(u, part, v):
            w = jnp.where(row8 == 0, 0.0, v) if part else v
            k.acc[m, u // 2, rows_of(u, part), :] = k.acc[m, u // 2, rows_of(u, part), :] + w
        unpack(i, C0 + m, store)

    def send(i, t):
        @pl.when(t == 0)
        def _():
            pack_psi(i, 1)
            pack_c(i, 1, 0, (1, 4))
            start(i, 1, C0 + 1)

        @pl.when(t == 1)
        def _():
            pack_psi(i, 0)
            pack_psi(i, 2)
            start(i, 0, 2)

        @pl.when(t == 2)
        def _():
            pack_c(i, 0, 0, (0, 5), (1, 3))
            pack_c(i, 2, 1, (1, 5))
            start(i, C0, C0 + 2)

    def receive(i, t):
        @pl.when(t == 0)
        def _():
            arrive(i, 1, C0 + 1)
            unpack_psi(i, 1)
            unpack_c(i, 1)

        @pl.when(t == 1)
        def _():
            arrive(i, C0, C0 + 2)
            unpack_c(i, 0)
            unpack_c(i, 2)

        @pl.when(t == 2)
        def _():
            arrive(i, 0, 2)
            unpack_psi(i, 0)
            unpack_psi(i, 2)

    def tell(i, t):
        def one_plane(n2):
            j = plane_of(t, n2)
            slot = 2 * t + n2
            fwd, bwd = zeros, zeros
            for h in BLOCKS:
                psi = psi_of(i, j, h)
                back = [zeros] * 6
                for n, off in STEPS:
                    chi = [zeros] * 6
                    adj(chi, lambda c: k.lko[lo(2, n, i, j), c, at(h), :], psi)
                    back = [back[c] + rot(chi[c], off) for c in COMPS]
                for c in COMPS:
                    k.acc[j, c, at(h), :] = back[c]
                    to = 4 * c + 24 * (h // BLK)
                    here = ylane // 4 == to // 4
                    fwd = jnp.where(here, rot(psi[c], to), fwd)
                    bwd = jnp.where(here, rot(back[c], to - YL), bwd)
            k.ysf[i, slot] = fwd
            k.ysc[i, slot] = bwd
            for h in range(2):
                acc = [zero8] * 6
                for n, first in ((0, R0 + 25), (1, R0 + 15 + 8 * h)):
                    if n or not h:
                        adj(acc, lambda c: k.lkt[lt(n, i, j), c, pl.ds(first, 8), :], [k.f[9 * i + j, c, pl.ds(first, 8), :] for c in COMPS])
                for c in COMPS:
                    k.tsc[i, slot, c, pl.ds(8 * h, 8), :] = acc[c]
                    k.tsf[i, slot, c, pl.ds(8 * h, 8), :] = k.f[9 * i + j, c, pl.ds(R0 + 8 * h, 8), :]

        loop(0, 2, one_plane)
        for cp in h_copies(i, t):
            cp.start()

    def post(i, t):
        o = 1 - i

        def one_plane(n2):
            j = plane_of(t, n2)
            for h in BLOCKS:
                psi = psi_of(i, j, h)
                for n, _ in STEPS:
                    chi = [zeros] * 6
                    adj(chi, lambda c: k.lko[lo(3, n, i, j), c, at(h), :], psi)
                    for c in COMPS:
                        k.xs[n, c, at(h, 8), :] = chi[c]
            for h in BLOCKS:
                x5 = lax.rem(row_b + h, XL)
                e = (((row_b + h) // XL + lane_b + (j + o)) & 1) == 1
                acc = [k.acc[j, c, at(h), :] for c in COMPS]
                for n, _ in STEPS:
                    for c in COMPS:
                        own = k.xs[n, c, at(h, 8), :]
                        far = jnp.where(x5 > 0, k.xs[n, c, at(h, 7), :], k.xs[n, c, at(h, 12), :])
                        close = rot(jnp.where(seg0, own, far), HALF)
                        acc[c] = acc[c] + (jnp.where(e, close, far) if n else jnp.where(e, own, close))
                for n, off in STEPS:
                    off *= XL
                    adj(acc, lambda c: k.lkt[lt(n, i, j), c, at(h, R0 - off), :], psi_of(i, j, h, -off))
                psi = psi_of(i, j, h)
                far = [jnp.where(x5 < 4, u, v) for u, v in zip(psi_of(i, j, h, 1), psi_of(i, j, h, -4))]
                close = [rot(jnp.where(seg0, far[c], psi[c]), HALF) for c in COMPS]
                mat(acc, lambda c: k.lko[lo(3, 0, o, j), c, at(h), :], [jnp.where(e, close[c], psi[c]) for c in COMPS])
                mat(acc, lambda c: k.lko[lo(3, 1, o, j), c, at(h), :], [jnp.where(e, far[c], close[c]) for c in COMPS])
                for c in COMPS:
                    k.acc[j, c, at(h), :] = acc[c]

        loop(0, 2, one_plane)

    m2 = mass[0] * mass[0]

    def store_odd(j, h, real, acc):
        for c in COMPS:
            k.f[9 + j, c, at(h, R0), :] = acc[c]

    def update_even(j, h, real, acc):
        cw, aw, ax, beta = (jnp.broadcast_to(k.cf[v, 0:1], (BLK, LANES)) for v in range(4))
        gg, dd = zeros, zeros
        for c in COMPS:
            sl, fl = (j, c, at(h), slice(None)), (j, c, at(h, R0), slice(None))
            w = jnp.where(real, k.f[fl], 0.0)
            n = m2 * w - acc[c]
            zv = n + beta * k.z[sl]
            sv = w + beta * k.s[sl]
            r = k.r[sl]
            pv = r + beta * k.p[sl]
            k.x[sl] = k.x[sl] + ax * pv
            r = r - ax * sv
            w = cw * w - aw * zv
            k.z[sl], k.s[sl], k.p[sl], k.r[sl], k.f[fl] = zv, sv, pv, r, w
            gg = gg + r * r
            dd = dd + w * r
        for v, t in enumerate((gg, dd)):
            k.gd[v] = k.gd[v] + (t[:8] + t[8:])

    def finish(i, t, update):
        o = 1 - i
        for cp in h_copies(i, t):
            cp.wait_recv()

        def one_plane(n2):
            j = plane_of(t, n2)
            slot = 2 * t + n2
            for c in COMPS:
                k.f[9 * i + j, c, pl.ds(R0 + VALID, R0), :] = k.trf[i, slot, c]
            yf, yc = k.yrf[i, slot], k.yrc[i, slot]
            for h in BLOCKS:
                frm = [4 * c + 24 * (h // BLK) for c in COMPS]
                top = (ylane >= YL) & (ylane < YL + 3)
                psi = [jnp.where(top, rot(yf, YL - frm[c]), v) for c, v in enumerate(psi_of(i, j, h))]
                acc = [k.acc[j, c, at(h), :] + jnp.where(ylane < 3, rot(yc, -frm[c]), 0.0) for c in COMPS]
                if h == 0:
                    acc = [acc[c] + k.trc[i, slot, c] for c in COMPS]
                for n, off in STEPS:
                    mat(acc, lambda c: k.lkt[lt(n, o, j), c, at(h, R0), :], psi_of(i, j, h, XL * off))
                for n, off in STEPS:
                    mat(acc, lambda c: k.lko[lo(1, n, o, j), c, at(h), :], psi_of(i, j + off, h))
                    jb, on = jnp.maximum(j - off, 0), jnp.where(j >= off, 1.0, 0.0)
                    adj(acc, lambda c: k.lko[lo(1, n, i, jb), c, at(h), :], [on * v for v in psi_of(i, jb, h)])
                for n, off in STEPS:
                    mat(acc, lambda c: k.lko[lo(2, n, o, j), c, at(h), :], [rot(psi[c], -off) for c in COMPS])
                real = row_b + h < VALID
                good = real & (ylane < YL)
                update(j, h, real, [jnp.where(good, acc[c], 0.0) for c in COMPS])

        loop(0, 2, one_plane)

    me = R0 + 4 * iy + it

    def a_copy(b, stage, first, rows, dev):
        here = k.ra.at[b, pl.ds(first, rows)]
        return remote(here, here, k.a_ss.at[b, stage], k.a_rs.at[b, stage], dev)

    def sum_start(b, n):
        mine = zeros[:1]
        for v in range(n):
            total = jnp.sum(jnp.sum(k.gd[v], axis=0, keepdims=True), axis=1, keepdims=True)
            mine = jnp.where(lane[:1] == v, total, mine)
        k.ra[b, pl.ds(iz, 1), :] = mine
        a_copy(b, 0, iz, 1, at_z()).start()

    def sum_next(b):
        a_copy(b, 0, 0, 1, at_z()).wait()
        k.ra[b, pl.ds(me, 1), :] = k.ra[b, 0:1, :] + k.ra[b, 1:2, :]
        for dev in slab:
            a_copy(b, 1, me, 1, dev).start()

    def sum_end(b, n):
        a_copy(b, 1, R0, len(slab), at_z()).wait()
        tile = jnp.sum(k.ra[b, R0:], axis=0, keepdims=True)
        return [jnp.broadcast_to(tile[:, v:v + 1], (8, LANES)) for v in range(n)]

    CW, AW, AX, BETA, GAMMA, ALPHA, FIRST = range(7)
    one = jnp.ones((8, LANES), F32)
    for v, t in ((CW, zero8), (AW, -one), (AX, zero8), (BETA, zero8), (GAMMA, one), (ALPHA, one)):
        k.cf[v] = t

    def scalars(step, gamma, delta):
        @pl.when(step == 1)
        def _():
            k.cf[ALPHA] = gamma / delta
            k.cf[FIRST] = gamma

        @pl.when(step > 1)
        def _():
            beta = gamma / k.cf[GAMMA]
            k.cf[BETA] = beta
            k.cf[ALPHA] = gamma / (delta - beta * gamma / k.cf[ALPHA])
            res[step - 2] = (gamma / k.cf[FIRST])[0, 0]
        k.cf[CW], k.cf[AW], k.cf[AX], k.cf[GAMMA] = one, k.cf[ALPHA], k.cf[ALPHA], gamma

    def phase(u):
        begin = (u < 5) | (u == 6) | (u == 7) | (u == 9)
        v = jnp.where(u > 9, u - 8, jnp.where(u > 6, 1, 0))
        n, ph = v // 3, lax.rem(v, 3)
        i = lax.rem(n, 2)
        step = n // 2
        b = lax.rem(step, 2)
        t = jnp.where(ph == 0, 0, jnp.where((ph == 1) == (i == 0), 1, 2))
        live = jnp.logical_not(begin)
        more = n < 2 * ITERS - 1

        @pl.when(begin)
        def _():
            loop(pick(PHASE_WORDS, jnp.minimum(u, 10)), pick(PHASE_WORDS, jnp.minimum(u + 1, 10)), load_step)

        @pl.when(u == 0)
        def _():
            for zi in range(ZL):
                src_copy(zi).wait()
            loop(0, ZL, src_plane)
            pl.semaphore_wait(barrier, R0)

        @pl.when(live & (i == 0) & (ph == 1) & (step > 0))
        def _():
            sum_next(b)

        @pl.when(live & (i == 1) & (ph == 0))
        def _():
            @pl.when(step > 0)
            def _():
                scalars(step, *sum_end(b, 2))
            k.gd[0], k.gd[1] = zero8, zero8

        @pl.when(live)
        def _():
            receive(i, t)

            @pl.when(i == 0)
            def _():
                finish(0, t, store_odd)

            @pl.when(i == 1)
            def _():
                finish(1, t, update_even)

        @pl.when(live & (ph == 2) & (i == 1) & more)
        def _():
            sum_start(1 - b, 2)

        o = jnp.where(begin, 0, 1 - i)

        loop(0, jnp.where(begin, jnp.where(u < 2, u + 1, 0), jnp.where(more, 1, 0)), lambda e: send(o, jnp.where(begin, jnp.where(u == 0, 1, 2 * e), t)))

        @pl.when((begin & ((u == 2) | (u == 4) | (u == 6))) | (live & more))
        def _():
            tell(o, jnp.where(begin, u // 2 - 1, t))

        def post_one(e):
            late = begin | (e == 2)
            post(jnp.where(late, o, i), jnp.where(begin, u // 3 - 1, jnp.where(late, 0, e + 1)))

        own = live & (ph == 0) & (n > 0)
        next_one = jnp.where(begin, (u == 3) | (u == 7) | (u == 9), (ph == 2) & more)
        loop(jnp.where(own, 0, 2), jnp.where(next_one, 3, 2), post_one)

        @pl.when(live & (ph == 2))
        def _():
            sent(i)

    loop(0, 8 + 3 * 2 * ITERS, phase)

    def dots(j, carry):
        for c in COMPS:
            w, r, s = k.f[j, c, pl.ds(R0, ROWS), :], k.r[j, c], k.s[j, c]
            carry = tuple(t + u * v for t, (u, v) in zip(carry, ((r, r), (w, r), (w, w), (r, s), (w, s), (s, s))))
        return carry

    for v, t in enumerate(lax.fori_loop(0, ZL, dots, (jnp.zeros((ROWS, LANES), F32),) * 6)):
        k.gd[v] = sum(t[8 * b:8 * b + 8] for b in range(4))
    sum_start(0, 6)
    sum_next(0)
    parts = (k.sst, k.stg.at[0], k.stg.at[1])

    def out_plane(j):
        for to, frm in zip(parts, (k.x, k.r, k.p)):
            for c in COMPS:
                for s in range(2):
                    to[pl.ds(j * SITE + 6 * s + c, VALID, 12), :] = rot(frm[j, c], HALF * s)[0:VALID, 0:YL]

    loop(0, ZL, out_plane)
    rr, wr, ww, rs, ws, ss = sum_end(0, 6)
    beta = rr / k.cf[GAMMA]
    alpha = rr / (wr - beta * rr / k.cf[ALPHA])
    last = rr - 2.0 * alpha * (wr + beta * rs) + alpha * alpha * (ww + 2.0 * beta * ws + beta * beta * ss)
    for v, t in ((ITERS - 2, rr), (ITERS - 1, last)):
        res[v] = (t / k.cf[FIRST])[0, 0]
    alpha, beta = (jnp.broadcast_to(v[0:1, 0:YL], (SITE, YL)) for v in (alpha, beta))

    def out_rows(j):
        here = pl.ds(j * SITE, SITE)
        x, r, p = (ref[here, :] for ref in parts)
        v = x + alpha * (r + beta * p)
        for t in range(TL):
            out[t, pl.ds(j * 60, 60), :] = v[60 * t:60 * (t + 1)]

    loop(0, ZL, out_rows)


def solution(mesh):
    link_spec = P(None, 't', 'zz', 'yy')
    field_spec = P('t', 'zz', 'yy')

    def local_solve(fat_links, long_links, source, quark_mass):
        fat, lng = (jnp.transpose(v, (0, 1, 2, 4, 5, 6, 7, 3)).reshape(4, TL, ZL, XL, QUAD, YL) for v in (fat_links, long_links))
        src = jnp.transpose(source, (0, 1, 3, 4, 5, 2)).reshape(TL, SITE, YL)
        anywhere, local, scalar = (pl.BlockSpec(memory_space=space) for space in (pl.ANY, pltpu.VMEM, pltpu.SMEM))
        sol, res = pl.pallas_call(
            kernel,
            out_shape=(pltpu.VMEM((TL, SITE, YL), F32), pltpu.SMEM((8,), F32)),
            in_specs=[anywhere] * 3 + [scalar],
            out_specs=(local, scalar),
            scratch_shapes=list(SCRATCH.values()),
            compiler_params=pltpu.CompilerParams(collective_id=0, has_side_effects=True, vmem_limit_bytes=65000000),
            name='cg',
        )(fat, lng, src, quark_mass)
        return jnp.transpose(sol.reshape(TL, ZL, XH, 3, 2, YL), (0, 1, 5, 2, 3, 4)), res

    return jax.shard_map(local_solve, mesh=mesh, in_specs=(link_spec, link_spec, field_spec, P()), out_specs=(field_spec, P()), check_vma=False)
```

```python
import jax
import jax.numpy as jnp
from jax import lax
from jax.experimental import pallas as pl
from jax.experimental.pallas import tpu as pltpu
from jax.sharding import PartitionSpec as P

ITERS = 8
MESH = pl.DeviceIdType.MESH
F32 = jnp.float32
TL, ZL, YL, XH = 6, 6, 48, 10
R0 = 16
ROWS, LANES, HALF, VALID = 32, 128, 64, 30
XL = 5
NSTG = 6
COMPS, LINKS = range(6), range(18)
C0 = 3
STEPS = ((0, 1), (1, 3))
SITE = VALID * 2 * 6
ORDER = 'z3z4z5t1y1t4y4z0z1x1x4t0y0t2y2t3y3t5y5x0x2z2x3x5'
FIRST_STEP = 'aadhlpptwwyy'
LOADS = 4 * ZL
PITCH, QUAD = 76, 72
BLK = 16
BLOCKS = range(0, ROWS, BLK)


def packed(values):
    return [sum(v << 5 * q for q, v in enumerate(values[w:w + 6])) for w in range(0, len(values), 6)]


def pick(words, q):
    word = words[-1]
    for w, value in enumerate(words[:-1]):
        word = jnp.where(q // 6 == w, value, word)
    return (word >> 5 * lax.rem(q, 6)) & 31


STEP_WORDS = packed(['tzyx'.index(ORDER[q]) * 8 + int(ORDER[q + 1]) for q in range(0, 2 * LOADS, 2)])
PHASE_WORDS = packed([ord(q) - ord('a') for q in FIRST_STEP])


def loop(first, last, act):
    def body(q, carry):
        act(q)
        return carry
    lax.fori_loop(first, last, body, 0)


def vec(*shape):
    return pltpu.VMEM(shape + (LANES,), F32)


def plane():
    return vec(ZL, 6, ROWS)


def sems(*shape):
    return pltpu.SemaphoreType.DMA(shape)


def halo_t():
    return vec(2, ZL, 6, R0)


def wires():
    return vec(2, 6, 136)


def halo_y():
    return vec(2, ZL, BLK)


SCRATCH = dict(
    lkt=vec(24, 18, 56), lko=vec(72, 18, ROWS), stg=pltpu.VMEM((2 * NSTG, ROWS * PITCH, YL), F32), sst=pltpu.VMEM((2304, YL), F32),
    f=vec(18, 6, 64), acc=plane(), cb=vec(2, 6, ROWS), xs=vec(2, 6, YL),
    r=plane(), p=plane(), s=plane(), z=plane(), x=plane(), zs=wires(), zr=wires(),
    tsf=halo_t(), trf=halo_t(), tsc=halo_t(), trc=halo_t(), ysf=halo_y(), yrf=halo_y(), ysc=halo_y(), yrc=halo_y(),
    ra=vec(2, 32), gd=vec(6, 8), cf=vec(8, 8),
    stg_sem=sems(NSTG, 2), io_sem=sems(ZL), z_ss=sems(2), z_rs=sems(2, 6), h_ss=sems(2, 4), h_rs=sems(2, 3, 4),
    a_ss=sems(2, 2), a_rs=sems(2, 2),
)


def terms(link, psi):
    for i in range(3):
        for j in range(3):
            at = 2 * (3 * i + j)
            yield i, j, link(at), link(at + 1), psi


def mat(acc, link, psi):
    for i, j, a, b, v in terms(link, psi):
        c, d = v[2 * j:2 * j + 2]
        acc[2 * i] = acc[2 * i] + (a * c - b * d)
        acc[2 * i + 1] = acc[2 * i + 1] + (a * d + b * c)


def adj(acc, link, psi):
    for j, i, a, b, v in terms(link, psi):
        c, d = v[2 * j:2 * j + 2]
        acc[2 * i] = acc[2 * i] - (a * c + b * d)
        acc[2 * i + 1] = acc[2 * i + 1] + (b * c - a * d)


def fold(v):
    return sum(v[first:first + 8] for first in range(0, len(v), 8))


def rot(v, n):
    n %= LANES
    return pltpu.roll(v, n, 1) if n else v


def kernel(fat, lng, src, mass, out, res, *scratch):
    k = type('Refs', (), {})()
    for name, ref in zip(SCRATCH, scratch):
        setattr(k, name, ref)
    iy, iz, it = lax.axis_index('yy'), lax.axis_index('zz'), lax.axis_index('t')

    def at_t(d):
        return (iy, iz, lax.rem(it + d, 4))

    def at_z():
        return (iy, 1 - iz, it)

    def at_y(d):
        return (lax.rem(iy + d, 4), iz, it)

    def remote(src_ref, dst_ref, send, recv, dev):
        return pltpu.make_async_remote_copy(src_ref=src_ref, dst_ref=dst_ref, send_sem=send, recv_sem=recv, device_id=dev, device_id_type=MESH)

    everyone = [((iy + d // 8) & 3, (iz + d // 4) & 1, (it + d) & 3) for d in range(1, ROWS)]
    slab = [((iy + d // 4) & 3, iz, (it + d) & 3) for d in range(1, R0)]

    def plane_of(t, n2):
        first = jnp.where(t == 0, 1, jnp.where(t == 1, 0, 3))
        return first + n2 * jnp.where(t == 0, 3, 2)

    def what(g):
        code = pick(STEP_WORDS, g)
        return code // 8, code & 7

    def stg_copies(g):
        slot = lax.rem(g, NSTG)
        di, zi = what(g)

        def to(n):
            return k.stg.at[2 * slot + n, pl.ds(0, VALID * PITCH)].reshape(TL, XL, PITCH, YL).at[:, :, pl.ds(0, QUAD)]
        return [pltpu.make_async_copy(ref.at[di, :, zi], to(n), k.stg_sem.at[slot, n]) for n, ref in enumerate((fat, lng))]

    def src_copy(zi):
        return pltpu.make_async_copy(src.at[:, pl.ds(60 * zi, 60)], k.sst.at[pl.ds(SITE * zi, SITE)].reshape(TL, 60, YL), k.io_sem.at[zi])

    for zi in range(ZL):
        src_copy(zi).start()
    for g in range(NSTG):
        for cp in stg_copies(jnp.int32(g)):
            cp.start()
    barrier = pltpu.get_barrier_semaphore()
    for dev in everyone:
        pl.semaphore_signal(barrier, inc=1, device_id=dev, device_id_type=MESH)

    lane8, row8 = (lax.broadcasted_iota(jnp.int32, (8, LANES), d) for d in (1, 0))
    ylane8 = lane8 % HALF
    lane, row = (lax.broadcasted_iota(jnp.int32, (ROWS, LANES), d) for d in (1, 0))
    lane_b, row_b = lane[:BLK], row[:BLK]
    ylane = lane_b % HALF
    seg0 = lane_b < HALF
    zero8 = jnp.zeros((8, LANES), F32)
    zeros = jnp.zeros((BLK, LANES), F32)

    def lt(n, o, zi):
        return (n * 2 + o) * ZL + zi

    def lo(di, n, o, zi):
        return (((di - 1) * 2 + n) * 2 + o) * ZL + zi

    def at(h, off=0):
        return pl.ds(off + h, BLK)

    def psi_of(i, j, h, off=0):
        return [k.f[9 * i + j, c, at(h, R0 + off), :] for c in COMPS]

    k.f[...] = jnp.zeros_like(k.f)
    for ref in (k.p, k.s, k.z, k.x, k.gd):
        ref[...] = jnp.zeros_like(ref)
    k.lkt[:, :, 0:R0, :] = jnp.zeros((24, 18, R0, LANES), F32)
    k.lkt[:, :, R0 + ROWS:, :] = jnp.zeros((24, 18, 8, LANES), F32)

    k.stg[:, VALID * PITCH:, :] = jnp.zeros((2 * NSTG, 2 * PITCH, YL), F32)
    def whole(half):
        rest = jnp.zeros((ROWS, LANES - YL), F32)
        first, second = (jnp.concatenate([v, rest], axis=1) for v in half)
        return first + rot(second, HALF)

    def src_plane(zi):
        for c in COMPS:
            v = jnp.where(row < VALID, whole([k.sst[pl.ds(zi * SITE + 6 * s + c, ROWS, 12), :] for s in range(2)]), 0.0)
            k.f[zi, c, pl.ds(R0, ROWS), :] = v
            k.r[zi, c] = v

    def convert(g, zi, ref, base, lead):
        slot = lax.rem(g, NSTG)
        even = ((row // XL + lane + zi) & 1) == 0
        for n in range(2):
            for c in LINKS:
                v = [whole([k.stg[2 * slot + n, pl.ds(c + (2 * s + h) * 18, ROWS, PITCH), :] for s in range(2)]) for h in range(2)]
                for o in range(2):
                    ref[lead(n, o, zi), c, pl.ds(base, ROWS), :] = jnp.where(even, v[o], v[1 - o])

    def load_step(g):
        di, zi = what(g)
        for cp in stg_copies(g):
            cp.wait()

        @pl.when(di == 0)
        def _():
            convert(g, zi, k.lkt, R0, lt)

        @pl.when(di > 0)
        def _():
            convert(g, zi, k.lko, 0, lambda n, o, zi: lo(di, n, o, zi))

        @pl.when(g + NSTG < LOADS)
        def _():
            for cp in stg_copies(g + NSTG):
                cp.start()

    def z_copy(i, m):
        return remote(k.zs.at[i, m, used], k.zr.at[i, m, used], k.z_ss.at[i], k.z_rs.at[i, m], at_z())

    def h_copies(i, t, whole=False):
        pairs = ((k.tsf, k.trf, at_t(3)), (k.tsc, k.trc, at_t(1)), (k.ysf, k.yrf, at_y(3)), (k.ysc, k.yrc, at_y(1)))
        some = pl.ds(0, ZL) if whole else pl.ds(2 * t, 2)
        return [remote(a.at[i, some], b.at[i, some], k.h_ss.at[i, n], k.h_rs.at[i, t, n], dev) for n, (a, b, dev) in enumerate(pairs)]

    def sent(i):
        remote(k.zs.at[i, :, used], k.zr.at[i, :, used], k.z_ss.at[i], k.z_rs.at[i, 0], at_z()).wait_send()
        for cp in h_copies(i, 0, True):
            cp.wait_send()

    gap = ylane8 >= YL
    used = pl.ds(0, 135)

    def rows_of(u, part, off=0):
        return pl.ds(off + 15 * (u % 2) + part, 8)

    def wire(host, part):
        return pl.ds(15 * host + part, 8)

    def pack(load, i, m):
        for u in range(3):
            for part in (0, 7):
                guest = load(9 + u, part)
                for q in range(3):
                    k.zs[i, m, wire(3 * q + u, part), :] = jnp.where(gap, rot(guest, YL - R0 * q), load(3 * q + u, part))

    def unpack(i, m, store):
        for u in range(3):
            for part in (0, 7):
                guest = zero8
                for q in range(3):
                    h = k.zr[i, m, wire(3 * q + u, part), :]
                    store(3 * q + u, part, jnp.where(gap, 0.0, h))
                    guest = jnp.where(ylane8 // R0 == q, rot(h, R0 * q - YL), guest)
                store(9 + u, part, guest)

    def start(i, *ms):
        for m in ms:
            z_copy(i, m).start()

    def arrive(i, *ms):
        for m in ms:
            z_copy(i, m).wait_recv()

    def pack_psi(i, m):
        pack(lambda u, part: k.f[9 * i + m, u // 2, rows_of(u, part, R0), :], i, m)

    def pack_c(i, m, b, *terms):
        for h in BLOCKS:
            acc = [zeros] * 6
            for n, j in terms:
                adj(acc, lambda c: k.lko[lo(1, n, i, j), c, at(h), :], psi_of(i, j, h))
            for c in COMPS:
                k.cb[b, c, at(h), :] = acc[c]
        pack(lambda u, part: k.cb[b, u // 2, rows_of(u, part), :], i, C0 + m)

    def unpack_psi(i, m):
        def store(u, part, v):
            k.f[9 * i + 6 + m, u // 2, rows_of(u, part, R0), :] = v
        unpack(i, m, store)

    def unpack_c(i, m):
        def store(u, part, v):
            w = jnp.where(row8 == 0, 0.0, v) if part else v
            k.acc[m, u // 2, rows_of(u, part), :] = k.acc[m, u // 2, rows_of(u, part), :] + w
        unpack(i, C0 + m, store)

    def send(i, t):
        @pl.when(t == 0)
        def _():
            pack_psi(i, 1)
            pack_c(i, 1, 0, (1, 4))
            start(i, 1, C0 + 1)

        @pl.when(t == 1)
        def _():
            pack_psi(i, 0)
            pack_psi(i, 2)
            start(i, 0, 2)

        @pl.when(t == 2)
        def _():
            pack_c(i, 0, 0, (0, 5), (1, 3))
            pack_c(i, 2, 1, (1, 5))
            start(i, C0, C0 + 2)

    def receive(i, t):
        @pl.when(t == 0)
        def _():
            arrive(i, 1, C0 + 1)
            unpack_psi(i, 1)
            unpack_c(i, 1)

        @pl.when(t == 1)
        def _():
            arrive(i, C0, C0 + 2)
            unpack_c(i, 0)
            unpack_c(i, 2)

        @pl.when(t == 2)
        def _():
            arrive(i, 0, 2)
            unpack_psi(i, 0)
            unpack_psi(i, 2)

    def tell(i, t):
        def one_plane(n2):
            j = plane_of(t, n2)
            slot = 2 * t + n2
            fwd, bwd = zeros, zeros
            for h in BLOCKS:
                psi = psi_of(i, j, h)
                back = [zeros] * 6
                for n, off in STEPS:
                    chi = [zeros] * 6
                    adj(chi, lambda c: k.lko[lo(2, n, i, j), c, at(h), :], psi)
                    back = [back[c] + rot(chi[c], off) for c in COMPS]
                for c in COMPS:
                    k.acc[j, c, at(h), :] = back[c]
                    to = 4 * c + 24 * (h // BLK)
                    here = ylane // 4 == to // 4
                    fwd = jnp.where(here, rot(psi[c], to), fwd)
                    bwd = jnp.where(here, rot(back[c], to - YL), bwd)
            k.ysf[i, slot] = fwd
            k.ysc[i, slot] = bwd
            for h in range(2):
                acc = [zero8] * 6
                for n, first in ((0, R0 + 25), (1, R0 + 15 + 8 * h)):
                    if n or not h:
                        adj(acc, lambda c: k.lkt[lt(n, i, j), c, pl.ds(first, 8), :], [k.f[9 * i + j, c, pl.ds(first, 8), :] for c in COMPS])
                for c in COMPS:
                    k.tsc[i, slot, c, pl.ds(8 * h, 8), :] = acc[c]
                    k.tsf[i, slot, c, pl.ds(8 * h, 8), :] = k.f[9 * i + j, c, pl.ds(R0 + 8 * h, 8), :]

        loop(0, 2, one_plane)
        for cp in h_copies(i, t):
            cp.start()

    def post(i, t):
        o = 1 - i

        def one_plane(n2):
            j = plane_of(t, n2)
            for h in BLOCKS:
                psi = psi_of(i, j, h)
                for n, _ in STEPS:
                    chi = [zeros] * 6
                    adj(chi, lambda c: k.lko[lo(3, n, i, j), c, at(h), :], psi)
                    for c in COMPS:
                        k.xs[n, c, at(h, 8), :] = chi[c]
            for h in BLOCKS:
                x5 = lax.rem(row_b + h, XL)
                e = (((row_b + h) // XL + lane_b + (j + o)) & 1) == 1
                acc = [k.acc[j, c, at(h), :] for c in COMPS]
                for n, _ in STEPS:
                    for c in COMPS:
                        own = k.xs[n, c, at(h, 8), :]
                        far = jnp.where(x5 > 0, k.xs[n, c, at(h, 7), :], k.xs[n, c, at(h, 12), :])
                        close = rot(jnp.where(seg0, own, far), HALF)
                        acc[c] = acc[c] + (jnp.where(e, close, far) if n else jnp.where(e, own, close))
                for n, off in STEPS:
                    off *= XL
                    adj(acc, lambda c: k.lkt[lt(n, i, j), c, at(h, R0 - off), :], psi_of(i, j, h, -off))
                psi = psi_of(i, j, h)
                far = [jnp.where(x5 < 4, u, v) for u, v in zip(psi_of(i, j, h, 1), psi_of(i, j, h, -4))]
                close = [rot(jnp.where(seg0, far[c], psi[c]), HALF) for c in COMPS]
                mat(acc, lambda c: k.lko[lo(3, 0, o, j), c, at(h), :], [jnp.where(e, close[c], psi[c]) for c in COMPS])
                mat(acc, lambda c: k.lko[lo(3, 1, o, j), c, at(h), :], [jnp.where(e, far[c], close[c]) for c in COMPS])
                for c in COMPS:
                    k.acc[j, c, at(h), :] = acc[c]

        loop(0, 2, one_plane)

    m2 = mass[0] * mass[0]

    def store_odd(j, h, real, acc):
        for c in COMPS:
            k.f[9 + j, c, at(h, R0), :] = acc[c]

    def update_even(j, h, real, acc):
        cw, aw, ax, beta = (jnp.broadcast_to(k.cf[v, 0:1], (BLK, LANES)) for v in range(4))
        gg, dd = zeros, zeros
        for c in COMPS:
            sl, fl = (j, c, at(h), slice(None)), (j, c, at(h, R0), slice(None))
            w = jnp.where(real, k.f[fl], 0.0)
            n = m2 * w - acc[c]
            zv = n + beta * k.z[sl]
            sv = w + beta * k.s[sl]
            r = k.r[sl]
            pv = r + beta * k.p[sl]
            k.x[sl] = k.x[sl] + ax * pv
            r = r - ax * sv
            w = cw * w - aw * zv
            k.z[sl], k.s[sl], k.p[sl], k.r[sl], k.f[fl] = zv, sv, pv, r, w
            gg = gg + r * r
            dd = dd + w * r
        for v, t in enumerate((gg, dd)):
            k.gd[v] = k.gd[v] + fold(t)

    def finish(i, t, update):
        o = 1 - i
        for cp in h_copies(i, t):
            cp.wait_recv()

        def one_plane(n2):
            j = plane_of(t, n2)
            slot = 2 * t + n2
            for c in COMPS:
                k.f[9 * i + j, c, pl.ds(R0 + VALID, R0), :] = k.trf[i, slot, c]
            yf, yc = k.yrf[i, slot], k.yrc[i, slot]
            for h in BLOCKS:
                frm = [4 * c + 24 * (h // BLK) for c in COMPS]
                top = (ylane >= YL) & (ylane < YL + 3)
                psi = [jnp.where(top, rot(yf, YL - frm[c]), v) for c, v in enumerate(psi_of(i, j, h))]
                acc = [k.acc[j, c, at(h), :] + jnp.where(ylane < 3, rot(yc, -frm[c]), 0.0) for c in COMPS]
                if h == 0:
                    acc = [acc[c] + k.trc[i, slot, c] for c in COMPS]
                for n, off in STEPS:
                    mat(acc, lambda c: k.lkt[lt(n, o, j), c, at(h, R0), :], psi_of(i, j, h, XL * off))
                for n, off in STEPS:
                    mat(acc, lambda c: k.lko[lo(1, n, o, j), c, at(h), :], psi_of(i, j + off, h))
                    jb, on = jnp.maximum(j - off, 0), jnp.where(j >= off, 1.0, 0.0)
                    adj(acc, lambda c: k.lko[lo(1, n, i, jb), c, at(h), :], [on * v for v in psi_of(i, jb, h)])
                for n, off in STEPS:
                    mat(acc, lambda c: k.lko[lo(2, n, o, j), c, at(h), :], [rot(psi[c], -off) for c in COMPS])
                real = row_b + h < VALID
                good = real & (ylane < YL)
                update(j, h, real, [jnp.where(good, acc[c], 0.0) for c in COMPS])

        loop(0, 2, one_plane)

    def a_copy(b, stage, first, rows, dev):
        here = k.ra.at[b, pl.ds(first, rows)]
        return remote(here, here, k.a_ss.at[b, stage], k.a_rs.at[b, stage], dev)

    def sum_start(b, n, stage, me, to):
        mine = zeros[:1]
        for v in range(n):
            total = jnp.sum(jnp.sum(k.gd[v], axis=0, keepdims=True), axis=1, keepdims=True)
            mine = jnp.where(lane[:1] == v, total, mine)
        k.ra[b, pl.ds(me, 1), :] = mine
        for dev in to:
            a_copy(b, stage, me, 1, dev).start()

    def sum_next(b):
        a_copy(b, 0, 0, 1, at_z()).wait()
        me = R0 + 4 * iy + it
        k.ra[b, pl.ds(me, 1), :] = k.ra[b, 0:1, :] + k.ra[b, 1:2, :]
        for dev in slab:
            a_copy(b, 1, me, 1, dev).start()

    def sum_end(b, n, to, first):
        a_copy(b, 1, first, len(to), at_z()).wait()
        tile = jnp.sum(k.ra[b, first:], axis=0, keepdims=True)
        return [jnp.broadcast_to(tile[:, v:v + 1], (8, LANES)) for v in range(n)]

    def dots(q):
        j = plane_of(jnp.where(q < 2, 0, jnp.where(q < 4, 2, 1)), lax.rem(q, 2))
        sums = [jnp.zeros((ROWS, LANES), F32)] * 4
        for c in COMPS:
            w, r, s = k.f[j, c, pl.ds(R0, ROWS), :], k.r[j, c], k.s[j, c]
            sums = [t + u * v for t, (u, v) in zip(sums, ((w, w), (r, s), (w, s), (s, s)))]
        for v, t in enumerate(sums):
            k.gd[2 + v] = k.gd[2 + v] + fold(t)

    CW, AW, AX, BETA, GAMMA, ALPHA, FIRST = range(7)
    one = jnp.ones((8, LANES), F32)
    for v, t in ((CW, zero8), (AW, -one), (AX, zero8), (BETA, zero8), (GAMMA, one), (ALPHA, one)):
        k.cf[v] = t

    def scalars(step, gamma, delta):
        @pl.when(step == 1)
        def _():
            k.cf[ALPHA] = gamma / delta
            k.cf[FIRST] = gamma

        @pl.when(step > 1)
        def _():
            beta = gamma / k.cf[GAMMA]
            k.cf[BETA] = beta
            k.cf[ALPHA] = gamma / (delta - beta * gamma / k.cf[ALPHA])
            res[step - 2] = (gamma / k.cf[FIRST])[0, 0]
        k.cf[CW], k.cf[AW], k.cf[AX], k.cf[GAMMA] = one, k.cf[ALPHA], k.cf[ALPHA], gamma

    def phase(u):
        begin = (u < 5) | (u == 6) | (u == 7) | (u == 9)
        v = jnp.where(u > 9, u - 8, jnp.where(u > 6, 1, 0))
        n, ph = v // 3, lax.rem(v, 3)
        i = lax.rem(n, 2)
        step = n // 2
        b = lax.rem(step, 2)
        t = jnp.where(ph == 0, 0, jnp.where((ph == 1) == (i == 0), 1, 2))
        live = jnp.logical_not(begin)
        more = n < 2 * ITERS - 1

        @pl.when(begin)
        def _():
            loop(pick(PHASE_WORDS, jnp.minimum(u, 10)), pick(PHASE_WORDS, jnp.minimum(u + 1, 10)), load_step)

        @pl.when(u == 0)
        def _():
            for zi in range(ZL):
                src_copy(zi).wait()
            loop(0, ZL, src_plane)
            pl.semaphore_wait(barrier, len(everyone))

        @pl.when(live & (i == 0) & (ph == 1) & (step > 0))
        def _():
            sum_next(b)

        @pl.when(live & (i == 1) & (ph == 0))
        def _():
            @pl.when(step > 0)
            def _():
                scalars(step, *sum_end(b, 2, slab, R0))
            k.gd[0], k.gd[1] = zero8, zero8

        @pl.when((ph == 2) & jnp.logical_not(more))
        def _():
            loop(0, 4, dots)

        @pl.when(live)
        def _():
            receive(i, t)

            @pl.when(i == 0)
            def _():
                finish(0, t, store_odd)

            @pl.when(i == 1)
            def _():
                finish(1, t, update_even)

        @pl.when(live & (ph == 2) & (i == 1) & more)
        def _():
            sum_start(1 - b, 2, 0, iz, [at_z()])

        o = jnp.where(begin, 0, 1 - i)

        loop(0, jnp.where(begin, jnp.where(u < 2, u + 1, 0), jnp.where(more, 1, 0)), lambda e: send(o, jnp.where(begin, jnp.where(u == 0, 1, 2 * e), t)))

        @pl.when((begin & ((u == 2) | (u == 4) | (u == 6))) | (live & more))
        def _():
            tell(o, jnp.where(begin, u // 2 - 1, t))

        def post_one(e):
            late = begin | (e == 2)
            post(jnp.where(late, o, i), jnp.where(begin, u // 3 - 1, jnp.where(late, 0, e + 1)))

        own = live & (ph == 0) & (n > 0)
        next_one = jnp.where(begin, (u == 3) | (u == 7) | (u == 9), (ph == 2) & more)
        loop(jnp.where(own, 0, 2), jnp.where(next_one, 3, 2), post_one)

        @pl.when(live & (ph == 2))
        def _():
            sent(i)

    loop(0, 8 + 3 * 2 * ITERS, phase)

    loop(4, ZL, dots)
    sum_start(0, 6, 1, 8 * iy + 4 * iz + it, everyone)
    parts = (k.sst, k.stg.at[0], k.stg.at[1])

    def out_plane(j):
        for to, frm in zip(parts, (k.x, k.r, k.p)):
            for c in COMPS:
                for s in range(2):
                    to[pl.ds(j * SITE + 6 * s + c, VALID, 12), :] = rot(frm[j, c], HALF * s)[0:VALID, 0:YL]

    loop(0, ZL, out_plane)
    rr, wr, ww, rs, ws, ss = sum_end(0, 6, everyone, 0)
    beta = rr / k.cf[GAMMA]
    alpha = rr / (wr - beta * rr / k.cf[ALPHA])
    last = rr - 2.0 * alpha * (wr + beta * rs) + alpha * alpha * (ww + 2.0 * beta * ws + beta * beta * ss)
    for v, t in ((ITERS - 2, rr), (ITERS - 1, last)):
        res[v] = (t / k.cf[FIRST])[0, 0]
    alpha, beta = (jnp.broadcast_to(v[0:1, 0:YL], (SITE, YL)) for v in (alpha, beta))

    def out_rows(j):
        here = pl.ds(j * SITE, SITE)
        x, r, p = (ref[here, :] for ref in parts)
        v = x + alpha * (r + beta * p)
        for t in range(TL):
            out[t, pl.ds(j * 60, 60), :] = v[60 * t:60 * (t + 1)]

    loop(0, ZL, out_rows)


def solution(mesh):
    link_spec = P(None, 't', 'zz', 'yy')
    field_spec = P('t', 'zz', 'yy')

    def local_solve(fat_links, long_links, source, quark_mass):
        fat, lng = (jnp.moveaxis(v, 3, -1).reshape(4, TL, ZL, XL, QUAD, YL) for v in (fat_links, long_links))
        src = jnp.moveaxis(source, 2, -1).reshape(TL, SITE, YL)
        anywhere, local, scalar = (pl.BlockSpec(memory_space=space) for space in (pl.ANY, pltpu.VMEM, pltpu.SMEM))
        sol, res = pl.pallas_call(
            kernel,
            out_shape=(pltpu.VMEM((TL, SITE, YL), F32), pltpu.SMEM((8,), F32)),
            in_specs=[anywhere] * 3 + [scalar],
            out_specs=(local, scalar),
            scratch_shapes=list(SCRATCH.values()),
            compiler_params=pltpu.CompilerParams(collective_id=0, has_side_effects=True, vmem_limit_bytes=65000000),
            name='cg',
        )(fat, lng, src, quark_mass)
        return jnp.moveaxis(sol.reshape(TL, ZL, XH, 3, 2, YL), -1, 2), res

    return jax.shard_map(local_solve, mesh=mesh, in_specs=(link_spec, link_spec, field_spec, P()), out_specs=(field_spec, P()), check_vma=False)
```

```python
import jax
import jax.numpy as jnp
from jax import lax
from jax.experimental import pallas as pl
from jax.experimental.pallas import tpu as pltpu
from jax.sharding import PartitionSpec as P

ITERS = 8
MESH = pl.DeviceIdType.MESH
F32 = jnp.float32
TL, ZL, YL, XH = 6, 6, 48, 10
R0 = 16
ROWS, LANES, HALF, VALID = 32, 128, 64, 30
XL = 5
NSTG = 6
COMPS, LINKS = range(6), range(18)
C0 = 3
STEPS = ((0, 1), (1, 3))
SITE = VALID * 2 * 6
ORDER = 'z3z4z5t1y1t4y4z0z1x1x4t0y0t2y2t3y3t5y5x0x2z2x3x5'
FIRST_STEP = 'aadhlpptwwyy'
LOADS = 4 * ZL
PITCH, QUAD = 76, 72
BLK = 16
BLOCKS = range(0, ROWS, BLK)


def packed(values):
    return [sum(v << 5 * q for q, v in enumerate(values[w:w + 6])) for w in range(0, len(values), 6)]


def pick(words, q):
    word = words[-1]
    for w, value in enumerate(words[:-1]):
        word = jnp.where(q // 6 == w, value, word)
    return (word >> 5 * lax.rem(q, 6)) & 31


STEP_WORDS = packed(['tzyx'.index(ORDER[q]) * 8 + int(ORDER[q + 1]) for q in range(0, 2 * LOADS, 2)])
PHASE_WORDS = packed([ord(q) - ord('a') for q in FIRST_STEP])


def loop(first, last, act):
    def body(q, carry):
        act(q)
        return carry
    lax.fori_loop(first, last, body, 0)


def vec(*shape):
    return pltpu.VMEM(shape + (LANES,), F32)


def plane():
    return vec(ZL, 6, ROWS)


def sems(*shape):
    return pltpu.SemaphoreType.DMA(shape)


def halo_t():
    return vec(2, ZL, 6, R0)


def wires():
    return vec(2, 6, 136)


def halo_y():
    return vec(2, ZL, BLK)


SCRATCH = dict(
    lkt=vec(24, 18, 56), lko=vec(72, 18, ROWS), stg=pltpu.VMEM((2 * NSTG, ROWS * PITCH, YL), F32), sst=pltpu.VMEM((2304, YL), F32),
    f=vec(18, 6, 64), acc=plane(), cb=vec(2, 6, ROWS), xs=vec(2, 6, YL),
    r=plane(), p=plane(), s=plane(), z=plane(), x=plane(), zs=wires(), zr=wires(),
    tsf=halo_t(), trf=halo_t(), tsc=halo_t(), trc=halo_t(), ysf=halo_y(), yrf=halo_y(), ysc=halo_y(), yrc=halo_y(),
    ra=vec(2, 32), gd=vec(7, 8), cf=vec(8, 8),
    stg_sem=sems(NSTG, 2), io_sem=sems(ZL), z_ss=sems(2), z_rs=sems(2, 6), h_ss=sems(2, 4), h_rs=sems(2, 3, 4),
    a_ss=sems(2, 2), a_rs=sems(2, 2),
)


def terms(link, psi):
    for i in range(3):
        for j in range(3):
            at = 2 * (3 * i + j)
            yield i, j, link(at), link(at + 1), psi


def mat(acc, link, psi):
    for i, j, a, b, v in terms(link, psi):
        c, d = v[2 * j:2 * j + 2]
        acc[2 * i] = acc[2 * i] + (a * c - b * d)
        acc[2 * i + 1] = acc[2 * i + 1] + (a * d + b * c)


def adj(acc, link, psi):
    for j, i, a, b, v in terms(link, psi):
        c, d = v[2 * j:2 * j + 2]
        acc[2 * i] = acc[2 * i] - (a * c + b * d)
        acc[2 * i + 1] = acc[2 * i + 1] + (b * c - a * d)


def fold(v):
    return sum(v[first:first + 8] for first in range(0, len(v), 8))


def rot(v, n):
    n %= LANES
    return pltpu.roll(v, n, 1) if n else v


def kernel(fat, lng, src, mass, out, res, *scratch):
    k = type('Refs', (), {})()
    for name, ref in zip(SCRATCH, scratch):
        setattr(k, name, ref)
    iy, iz, it = lax.axis_index('yy'), lax.axis_index('zz'), lax.axis_index('t')

    def at_t(d):
        return (iy, iz, lax.rem(it + d, 4))

    def at_z():
        return (iy, 1 - iz, it)

    def at_y(d):
        return (lax.rem(iy + d, 4), iz, it)

    def remote(src_ref, dst_ref, send, recv, dev):
        return pltpu.make_async_remote_copy(src_ref=src_ref, dst_ref=dst_ref, send_sem=send, recv_sem=recv, device_id=dev, device_id_type=MESH)

    def other(d):
        return (iy + d // 8) & 3, (iz + d // 4) & 1, (it + d) & 3

    everyone = [other(d) for d in range(1, ROWS)]
    slab = [((iy + d // 4) & 3, iz, (it + d) & 3) for d in range(1, R0)]

    def plane_of(t, n2):
        first = jnp.where(t == 0, 1, jnp.where(t == 1, 0, 3))
        return first + n2 * jnp.where(t == 0, 3, 2)

    def what(g):
        code = pick(STEP_WORDS, g)
        return code // 8, code & 7

    def stg_copies(g):
        slot = lax.rem(g, NSTG)
        di, zi = what(g)

        def to(n):
            return k.stg.at[2 * slot + n, pl.ds(0, VALID * PITCH)].reshape(TL, XL, PITCH, YL).at[:, :, pl.ds(0, QUAD)]
        return [pltpu.make_async_copy(ref.at[di, :, zi], to(n), k.stg_sem.at[slot, n]) for n, ref in enumerate((fat, lng))]

    def src_copy(zi):
        return pltpu.make_async_copy(src.at[:, pl.ds(60 * zi, 60)], k.sst.at[pl.ds(SITE * zi, SITE)].reshape(TL, 60, YL), k.io_sem.at[zi])

    for zi in range(ZL):
        src_copy(zi).start()
    for g in range(NSTG):
        for cp in stg_copies(jnp.int32(g)):
            cp.start()
    barrier = pltpu.get_barrier_semaphore()
    loop(1, ROWS, lambda d: pl.semaphore_signal(barrier, device_id=other(d), device_id_type=MESH))

    lane8, row8 = (lax.broadcasted_iota(jnp.int32, (8, LANES), d) for d in (1, 0))
    ylane8 = lane8 % HALF
    lane, row = (lax.broadcasted_iota(jnp.int32, (ROWS, LANES), d) for d in (1, 0))
    lane_b, row_b = lane[:BLK], row[:BLK]
    ylane = lane_b % HALF
    seg0 = lane_b < HALF
    zero8 = jnp.zeros((8, LANES), F32)
    zeros = jnp.zeros((BLK, LANES), F32)

    def lt(n, o, zi):
        return (n * 2 + o) * ZL + zi

    def lo(di, n, o, zi):
        return (((di - 1) * 2 + n) * 2 + o) * ZL + zi

    def at(h, off=0):
        return pl.ds(off + h, BLK)

    def psi_of(i, j, h, off=0):
        return [k.f[9 * i + j, c, at(h, R0 + off), :] for c in COMPS]

    k.f[...] = jnp.zeros_like(k.f)
    for ref in (k.p, k.s, k.z, k.x, k.gd):
        ref[...] = jnp.zeros_like(ref)
    k.lkt[:, :, 0:R0, :] = jnp.zeros((24, 18, R0, LANES), F32)
    k.lkt[:, :, R0 + ROWS:, :] = jnp.zeros((24, 18, 8, LANES), F32)

    k.stg[:, VALID * PITCH:, :] = jnp.zeros((2 * NSTG, 2 * PITCH, YL), F32)
    def whole(half):
        rest = jnp.zeros((ROWS, LANES - YL), F32)
        first, second = (jnp.concatenate([v, rest], axis=1) for v in half)
        return first + rot(second, HALF)

    def src_plane(zi):
        for c in COMPS:
            v = jnp.where(row < VALID, whole([k.sst[pl.ds(zi * SITE + 6 * s + c, ROWS, 12), :] for s in range(2)]), 0.0)
            k.f[zi, c, pl.ds(R0, ROWS), :] = v
            k.r[zi, c] = v

    def convert(g, zi, ref, base, lead):
        slot = lax.rem(g, NSTG)
        even = ((row // XL + lane + zi) & 1) == 0
        for n in range(2):
            for c in LINKS:
                v = [whole([k.stg[2 * slot + n, pl.ds(c + (2 * s + h) * 18, ROWS, PITCH), :] for s in range(2)]) for h in range(2)]
                for o in range(2):
                    ref[lead(n, o, zi), c, pl.ds(base, ROWS), :] = jnp.where(even, v[o], v[1 - o])

    def load_step(g):
        di, zi = what(g)
        for cp in stg_copies(g):
            cp.wait()

        @pl.when(di == 0)
        def _():
            convert(g, zi, k.lkt, R0, lt)

        @pl.when(di > 0)
        def _():
            convert(g, zi, k.lko, 0, lambda n, o, zi: lo(di, n, o, zi))

        @pl.when(g + NSTG < LOADS)
        def _():
            for cp in stg_copies(g + NSTG):
                cp.start()

    def z_copy(i, m):
        return remote(k.zs.at[i, m, used], k.zr.at[i, m, used], k.z_ss.at[i], k.z_rs.at[i, m], at_z())

    def h_copies(i, t, whole=False):
        pairs = ((k.tsf, k.trf, at_t(3)), (k.tsc, k.trc, at_t(1)), (k.ysf, k.yrf, at_y(3)), (k.ysc, k.yrc, at_y(1)))
        some = pl.ds(0, ZL) if whole else pl.ds(2 * t, 2)
        return [remote(a.at[i, some], b.at[i, some], k.h_ss.at[i, n], k.h_rs.at[i, t, n], dev) for n, (a, b, dev) in enumerate(pairs)]

    def sent(i):
        remote(k.zs.at[i, :, used], k.zr.at[i, :, used], k.z_ss.at[i], k.z_rs.at[i, 0], at_z()).wait_send()
        for cp in h_copies(i, 0, True):
            cp.wait_send()

    gap = ylane8 >= YL
    used = pl.ds(0, 135)

    def rows_of(u, part, off=0):
        return pl.ds(off + 15 * (u % 2) + part, 8)

    def wire(host, part):
        return pl.ds(15 * host + part, 8)

    def pack(load, i, m):
        for u in range(3):
            for part in (0, 7):
                guest = load(9 + u, part)
                for q in range(3):
                    k.zs[i, m, wire(3 * q + u, part), :] = jnp.where(gap, rot(guest, YL - R0 * q), load(3 * q + u, part))

    def unpack(i, m, store):
        for u in range(3):
            for part in (0, 7):
                guest = zero8
                for q in range(3):
                    h = k.zr[i, m, wire(3 * q + u, part), :]
                    store(3 * q + u, part, jnp.where(gap, 0.0, h))
                    guest = jnp.where(ylane8 // R0 == q, rot(h, R0 * q - YL), guest)
                store(9 + u, part, guest)

    def start(i, *ms):
        for m in ms:
            z_copy(i, m).start()

    def arrive(i, *ms):
        for m in ms:
            z_copy(i, m).wait_recv()

    def pack_psi(i, m):
        pack(lambda u, part: k.f[9 * i + m, u // 2, rows_of(u, part, R0), :], i, m)

    def pack_c(i, m, b, *terms):
        acc = [jnp.zeros((ROWS, LANES), F32)] * 6
        for n, j in terms:
            adj(acc, lambda c: k.lko[lo(1, n, i, j), c], [k.f[9 * i + j, c, pl.ds(R0, ROWS), :] for c in COMPS])
        for c in COMPS:
            k.cb[b, c] = acc[c]
        pack(lambda u, part: k.cb[b, u // 2, rows_of(u, part), :], i, C0 + m)

    def fresh(v, part):
        return jnp.where(row8 == 0, 0.0, v) if part else v

    def unpack_psi(i, m):
        def store(u, part, v):
            k.f[9 * i + 6 + m, u // 2, rows_of(u, part, R0), :] = v
        unpack(i, m, store)

    def unpack_c(i, m):
        def store(u, part, v):
            sl = (m, u // 2, rows_of(u, part), slice(None))
            k.acc[sl] = k.acc[sl] + fresh(v, part)
        unpack(i, C0 + m, store)

    def correct(m):
        aw = k.cf[1]

        def store(u, part, v):
            sl = (m, u // 2, rows_of(u, part, R0), slice(None))
            k.f[sl] = k.f[sl] + aw * fresh(v, part)
        unpack(1, C0 + m, store)

    def send(i, t):
        @pl.when(t == 0)
        def _():
            pack_psi(i, 1)
            pack_c(i, 1, 0, (1, 4))
            start(i, 1, C0 + 1)

        @pl.when(t == 1)
        def _():
            pack_psi(i, 0)
            pack_psi(i, 2)
            start(i, 0, 2)

        @pl.when(t == 2)
        def _():
            pack_c(i, 0, 0, (0, 5), (1, 3))
            pack_c(i, 2, 1, (1, 5))
            start(i, C0, C0 + 2)

    def receive(i, t):
        @pl.when(t == 0)
        def _():
            arrive(i, 1, C0 + 1)
            unpack_psi(i, 1)
            unpack_c(i, 1)

        @pl.when(t == 1)
        def _():
            arrive(i, C0, C0 + 2)
            unpack_c(i, 0)
            unpack_c(i, 2)

        @pl.when(t == 2)
        def _():
            arrive(i, 0, 2)
            unpack_psi(i, 0)
            unpack_psi(i, 2)

    def tell(i, t):
        def one_plane(n2):
            j = plane_of(t, n2)
            slot = 2 * t + n2
            fwd, bwd = zeros, zeros
            for h in BLOCKS:
                psi = psi_of(i, j, h)
                back = [zeros] * 6
                for n, off in STEPS:
                    chi = [zeros] * 6
                    adj(chi, lambda c: k.lko[lo(2, n, i, j), c, at(h), :], psi)
                    back = [back[c] + rot(chi[c], off) for c in COMPS]
                for c in COMPS:
                    k.acc[j, c, at(h), :] = back[c]
                    to = 4 * c + 24 * (h // BLK)
                    here = ylane // 4 == to // 4
                    fwd = jnp.where(here, rot(psi[c], to), fwd)
                    bwd = jnp.where(here, rot(back[c], to - YL), bwd)
            k.ysf[i, slot] = fwd
            k.ysc[i, slot] = bwd
            for h in range(2):
                acc = [zero8] * 6
                for n, first in ((0, R0 + 25), (1, R0 + 15 + 8 * h)):
                    if n or not h:
                        adj(acc, lambda c: k.lkt[lt(n, i, j), c, pl.ds(first, 8), :], [k.f[9 * i + j, c, pl.ds(first, 8), :] for c in COMPS])
                for c in COMPS:
                    k.tsc[i, slot, c, pl.ds(8 * h, 8), :] = acc[c]
                    k.tsf[i, slot, c, pl.ds(8 * h, 8), :] = k.f[9 * i + j, c, pl.ds(R0 + 8 * h, 8), :]

        loop(0, 2, one_plane)
        for cp in h_copies(i, t):
            cp.start()

    def post(i, t):
        o = 1 - i

        def one_plane(n2):
            j = plane_of(t, n2)
            for h in BLOCKS:
                psi = psi_of(i, j, h)
                for n, _ in STEPS:
                    chi = [zeros] * 6
                    adj(chi, lambda c: k.lko[lo(3, n, i, j), c, at(h), :], psi)
                    for c in COMPS:
                        k.xs[n, c, at(h, 8), :] = chi[c]
            for h in BLOCKS:
                x5 = lax.rem(row_b + h, XL)
                e = (((row_b + h) // XL + lane_b + (j + o)) & 1) == 1
                acc = [k.acc[j, c, at(h), :] for c in COMPS]
                for n, _ in STEPS:
                    for c in COMPS:
                        own = k.xs[n, c, at(h, 8), :]
                        far = jnp.where(x5 > 0, k.xs[n, c, at(h, 7), :], k.xs[n, c, at(h, 12), :])
                        close = rot(jnp.where(seg0, own, far), HALF)
                        acc[c] = acc[c] + (jnp.where(e, close, far) if n else jnp.where(e, own, close))
                for n, off in STEPS:
                    off *= XL
                    adj(acc, lambda c: k.lkt[lt(n, i, j), c, at(h, R0 - off), :], psi_of(i, j, h, -off))
                psi = psi_of(i, j, h)
                far = [jnp.where(x5 < 4, u, v) for u, v in zip(psi_of(i, j, h, 1), psi_of(i, j, h, -4))]
                close = [rot(jnp.where(seg0, far[c], psi[c]), HALF) for c in COMPS]
                mat(acc, lambda c: k.lko[lo(3, 0, o, j), c, at(h), :], [jnp.where(e, close[c], psi[c]) for c in COMPS])
                mat(acc, lambda c: k.lko[lo(3, 1, o, j), c, at(h), :], [jnp.where(e, far[c], close[c]) for c in COMPS])
                for c in COMPS:
                    k.acc[j, c, at(h), :] = acc[c]

        loop(0, 2, one_plane)

    m2 = mass[0] * mass[0]

    def store_odd(j, h, real, acc):
        for c in COMPS:
            k.f[9 + j, c, at(h, R0), :] = acc[c]

    def update_even(j, h, real, acc):
        cw, aw, ax, beta = (jnp.broadcast_to(k.cf[v, 0:1], (BLK, LANES)) for v in range(4))
        gg, dd = zeros, zeros
        for c in COMPS:
            sl, fl = (j, c, at(h), slice(None)), (j, c, at(h, R0), slice(None))
            w = jnp.where(real, k.f[fl], 0.0)
            n = m2 * w - acc[c]
            zv = n + beta * k.z[sl]
            sv = w + beta * k.s[sl]
            r = k.r[sl]
            pv = r + beta * k.p[sl]
            k.x[sl] = k.x[sl] + ax * pv
            r = r - ax * sv
            w = cw * w - aw * zv
            k.z[sl], k.s[sl], k.p[sl], k.r[sl], k.f[fl] = zv, sv, pv, r, w
            gg = gg + r * r
            dd = dd + w * r
        for v, t in enumerate((gg, dd)):
            k.gd[v] = k.gd[v] + fold(t)

    def finish(i, t, update):
        o = 1 - i
        for cp in h_copies(i, t):
            cp.wait_recv()

        def one_plane(n2):
            j = plane_of(t, n2)
            slot = 2 * t + n2
            for c in COMPS:
                k.f[9 * i + j, c, pl.ds(R0 + VALID, R0), :] = k.trf[i, slot, c]
            yf, yc = k.yrf[i, slot], k.yrc[i, slot]
            for h in BLOCKS:
                frm = [4 * c + 24 * (h // BLK) for c in COMPS]
                top = (ylane >= YL) & (ylane < YL + 3)
                psi = [jnp.where(top, rot(yf, YL - frm[c]), v) for c, v in enumerate(psi_of(i, j, h))]
                acc = [k.acc[j, c, at(h), :] + jnp.where(ylane < 3, rot(yc, -frm[c]), 0.0) for c in COMPS]
                if h == 0:
                    acc = [acc[c] + k.trc[i, slot, c] for c in COMPS]
                for n, off in STEPS:
                    mat(acc, lambda c: k.lkt[lt(n, o, j), c, at(h, R0), :], psi_of(i, j, h, XL * off))
                for n, off in STEPS:
                    mat(acc, lambda c: k.lko[lo(1, n, o, j), c, at(h), :], psi_of(i, j + off, h))
                    jb, on = jnp.maximum(j - off, 0), jnp.where(j >= off, 1.0, 0.0)
                    adj(acc, lambda c: k.lko[lo(1, n, i, jb), c, at(h), :], [on * v for v in psi_of(i, jb, h)])
                for n, off in STEPS:
                    mat(acc, lambda c: k.lko[lo(2, n, o, j), c, at(h), :], [rot(psi[c], -off) for c in COMPS])
                real = row_b + h < VALID
                good = real & (ylane < YL)
                update(j, h, real, [jnp.where(good, acc[c], 0.0) for c in COMPS])

        loop(0, 2, one_plane)

    def a_copy(b, stage, first, rows, dev):
        here = k.ra.at[b, pl.ds(first, rows)]
        return remote(here, here, k.a_ss.at[b, stage], k.a_rs.at[b, stage], dev)

    def sum_start(b, n, stage, me, to):
        mine = zeros[:1]
        for v in range(n):
            total = jnp.sum(jnp.sum(k.gd[v], axis=0, keepdims=True), axis=1, keepdims=True)
            mine = jnp.where(lane[:1] == v, total, mine)
        k.ra[b, pl.ds(me, 1), :] = mine
        for dev in to:
            a_copy(b, stage, me, 1, dev).start()

    def sum_next(b):
        a_copy(b, 0, 0, 1, at_z()).wait()
        me = R0 + 4 * iy + it
        k.ra[b, pl.ds(me, 1), :] = k.ra[b, 0:1, :] + k.ra[b, 1:2, :]
        for dev in slab:
            a_copy(b, 1, me, 1, dev).start()

    def sum_end(b, n, to, first):
        a_copy(b, 1, first, len(to), at_z()).wait()
        tile = jnp.sum(k.ra[b, first:], axis=0, keepdims=True)
        return [jnp.broadcast_to(tile[:, v:v + 1], (8, LANES)) for v in range(n)]

    def dots(q):
        j = plane_of(jnp.where(q < 2, 0, jnp.where(q < 4, 2, 1)), lax.rem(q, 2))
        sums = [jnp.zeros((ROWS, LANES), F32)] * 5
        for c in COMPS:
            w, r, s = k.f[j, c, pl.ds(R0, ROWS), :], k.r[j, c], k.s[j, c]
            sums = [t + u * v for t, (u, v) in zip(sums, ((w, r), (w, w), (r, s), (w, s), (s, s)))]
        for v, t in enumerate(sums):
            k.gd[2 + v] = k.gd[2 + v] + fold(t)

    CW, AW, AX, BETA, GAMMA, ALPHA, FIRST = range(7)
    one = jnp.ones((8, LANES), F32)
    for v, t in ((CW, zero8), (AW, -one), (AX, zero8), (BETA, zero8), (GAMMA, one), (ALPHA, one)):
        k.cf[v] = t

    def scalars(step, gamma, delta):
        @pl.when(step == 1)
        def _():
            k.cf[ALPHA] = gamma / delta
            k.cf[FIRST] = gamma

        @pl.when(step > 1)
        def _():
            beta = gamma / k.cf[GAMMA]
            k.cf[BETA] = beta
            k.cf[ALPHA] = gamma / (delta - beta * gamma / k.cf[ALPHA])
            res[step - 2] = (gamma / k.cf[FIRST])[0, 0]
        k.cf[CW], k.cf[AW], k.cf[AX], k.cf[GAMMA] = one, k.cf[ALPHA], k.cf[ALPHA], gamma

    def phase(u):
        begin = (u < 5) | (u == 6) | (u == 7) | (u == 9)
        v = jnp.where(u > 9, u - 8, jnp.where(u > 6, 1, 0))
        n, ph = v // 3, lax.rem(v, 3)
        i = lax.rem(n, 2)
        even, odd, starts, ends = i == 0, i == 1, ph == 0, ph == 2
        step = n // 2
        b = lax.rem(step, 2)
        t = jnp.where(starts, 0, jnp.where((ph == 1) == even, 1, 2))
        live = jnp.logical_not(begin)
        more = n < 2 * ITERS - 1

        @pl.when(begin)
        def _():
            loop(pick(PHASE_WORDS, jnp.minimum(u, 10)), pick(PHASE_WORDS, jnp.minimum(u + 1, 10)), load_step)

        @pl.when(u == 0)
        def _():
            for zi in range(ZL):
                src_copy(zi).wait()
            loop(0, ZL, src_plane)
            pl.semaphore_wait(barrier, len(everyone))

        @pl.when(live & even & (ph == 1) & (step > 0))
        def _():
            sum_next(b)

        @pl.when(live & odd & starts)
        def _():
            @pl.when(step > 0)
            def _():
                scalars(step, *sum_end(b, 2, slab, R0))
            k.gd[0], k.gd[1] = zero8, zero8

        last = ends & jnp.logical_not(more)

        @pl.when(last)
        def _():
            loop(0, 4, dots)

        @pl.when(live & jnp.logical_not(last))
        def _():
            receive(i, t)

        @pl.when(live)
        def _():
            @pl.when(even)
            def _():
                finish(0, t, store_odd)

            @pl.when(odd)
            def _():
                finish(1, t, update_even)

        @pl.when(last)
        def _():
            arrive(1, C0, C0 + 2)
            loop(0, 2, lambda e: correct(2 * e))

        @pl.when(live & ends & odd & more)
        def _():
            sum_start(1 - b, 2, 0, iz, [at_z()])

        o = jnp.where(begin, 0, 1 - i)

        loop(0, jnp.where(begin, jnp.where(u < 2, u + 1, 0), more.astype(jnp.int32)), lambda e: send(o, jnp.where(begin, jnp.where(u == 0, 1, 2 * e), t)))

        tells = jnp.where(begin, (u == 2) | (u == 4) | (u == 6), more).astype(jnp.int32)
        tells = jnp.where(live & (n == 0), jnp.where(starts, 1, 2 * ends.astype(jnp.int32)), tells)
        loop(0, tells, lambda e: tell(o, jnp.where(begin, u // 2 - 1, t - e)))

        @pl.when(jnp.where(begin, (u == 3) | (u == 7) | (u == 9), jnp.where(ends, more, n > 0)))
        def _():
            post(jnp.where(begin | ends, o, i), jnp.where(begin, u // 3 - 1, jnp.where(ends, 0, jnp.where(starts == even, 1, 2))))

        @pl.when(live & ends)
        def _():
            sent(i)

    loop(0, 8 + 3 * 2 * ITERS, phase)

    loop(4, ZL, dots)
    sum_start(0, 7, 1, 8 * iy + 4 * iz + it, everyone)
    parts = (k.sst, k.stg.at[0], k.stg.at[1])

    def out_plane(j):
        for to, frm in zip(parts, (k.x, k.r, k.p)):
            for c in COMPS:
                for s in range(2):
                    to[pl.ds(j * SITE + 6 * s + c, VALID, 12), :] = rot(frm[j, c], HALF * s)[0:VALID, 0:YL]

    loop(0, ZL, out_plane)
    rr, _, wr, ww, rs, ws, ss = sum_end(0, 7, everyone, 0)
    beta = rr / k.cf[GAMMA]
    alpha = rr / (wr - beta * rr / k.cf[ALPHA])
    last = rr - 2.0 * alpha * (wr + beta * rs) + alpha * alpha * (ww + 2.0 * beta * ws + beta * beta * ss)
    for v, t in ((ITERS - 2, rr), (ITERS - 1, last)):
        res[v] = (t / k.cf[FIRST])[0, 0]
    alpha, beta = (jnp.broadcast_to(v[0:1, 0:YL], (SITE, YL)) for v in (alpha, beta))

    def out_rows(j):
        here = pl.ds(j * SITE, SITE)
        x, r, p = (ref[here, :] for ref in parts)
        v = x + alpha * (r + beta * p)
        for t in range(TL):
            out[t, pl.ds(j * 60, 60), :] = v[60 * t:60 * (t + 1)]

    loop(0, ZL, out_rows)


def solution(mesh):
    link_spec = P(None, 't', 'zz', 'yy')
    field_spec = P('t', 'zz', 'yy')

    def local_solve(fat_links, long_links, source, quark_mass):
        fat, lng = (jnp.moveaxis(v, 3, -1).reshape(4, TL, ZL, XL, QUAD, YL) for v in (fat_links, long_links))
        src = jnp.moveaxis(source, 2, -1).reshape(TL, SITE, YL)
        anywhere, local, scalar = (pl.BlockSpec(memory_space=space) for space in (pl.ANY, pltpu.VMEM, pltpu.SMEM))
        sol, res = pl.pallas_call(
            kernel,
            out_shape=(pltpu.VMEM((TL, SITE, YL), F32), pltpu.SMEM((8,), F32)),
            in_specs=[anywhere] * 3 + [scalar],
            out_specs=(local, scalar),
            scratch_shapes=list(SCRATCH.values()),
            compiler_params=pltpu.CompilerParams(collective_id=0, has_side_effects=True, vmem_limit_bytes=65000000),
            name='cg',
        )(fat, lng, src, quark_mass)
        return jnp.moveaxis(sol.reshape(TL, ZL, XH, 3, 2, YL), -1, 2), res

    return jax.shard_map(local_solve, mesh=mesh, in_specs=(link_spec, link_spec, field_spec, P()), out_specs=(field_spec, P()), check_vma=False)
```

```python
import jax
import jax.numpy as jnp
from jax import lax
from jax.experimental import pallas as pl
from jax.experimental.pallas import tpu as pltpu
from jax.sharding import PartitionSpec as P

ITERS = 8
MESH = pl.DeviceIdType.MESH
F32 = jnp.float32
TL, ZL, YL, XH = 6, 6, 48, 10
R0 = 16
ROWS, LANES, HALF, VALID = 32, 128, 64, 30
XL = 5
NSTG = 6
COMPS, LINKS = range(6), range(18)
C0 = 3
STEPS = ((0, 1), (1, 3))
SITE = VALID * 2 * 6
ORDER = 'z3z4z5t1y1t4y4z0z1x1x4t0y0t2y2t3y3t5y5x0x2z2x3x5'
FIRST_STEP = 'aadhlpptwwyy'
LOADS = 4 * ZL
PITCH, QUAD = 76, 72
BLK = 16
BLOCKS = range(0, ROWS, BLK)


def packed(values):
    return [sum(v << 5 * q for q, v in enumerate(values[w:w + 6])) for w in range(0, len(values), 6)]


def pick(words, q):
    word = words[-1]
    for w, value in enumerate(words[:-1]):
        word = jnp.where(q // 6 == w, value, word)
    return (word >> 5 * lax.rem(q, 6)) & 31


STEP_WORDS = packed(['tzyx'.index(ORDER[q]) * 8 + int(ORDER[q + 1]) for q in range(0, 2 * LOADS, 2)])
PHASE_WORDS = packed([ord(q) - ord('a') for q in FIRST_STEP])


def loop(first, last, act):
    def body(q, carry):
        act(q)
        return carry
    lax.fori_loop(first, last, body, 0)


def vec(*shape):
    return pltpu.VMEM(shape + (LANES,), F32)


def plane():
    return vec(ZL, 6, ROWS)


def sems(*shape):
    return pltpu.SemaphoreType.DMA(shape)


def halo_t():
    return vec(2, ZL, 6, R0)


def wires():
    return vec(2, 6, 136)


def halo_y():
    return vec(2, ZL, BLK)


SCRATCH = dict(
    lkt=vec(24, 18, 56), lko=vec(72, 18, ROWS), stg=pltpu.VMEM((2 * NSTG, ROWS * PITCH, YL), F32), sst=pltpu.VMEM((2304, YL), F32),
    f=vec(18, 6, 64), acc=plane(), cb=vec(2, 6, ROWS), xs=vec(2, 6, YL),
    r=plane(), p=plane(), s=plane(), z=plane(), x=plane(), zs=wires(), zr=wires(),
    tsf=halo_t(), trf=halo_t(), tsc=halo_t(), trc=halo_t(), ysf=halo_y(), yrf=halo_y(), ysc=halo_y(), yrc=halo_y(),
    ra=vec(2, 32), gd=vec(7, 8), cf=vec(8, 8),
    stg_sem=sems(NSTG), io_sem=sems(1), z_ss=sems(2), z_rs=sems(2, 3), h_ss=sems(2, 2), h_rs=sems(2, 3, 2),
    a_ss=sems(2, 2), a_rs=sems(2, 2),
)


def terms(link, psi):
    for i in range(3):
        for j in range(3):
            at = 2 * (3 * i + j)
            yield i, j, link(at), link(at + 1), psi


def mat(acc, link, psi):
    for i, j, a, b, v in terms(link, psi):
        c, d = v[2 * j:2 * j + 2]
        acc[2 * i] = acc[2 * i] + (a * c - b * d)
        acc[2 * i + 1] = acc[2 * i + 1] + (a * d + b * c)


def adj(acc, link, psi):
    for j, i, a, b, v in terms(link, psi):
        c, d = v[2 * j:2 * j + 2]
        acc[2 * i] = acc[2 * i] - (a * c + b * d)
        acc[2 * i + 1] = acc[2 * i + 1] + (b * c - a * d)


def fold(v):
    return sum(v[first:first + 8] for first in range(0, len(v), 8))


def rot(v, n):
    n %= LANES
    return pltpu.roll(v, n, 1) if n else v


def kernel(fat, lng, src, mass, out, res, *scratch):
    k = type('Refs', (), {})()
    for name, ref in zip(SCRATCH, scratch):
        setattr(k, name, ref)
    iy, iz, it = lax.axis_index('yy'), lax.axis_index('zz'), lax.axis_index('t')

    def at_t(d):
        return (iy, iz, lax.rem(it + d, 4))

    def at_z():
        return (iy, 1 - iz, it)

    def at_y(d):
        return (lax.rem(iy + d, 4), iz, it)

    def remote(src_ref, dst_ref, send, recv, dev):
        return pltpu.make_async_remote_copy(src_ref=src_ref, dst_ref=dst_ref, send_sem=send, recv_sem=recv, device_id=dev, device_id_type=MESH)

    def other(d):
        return (iy + d // 8) & 3, (iz + d // 4) & 1, (it + d) & 3

    everyone = [other(d) for d in range(1, ROWS)]
    slab = [((iy + d // 4) & 3, iz, (it + d) & 3) for d in range(1, R0)]

    def plane_of(t, n2):
        first = jnp.where(t == 0, 1, jnp.where(t == 1, 0, 3))
        return first + n2 * jnp.where(t == 0, 3, 2)

    def what(g):
        code = pick(STEP_WORDS, g)
        return code // 8, code & 7

    def stg_copies(g):
        slot = lax.rem(g, NSTG)
        di, zi = what(g)

        def to(n):
            return k.stg.at[2 * slot + n, pl.ds(0, VALID * PITCH)].reshape(TL, XL, PITCH, YL).at[:, :, pl.ds(0, QUAD)]
        return [pltpu.make_async_copy(ref.at[di, :, zi], to(n), k.stg_sem.at[slot]) for n, ref in enumerate((fat, lng))]

    def src_copy(zi):
        return pltpu.make_async_copy(src.at[:, pl.ds(60 * zi, 60)], k.sst.at[pl.ds(SITE * zi, SITE)].reshape(TL, 60, YL), k.io_sem.at[0])

    for zi in range(ZL):
        src_copy(zi).start()
    for g in range(NSTG):
        for cp in stg_copies(jnp.int32(g)):
            cp.start()
    barrier = pltpu.get_barrier_semaphore()
    loop(1, ROWS, lambda d: pl.semaphore_signal(barrier, device_id=other(d), device_id_type=MESH))

    lane8, row8 = (lax.broadcasted_iota(jnp.int32, (8, LANES), d) for d in (1, 0))
    ylane8 = lane8 % HALF
    lane, row = (lax.broadcasted_iota(jnp.int32, (ROWS, LANES), d) for d in (1, 0))
    lane_b, row_b = lane[:BLK], row[:BLK]
    ylane = lane_b % HALF
    seg0 = lane_b < HALF
    zero8 = jnp.zeros((8, LANES), F32)
    zeros = jnp.zeros((BLK, LANES), F32)

    def lt(n, o, zi):
        return (n * 2 + o) * ZL + zi

    def lo(di, n, o, zi):
        return (((di - 1) * 2 + n) * 2 + o) * ZL + zi

    def at(h, off=0):
        return pl.ds(off + h, BLK)

    def psi_of(i, j, h, off=0):
        return [k.f[9 * i + j, c, at(h, R0 + off), :] for c in COMPS]

    k.f[...] = jnp.zeros_like(k.f)
    for ref in (k.p, k.s, k.z, k.x, k.gd):
        ref[...] = jnp.zeros_like(ref)
    k.lkt[:, :, 0:R0, :] = jnp.zeros((24, 18, R0, LANES), F32)
    k.lkt[:, :, R0 + ROWS:, :] = jnp.zeros((24, 18, 8, LANES), F32)

    k.stg[:, VALID * PITCH:, :] = jnp.zeros((2 * NSTG, 2 * PITCH, YL), F32)
    def whole(half):
        rest = jnp.zeros((ROWS, LANES - YL), F32)
        first, second = (jnp.concatenate([v, rest], axis=1) for v in half)
        return first + rot(second, HALF)

    def src_plane(zi):
        for c in COMPS:
            v = jnp.where(row < VALID, whole([k.sst[pl.ds(zi * SITE + 6 * s + c, ROWS, 12), :] for s in range(2)]), 0.0)
            k.f[zi, c, pl.ds(R0, ROWS), :] = v
            k.r[zi, c] = v

    def convert(g, zi, ref, base, lead):
        slot = lax.rem(g, NSTG)
        even = ((row // XL + lane + zi) & 1) == 0
        for n in range(2):
            for c in LINKS:
                v = [whole([k.stg[2 * slot + n, pl.ds(c + (2 * s + h) * 18, ROWS, PITCH), :] for s in range(2)]) for h in range(2)]
                for o in range(2):
                    ref[lead(n, o, zi), c, pl.ds(base, ROWS), :] = jnp.where(even, v[o], v[1 - o])

    def load_step(g):
        di, zi = what(g)
        slots = pl.ds(2 * lax.rem(g, NSTG), 2)
        used_rows = slice(TL * SITE)
        pltpu.make_async_copy(k.stg.at[slots, used_rows], k.stg.at[slots, used_rows], k.stg_sem.at[lax.rem(g, NSTG)]).wait()

        @pl.when(di == 0)
        def _():
            convert(g, zi, k.lkt, R0, lt)

        @pl.when(di > 0)
        def _():
            convert(g, zi, k.lko, 0, lambda n, o, zi: lo(di, n, o, zi))

        @pl.when(g + NSTG < LOADS)
        def _():
            for cp in stg_copies(g + NSTG):
                cp.start()

    def z_copy(i, m, t):
        return remote(k.zs.at[i, m, used], k.zr.at[i, m, used], k.z_ss.at[i], k.z_rs.at[i, t], at_z())

    def h_copies(i, t):
        pairs = ((k.tsf, k.trf, at_t(3)), (k.tsc, k.trc, at_t(1)), (k.ysf, k.yrf, at_y(3)), (k.ysc, k.yrc, at_y(1)))
        two = pl.ds(2 * t, 2)
        return [remote(a.at[i, two], b.at[i, two], k.h_ss.at[i, n // 2], k.h_rs.at[i, t, n // 2], dev) for n, (a, b, dev) in enumerate(pairs)]

    def h_waits(i, t, *some):
        return [remote(a.at[some], b.at[some], k.h_ss.at[i, n], k.h_rs.at[i, t, n], at_t(1)) for n, (a, b) in enumerate(((k.tsf, k.trf), (k.ysf, k.yrf)))]

    def sent(i):
        remote(k.zs.at[i, :, used], k.zr.at[i, :, used], k.z_ss.at[i], k.z_rs.at[i, 0], at_z()).wait_send()
        for cp in h_waits(i, 0, slice(None)):
            cp.wait_send()

    gap = ylane8 >= YL
    used = slice(135)

    def rows_of(u, part, off=0):
        return pl.ds(off + 15 * (u % 2) + part, 8)

    def wire(host, part):
        return pl.ds(15 * host + part, 8)

    def pack(load, i, m):
        for u in range(3):
            for part in (0, 7):
                guest = load(9 + u, part)
                for q in range(3):
                    k.zs[i, m, wire(3 * q + u, part), :] = jnp.where(gap, rot(guest, YL - R0 * q), load(3 * q + u, part))

    def unpack(i, m, store):
        for u in range(3):
            for part in (0, 7):
                guest = zero8
                for q in range(3):
                    h = k.zr[i, m, wire(3 * q + u, part), :]
                    store(3 * q + u, part, jnp.where(gap, 0.0, h))
                    guest = jnp.where(ylane8 // R0 == q, rot(h, R0 * q - YL), guest)
                store(9 + u, part, guest)

    def start(i, m, t):
        z_copy(i, m, t).start()

    def arrive(i, t):
        z_copy(i, slice(2), t).wait_recv()

    def pack_psi(i, m):
        pack(lambda u, part: k.f[9 * i + m, u // 2, rows_of(u, part, R0), :], i, m)

    def pack_c(i, m, b, *terms):
        acc = [jnp.zeros((ROWS, LANES), F32)] * 6
        for n, j in terms:
            adj(acc, lambda c: k.lko[lo(1, n, i, j), c], [k.f[9 * i + j, c, pl.ds(R0, ROWS), :] for c in COMPS])
        for c in COMPS:
            k.cb[b, c] = acc[c]
        pack(lambda u, part: k.cb[b, u // 2, rows_of(u, part), :], i, C0 + m)

    def fresh(v, part):
        return jnp.where(row8 == 0, 0.0, v) if part else v

    def unpack_psi(i, m):
        def store(u, part, v):
            k.f[9 * i + 6 + m, u // 2, rows_of(u, part, R0), :] = v
        unpack(i, m, store)

    def unpack_c(i, m):
        def store(u, part, v):
            sl = (m, u // 2, rows_of(u, part), slice(None))
            k.acc[sl] = k.acc[sl] + fresh(v, part)
        unpack(i, C0 + m, store)

    def correct(m):
        aw = k.cf[1]

        def store(u, part, v):
            sl = (m, u // 2, rows_of(u, part, R0), slice(None))
            k.f[sl] = k.f[sl] + aw * fresh(v, part)
        unpack(1, C0 + m, store)

    def send(i, t):
        @pl.when(t == 0)
        def _():
            pack_psi(i, 1)
            start(i, 1, 0)
            pack_c(i, 1, 0, (1, 4))
            start(i, C0 + 1, 0)

        @pl.when(t == 1)
        def _():
            for m in (0, 2):
                pack_psi(i, m)
                start(i, m, 2)

        @pl.when(t == 2)
        def _():
            pack_c(i, 2, 1, (1, 5))
            start(i, C0 + 2, 1)
            pack_c(i, 0, 0, (0, 5), (1, 3))
            start(i, C0, 1)

    def receive(i, t):
        @pl.when(t == 0)
        def _():
            arrive(i, t)
            unpack_psi(i, 1)
            unpack_c(i, 1)

        @pl.when(t == 1)
        def _():
            arrive(i, t)
            unpack_c(i, 0)
            unpack_c(i, 2)

        @pl.when(t == 2)
        def _():
            arrive(i, t)
            unpack_psi(i, 0)
            unpack_psi(i, 2)

    def tell(i, t):
        def one_plane(n2):
            j = plane_of(t, n2)
            slot = 2 * t + n2
            fwd, bwd = zeros, zeros
            for h in BLOCKS:
                psi = psi_of(i, j, h)
                chis = []
                for n, off in STEPS:
                    chis.append([zeros] * 6)
                    adj(chis[n], lambda c: k.lko[lo(2, n, i, j), c, at(h), :], psi)
                for c in COMPS:
                    def back(by):
                        near, far = (rot(chis[n][c], off + by) for n, off in STEPS)
                        return near + far
                    k.acc[j, c, at(h), :] = back(0)
                    to = 4 * c + 24 * (h // BLK)
                    here = ylane // 4 == to // 4
                    fwd = jnp.where(here, rot(psi[c], to), fwd)
                    bwd = jnp.where(here, back(to - YL), bwd)
            k.ysf[i, slot] = fwd
            k.ysc[i, slot] = bwd
            for h in range(2):
                acc = [zero8] * 6
                for n, first in ((0, R0 + 25), (1, R0 + 15 + 8 * h)):
                    if n or not h:
                        adj(acc, lambda c: k.lkt[lt(n, i, j), c, pl.ds(first, 8), :], [k.f[9 * i + j, c, pl.ds(first, 8), :] for c in COMPS])
                for c in COMPS:
                    k.tsc[i, slot, c, pl.ds(8 * h, 8), :] = acc[c]
                    k.tsf[i, slot, c, pl.ds(8 * h, 8), :] = k.f[9 * i + j, c, pl.ds(R0 + 8 * h, 8), :]

        loop(0, 2, one_plane)
        for cp in h_copies(i, t):
            cp.start()

    def post(i, t):
        o = 1 - i

        def one_plane(n2):
            j = plane_of(t, n2)
            for h in BLOCKS:
                psi = psi_of(i, j, h)
                for n, _ in STEPS:
                    chi = [zeros] * 6
                    adj(chi, lambda c: k.lko[lo(3, n, i, j), c, at(h), :], psi)
                    for c in COMPS:
                        k.xs[n, c, at(h, 8), :] = chi[c]
            for h in BLOCKS:
                x5 = lax.rem(row_b + h, XL)
                e = (((row_b + h) // XL + lane_b + (j + o)) & 1) == 1
                acc = [k.acc[j, c, at(h), :] for c in COMPS]
                for n, _ in STEPS:
                    for c in COMPS:
                        own = k.xs[n, c, at(h, 8), :]
                        far = jnp.where(x5 > 0, k.xs[n, c, at(h, 7), :], k.xs[n, c, at(h, 12), :])
                        close = rot(jnp.where(seg0, own, far), HALF)
                        acc[c] = acc[c] + (jnp.where(e, close, far) if n else jnp.where(e, own, close))
                for n, off in STEPS:
                    off *= XL
                    adj(acc, lambda c: k.lkt[lt(n, i, j), c, at(h, R0 - off), :], psi_of(i, j, h, -off))
                psi = psi_of(i, j, h)
                far = [jnp.where(x5 < 4, u, v) for u, v in zip(psi_of(i, j, h, 1), psi_of(i, j, h, -4))]
                close = [rot(jnp.where(seg0, far[c], psi[c]), HALF) for c in COMPS]
                mat(acc, lambda c: k.lko[lo(3, 0, o, j), c, at(h), :], [jnp.where(e, close[c], psi[c]) for c in COMPS])
                mat(acc, lambda c: k.lko[lo(3, 1, o, j), c, at(h), :], [jnp.where(e, far[c], close[c]) for c in COMPS])
                for c in COMPS:
                    k.acc[j, c, at(h), :] = acc[c]

        loop(0, 2, one_plane)

    m2 = mass[0] * mass[0]

    def store_odd(j, h, real, acc):
        for c in COMPS:
            k.f[9 + j, c, at(h, R0), :] = acc[c]

    def update_even(j, h, real, acc):
        cw, aw, ax, beta = (jnp.broadcast_to(k.cf[v, 0:1], (BLK, LANES)) for v in range(4))
        gg, dd = zeros, zeros
        for c in COMPS:
            sl, fl = (j, c, at(h), slice(None)), (j, c, at(h, R0), slice(None))
            w = jnp.where(real, k.f[fl], 0.0)
            n = m2 * w - acc[c]
            zv = n + beta * k.z[sl]
            sv = w + beta * k.s[sl]
            r = k.r[sl]
            pv = r + beta * k.p[sl]
            k.x[sl] = k.x[sl] + ax * pv
            r = r - ax * sv
            w = cw * w - aw * zv
            k.z[sl], k.s[sl], k.p[sl], k.r[sl], k.f[fl] = zv, sv, pv, r, w
            gg = gg + r * r
            dd = dd + w * r
        for v, t in enumerate((gg, dd)):
            k.gd[v] = k.gd[v] + fold(t)

    def finish(i, t, update):
        o = 1 - i
        for cp in h_waits(i, t, i, slice(4)):
            cp.wait_recv()

        def one_plane(n2):
            j = plane_of(t, n2)
            slot = 2 * t + n2
            for c in COMPS:
                k.f[9 * i + j, c, pl.ds(R0 + VALID, R0), :] = k.trf[i, slot, c]
            yf, yc = k.yrf[i, slot], k.yrc[i, slot]
            for h in BLOCKS:
                frm = [4 * c + 24 * (h // BLK) for c in COMPS]
                top = (ylane >= YL) & (ylane < YL + 3)
                psi = [jnp.where(top, rot(yf, YL - frm[c]), v) for c, v in enumerate(psi_of(i, j, h))]
                acc = [k.acc[j, c, at(h), :] + jnp.where(ylane < 3, rot(yc, -frm[c]), 0.0) for c in COMPS]
                if h == 0:
                    acc = [acc[c] + k.trc[i, slot, c] for c in COMPS]
                for n, off in STEPS:
                    mat(acc, lambda c: k.lkt[lt(n, o, j), c, at(h, R0), :], psi_of(i, j, h, XL * off))
                for n, off in STEPS:
                    mat(acc, lambda c: k.lko[lo(1, n, o, j), c, at(h), :], psi_of(i, j + off, h))
                    jb, on = jnp.maximum(j - off, 0), jnp.where(j >= off, 1.0, 0.0)
                    adj(acc, lambda c: k.lko[lo(1, n, i, jb), c, at(h), :], [on * v for v in psi_of(i, jb, h)])
                for n, off in STEPS:
                    mat(acc, lambda c: k.lko[lo(2, n, o, j), c, at(h), :], [rot(psi[c], -off) for c in COMPS])
                real = row_b + h < VALID
                good = real & (ylane < YL)
                update(j, h, real, [jnp.where(good, acc[c], 0.0) for c in COMPS])

        loop(0, 2, one_plane)

    def a_copy(b, stage, first, rows, dev):
        here = k.ra.at[b, pl.ds(first, rows)]
        return remote(here, here, k.a_ss.at[b, stage], k.a_rs.at[b, stage], dev)

    def sum_start(b, n, stage, me, to):
        mine = zeros[:1]
        for v in range(n):
            total = jnp.sum(jnp.sum(k.gd[v], axis=0, keepdims=True), axis=1, keepdims=True)
            mine = jnp.where(lane[:1] == v, total, mine)
        k.ra[b, pl.ds(me, 1), :] = mine
        for dev in to:
            a_copy(b, stage, me, 1, dev).start()

    def sum_next(b):
        a_copy(b, 0, 0, 1, at_z()).wait()
        me = R0 + 4 * iy + it
        k.ra[b, pl.ds(me, 1), :] = k.ra[b, 0:1, :] + k.ra[b, 1:2, :]
        for dev in slab:
            a_copy(b, 1, me, 1, dev).start()

    def sum_end(b, n, to, first):
        a_copy(b, 1, first, len(to), at_z()).wait()
        tile = jnp.sum(k.ra[b, first:], axis=0, keepdims=True)
        return [jnp.broadcast_to(tile[:, v:v + 1], (8, LANES)) for v in range(n)]

    def dots(q):
        j = plane_of(jnp.where(q < 2, 0, jnp.where(q < 4, 2, 1)), lax.rem(q, 2))
        sums = [jnp.zeros((ROWS, LANES), F32)] * 5
        for c in COMPS:
            w, r, s = k.f[j, c, pl.ds(R0, ROWS), :], k.r[j, c], k.s[j, c]
            sums = [t + u * v for t, (u, v) in zip(sums, ((w, r), (w, w), (r, s), (w, s), (s, s)))]
        for v, t in enumerate(sums):
            k.gd[2 + v] = k.gd[2 + v] + fold(t)

    CW, AW, AX, BETA, GAMMA, ALPHA, FIRST = range(7)
    one = jnp.ones((8, LANES), F32)
    for v, t in ((CW, zero8), (AW, -one), (AX, zero8), (BETA, zero8), (GAMMA, one), (ALPHA, one)):
        k.cf[v] = t

    def scalars(step, gamma, delta):
        @pl.when(step == 1)
        def _():
            k.cf[ALPHA] = gamma / delta
            k.cf[FIRST] = gamma

        @pl.when(step > 1)
        def _():
            beta = gamma / k.cf[GAMMA]
            k.cf[BETA] = beta
            k.cf[ALPHA] = gamma / (delta - beta * gamma / k.cf[ALPHA])
            res[step - 2] = (gamma / k.cf[FIRST])[0, 0]
        k.cf[CW], k.cf[AW], k.cf[AX], k.cf[GAMMA] = one, k.cf[ALPHA], k.cf[ALPHA], gamma

    def phase(u):
        begin = (u < 5) | (u == 6) | (u == 7) | (u == 9)
        v = jnp.where(u > 9, u - 8, jnp.where(u > 6, 1, 0))
        n, ph = v // 3, lax.rem(v, 3)
        i = lax.rem(n, 2)
        even, odd, starts, ends = i == 0, i == 1, ph == 0, ph == 2
        step = n // 2
        b = lax.rem(step, 2)
        t = jnp.where(starts, 0, jnp.where((ph == 1) == even, 1, 2))
        live = jnp.logical_not(begin)
        more = n < 2 * ITERS - 1

        @pl.when(begin)
        def _():
            loop(pick(PHASE_WORDS, jnp.minimum(u, 10)), pick(PHASE_WORDS, jnp.minimum(u + 1, 10)), load_step)

        @pl.when(u == 0)
        def _():
            all_rows = k.sst.at[:ZL * SITE]
            pltpu.make_async_copy(all_rows, all_rows, k.io_sem.at[0]).wait()
            loop(0, ZL, src_plane)
            pl.semaphore_wait(barrier, len(everyone))

        @pl.when(live & even & (ph == 1) & (step > 0))
        def _():
            sum_next(b)

        @pl.when(live & odd & starts)
        def _():
            @pl.when(step > 0)
            def _():
                scalars(step, *sum_end(b, 2, slab, R0))
            k.gd[0], k.gd[1] = zero8, zero8

        last = ends & jnp.logical_not(more)

        @pl.when(last)
        def _():
            loop(0, 4, dots)

        @pl.when(live & jnp.logical_not(last))
        def _():
            receive(i, t)

        @pl.when(live)
        def _():
            @pl.when(even)
            def _():
                finish(0, t, store_odd)

            @pl.when(odd)
            def _():
                finish(1, t, update_even)

        @pl.when(last)
        def _():
            arrive(i, t)
            loop(0, 2, lambda e: correct(2 * e))

        @pl.when(live & ends & odd & more)
        def _():
            sum_start(1 - b, 2, 0, iz, [at_z()])

        o = jnp.where(begin, 0, 1 - i)

        loop(0, jnp.where(begin, jnp.where(u < 2, u + 1, 0), more.astype(jnp.int32)), lambda e: send(o, jnp.where(begin, jnp.where(u == 0, 1, 2 * e), t)))

        tells = jnp.where(begin, (u == 2) | (u == 4) | (u == 6), more).astype(jnp.int32)
        tells = jnp.where(live & (n == 0), jnp.where(starts, 1, 2 * ends.astype(jnp.int32)), tells)
        loop(0, tells, lambda e: tell(o, jnp.where(begin, u // 2 - 1, t - e)))

        @pl.when(jnp.where(begin, (u == 3) | (u == 7) | (u == 9), jnp.where(ends, more, n > 0)))
        def _():
            post(jnp.where(begin | ends, o, i), jnp.where(begin, u // 3 - 1, jnp.where(ends, 0, jnp.where(starts == even, 1, 2))))

        @pl.when(live & ends)
        def _():
            sent(i)

    loop(0, 8 + 3 * 2 * ITERS, phase)

    loop(4, ZL, dots)
    sum_start(0, 7, 1, 8 * iy + 4 * iz + it, everyone)
    parts = (k.sst, k.stg.at[0], k.stg.at[1])

    def out_plane(j):
        for to, frm in zip(parts, (k.x, k.r, k.p)):
            for c in COMPS:
                for s in range(2):
                    to[pl.ds(j * SITE + 6 * s + c, VALID, 12), :] = rot(frm[j, c], HALF * s)[0:VALID, 0:YL]

    loop(0, ZL, out_plane)
    rr, _, wr, ww, rs, ws, ss = sum_end(0, 7, everyone, 0)
    beta = rr / k.cf[GAMMA]
    alpha = rr / (wr - beta * rr / k.cf[ALPHA])
    last = rr - 2.0 * alpha * (wr + beta * rs) + alpha * alpha * (ww + 2.0 * beta * ws + beta * beta * ss)
    for v, t in ((ITERS - 2, rr), (ITERS - 1, last)):
        res[v] = (t / k.cf[FIRST])[0, 0]
    alpha, beta = (jnp.broadcast_to(v[0:1, 0:YL], (SITE, YL)) for v in (alpha, beta))

    def out_rows(j):
        here = pl.ds(j * SITE, SITE)
        x, r, p = (ref[here, :] for ref in parts)
        v = x + alpha * (r + beta * p)
        for t in range(TL):
            out[t, pl.ds(j * 60, 60), :] = v[60 * t:60 * (t + 1)]

    loop(0, ZL, out_rows)


def solution(mesh):
    link_spec = P(None, 't', 'zz', 'yy')
    field_spec = P('t', 'zz', 'yy')

    def local_solve(fat_links, long_links, source, quark_mass):
        fat, lng = (jnp.moveaxis(v, 3, -1).reshape(4, TL, ZL, XL, QUAD, YL) for v in (fat_links, long_links))
        src = jnp.moveaxis(source, 2, -1).reshape(TL, SITE, YL)
        anywhere, local, scalar = (pl.BlockSpec(memory_space=space) for space in (pl.ANY, pltpu.VMEM, pltpu.SMEM))
        sol, res = pl.pallas_call(
            kernel,
            out_shape=(pltpu.VMEM((TL, SITE, YL), F32), pltpu.SMEM((8,), F32)),
            in_specs=[anywhere] * 3 + [scalar],
            out_specs=(local, scalar),
            scratch_shapes=list(SCRATCH.values()),
            compiler_params=pltpu.CompilerParams(collective_id=0, has_side_effects=True, vmem_limit_bytes=65000000),
            name='cg',
        )(fat, lng, src, quark_mass)
        return jnp.moveaxis(sol.reshape(TL, ZL, XH, 3, 2, YL), -1, 2), res

    return jax.shard_map(local_solve, mesh=mesh, in_specs=(link_spec, link_spec, field_spec, P()), out_specs=(field_spec, P()), check_vma=False)
```

```python
import jax
import jax.numpy as jnp
from jax import lax
from jax.experimental import pallas as pl
from jax.experimental.pallas import tpu as pltpu
from jax.sharding import PartitionSpec as P

ITERS = 8
MESH = pl.DeviceIdType.MESH
F32 = jnp.float32
TL, ZL, YL, XH = 6, 6, 48, 10
R0 = 16
ROWS, LANES, HALF, VALID = 32, 128, 64, 30
XL = 5
NSTG = 6
COMPS, LINKS = range(6), range(18)
C0 = 3
STEPS = ((0, 1), (1, 3))
SITE = VALID * 2 * 6
ORDER = 'z3z4z5t1y1t4y4z0z1x1x4t0y0t2y2t3y3t5y5x0x2z2x3x5'
FIRST_STEP = 'aadhlpptwwyy'
LOADS = 4 * ZL
PITCH, QUAD = 76, 72
BLK = 16
BLOCKS = range(0, ROWS, BLK)


def packed(values):
    return [sum(v << 5 * q for q, v in enumerate(values[w:w + 6])) for w in range(0, len(values), 6)]


def pick(words, q):
    word = words[-1]
    for w, value in enumerate(words[:-1]):
        word = jnp.where(q // 6 == w, value, word)
    return (word >> 5 * lax.rem(q, 6)) & 31


STEP_WORDS = packed(['tzyx'.index(ORDER[q]) * 8 + int(ORDER[q + 1]) for q in range(0, 2 * LOADS, 2)])
PHASE_WORDS = packed([ord(q) - ord('a') for q in FIRST_STEP])


def loop(first, last, act):
    def body(q, carry):
        act(q)
        return carry
    lax.fori_loop(first, last, body, 0)


def vec(*shape):
    return pltpu.VMEM(shape + (LANES,), F32)


def plane():
    return vec(ZL, 6, ROWS)


def sems(*shape):
    return pltpu.SemaphoreType.DMA(shape)


def halo_t():
    return vec(2, ZL, 6, R0)


def wires():
    return vec(2, 6, 136)


def halo_y():
    return vec(2, ZL, BLK)


SCRATCH = dict(
    lkt=vec(24, 18, 56), lko=vec(72, 18, ROWS), stg=pltpu.VMEM((2 * NSTG, ROWS * PITCH, YL), F32), sst=pltpu.VMEM((2304, YL), F32),
    f=vec(18, 6, 64), acc=plane(), cb=vec(2, 6, ROWS), xs=vec(2, 6, YL),
    r=plane(), p=plane(), s=plane(), z=plane(), x=plane(), zs=wires(), zr=wires(),
    tsf=halo_t(), trf=halo_t(), tsc=halo_t(), trc=halo_t(), ysf=halo_y(), yrf=halo_y(), ysc=halo_y(), yrc=halo_y(),
    ra=vec(2, 32), gd=vec(7, 8), cf=vec(8, 8),
    stg_sem=sems(NSTG), io_sem=sems(1), z_ss=sems(2), z_rs=sems(2, 3), h_ss=sems(2, 2), h_rs=sems(2, 3, 2),
    a_ss=sems(2, 2), a_rs=sems(2, 2),
)


def terms(link, psi):
    for i in range(3):
        for j in range(3):
            at = 2 * (3 * i + j)
            yield i, j, link(at), link(at + 1), psi


def mat(acc, link, psi):
    for i, j, a, b, v in terms(link, psi):
        c, d = v[2 * j:2 * j + 2]
        acc[2 * i] = acc[2 * i] + (a * c - b * d)
        acc[2 * i + 1] = acc[2 * i + 1] + (a * d + b * c)


def adj(acc, link, psi):
    for j, i, a, b, v in terms(link, psi):
        c, d = v[2 * j:2 * j + 2]
        acc[2 * i] = acc[2 * i] - (a * c + b * d)
        acc[2 * i + 1] = acc[2 * i + 1] + (b * c - a * d)


def fold(v):
    return sum(v[first:first + 8] for first in range(0, len(v), 8))


def rot(v, n):
    n %= LANES
    return pltpu.roll(v, n, 1) if n else v


def kernel(fat, lng, src, mass, out, res, *scratch):
    k = type('Refs', (), {})()
    for name, ref in zip(SCRATCH, scratch):
        setattr(k, name, ref)
    iy, iz, it = lax.axis_index('yy'), lax.axis_index('zz'), lax.axis_index('t')

    def at_t(d):
        return (iy, iz, lax.rem(it + d, 4))

    def at_z():
        return (iy, 1 - iz, it)

    def at_y(d):
        return (lax.rem(iy + d, 4), iz, it)

    def remote(src_ref, dst_ref, send, recv, dev):
        return pltpu.make_async_remote_copy(src_ref=src_ref, dst_ref=dst_ref, send_sem=send, recv_sem=recv, device_id=dev, device_id_type=MESH)

    def other(d):
        return (iy + d // 8) & 3, (iz + d // 4) & 1, (it + d) & 3

    everyone = [other(d) for d in range(1, ROWS)]
    slab = [((iy + d // 4) & 3, iz, (it + d) & 3) for d in range(1, R0)]

    def plane_of(t, n2):
        first = jnp.where(t == 0, 1, jnp.where(t == 1, 0, 3))
        return first + n2 * jnp.where(t == 0, 3, 2)

    def what(g):
        code = pick(STEP_WORDS, g)
        return code // 8, code & 7

    def stg_copies(g):
        slot = lax.rem(g, NSTG)
        di, zi = what(g)

        def to(n):
            return k.stg.at[2 * slot + n, pl.ds(0, VALID * PITCH)].reshape(TL, XL, PITCH, YL).at[:, :, pl.ds(0, QUAD)]
        return [pltpu.make_async_copy(ref.at[di, :, zi], to(n), k.stg_sem.at[slot]) for n, ref in enumerate((fat, lng))]

    def src_copy(zi):
        return pltpu.make_async_copy(src.at[:, pl.ds(60 * zi, 60)], k.sst.at[pl.ds(SITE * zi, SITE)].reshape(TL, 60, YL), k.io_sem.at[0])

    for zi in range(ZL):
        src_copy(zi).start()
    for g in range(NSTG):
        for cp in stg_copies(jnp.int32(g)):
            cp.start()
    barrier = pltpu.get_barrier_semaphore()
    loop(1, ROWS, lambda d: pl.semaphore_signal(barrier, device_id=other(d), device_id_type=MESH))

    lane8, row8 = (lax.broadcasted_iota(jnp.int32, (8, LANES), d) for d in (1, 0))
    ylane8 = lane8 % HALF
    lane, row = (lax.broadcasted_iota(jnp.int32, (ROWS, LANES), d) for d in (1, 0))
    lane_b, row_b = lane[:BLK], row[:BLK]
    ylane = lane_b % HALF
    seg0 = lane_b < HALF
    zero8 = jnp.zeros((8, LANES), F32)
    zeros = jnp.zeros((BLK, LANES), F32)

    def lt(n, o, zi):
        return (n * 2 + o) * ZL + zi

    def lo(di, n, o, zi):
        return (((di - 1) * 2 + n) * 2 + o) * ZL + zi

    def at(h, off=0):
        return pl.ds(off + h, BLK)

    def psi_of(i, j, h, off=0):
        return [k.f[9 * i + j, c, at(h, R0 + off), :] for c in COMPS]

    k.f[...] = jnp.zeros_like(k.f)
    for ref in (k.p, k.s, k.z, k.x, k.gd):
        ref[...] = jnp.zeros_like(ref)
    k.lkt[:, :, 0:R0, :] = jnp.zeros((24, 18, R0, LANES), F32)
    k.lkt[:, :, R0 + ROWS:, :] = jnp.zeros((24, 18, 8, LANES), F32)

    k.stg[:, VALID * PITCH:, :] = jnp.zeros((2 * NSTG, 2 * PITCH, YL), F32)
    def whole(half):
        rest = jnp.zeros((ROWS, LANES - YL), F32)
        first, second = (jnp.concatenate([v, rest], axis=1) for v in half)
        return first + rot(second, HALF)

    def src_plane(zi):
        for c in COMPS:
            v = jnp.where(row < VALID, whole([k.sst[pl.ds(zi * SITE + 6 * s + c, ROWS, 12), :] for s in range(2)]), 0.0)
            k.f[zi, c, pl.ds(R0, ROWS), :] = v
            k.r[zi, c] = v

    def convert(g, zi, ref, base, lead):
        slot = lax.rem(g, NSTG)
        even = ((row // XL + lane + zi) & 1) == 0
        for n in range(2):
            for c in LINKS:
                v = [whole([k.stg[2 * slot + n, pl.ds(c + (2 * s + h) * 18, ROWS, PITCH), :] for s in range(2)]) for h in range(2)]
                for o in range(2):
                    ref[lead(n, o, zi), c, pl.ds(base, ROWS), :] = jnp.where(even, v[o], v[1 - o])

    def load_step(g):
        di, zi = what(g)
        slots = pl.ds(2 * lax.rem(g, NSTG), 2)
        used_rows = slice(TL * SITE)
        pltpu.make_async_copy(k.stg.at[slots, used_rows], k.stg.at[slots, used_rows], k.stg_sem.at[lax.rem(g, NSTG)]).wait()

        @pl.when(di == 0)
        def _():
            convert(g, zi, k.lkt, R0, lt)

        @pl.when(di > 0)
        def _():
            convert(g, zi, k.lko, 0, lambda n, o, zi: lo(di, n, o, zi))

        @pl.when(g + NSTG < LOADS)
        def _():
            for cp in stg_copies(g + NSTG):
                cp.start()

    def z_copy(i, m, t):
        return remote(k.zs.at[i, m, used], k.zr.at[i, m, used], k.z_ss.at[i], k.z_rs.at[i, t], at_z())

    def h_copies(i, t):
        pairs = ((k.tsf, k.trf, at_t(3)), (k.tsc, k.trc, at_t(1)), (k.ysf, k.yrf, at_y(3)), (k.ysc, k.yrc, at_y(1)))
        two = pl.ds(2 * t, 2)
        return [remote(a.at[i, two], b.at[i, two], k.h_ss.at[i, n // 2], k.h_rs.at[i, t, n // 2], dev) for n, (a, b, dev) in enumerate(pairs)]

    def h_waits(i, t, *some):
        return [remote(a.at[some], b.at[some], k.h_ss.at[i, n], k.h_rs.at[i, t, n], at_t(1)) for n, (a, b) in enumerate(((k.tsf, k.trf), (k.ysf, k.yrf)))]

    def sent(i):
        remote(k.zs.at[i, :, used], k.zr.at[i, :, used], k.z_ss.at[i], k.z_rs.at[i, 0], at_z()).wait_send()
        for cp in h_waits(i, 0, slice(None)):
            cp.wait_send()

    gap = ylane8 >= YL
    used = slice(135)

    def rows_of(u, part, off=0):
        return pl.ds(off + 15 * (u % 2) + part, 8)

    def wire(host, part):
        return pl.ds(15 * host + part, 8)

    def pack(load, i, m):
        for u in range(3):
            for part in (0, 7):
                guest = load(9 + u, part)
                for q in range(3):
                    k.zs[i, m, wire(3 * q + u, part), :] = jnp.where(gap, rot(guest, YL - R0 * q), load(3 * q + u, part))

    def unpack(i, m, store):
        for u in range(3):
            for part in (0, 7):
                guest = zero8
                for q in range(3):
                    h = k.zr[i, m, wire(3 * q + u, part), :]
                    store(3 * q + u, part, jnp.where(gap, 0.0, h))
                    guest = jnp.where(ylane8 // R0 == q, rot(h, R0 * q - YL), guest)
                store(9 + u, part, guest)

    def start(i, m, t):
        z_copy(i, m, t).start()

    def arrive(i, t):
        z_copy(i, slice(2), t).wait_recv()

    def pack_psi(i, m):
        pack(lambda u, part: k.f[9 * i + m, u // 2, rows_of(u, part, R0), :], i, m)

    def pack_c(i, m, b, *terms):
        acc = [jnp.zeros((ROWS, LANES), F32)] * 6
        for n, j in terms:
            adj(acc, lambda c: k.lko[lo(1, n, i, j), c], [k.f[9 * i + j, c, pl.ds(R0, ROWS), :] for c in COMPS])
        for c in COMPS:
            k.cb[b, c] = acc[c]
        pack(lambda u, part: k.cb[b, u // 2, rows_of(u, part), :], i, C0 + m)

    def fresh(v, part):
        return jnp.where(row8 == 0, 0.0, v) if part else v

    def unpack_psi(i, m):
        def store(u, part, v):
            k.f[9 * i + 6 + m, u // 2, rows_of(u, part, R0), :] = v
        unpack(i, m, store)

    def unpack_c(i, m):
        def store(u, part, v):
            sl = (m, u // 2, rows_of(u, part), slice(None))
            k.acc[sl] = k.acc[sl] + fresh(v, part)
        unpack(i, C0 + m, store)

    def correct(m):
        aw = k.cf[1]

        def store(u, part, v):
            sl = (m, u // 2, rows_of(u, part, R0), slice(None))
            k.f[sl] = k.f[sl] + aw * fresh(v, part)
        unpack(1, C0 + m, store)

    def send(i, t):
        @pl.when(t == 0)
        def _():
            pack_psi(i, 1)
            start(i, 1, 0)
            pack_c(i, 1, 0, (1, 4))
            start(i, C0 + 1, 0)

        @pl.when(t == 1)
        def _():
            for m in (0, 2):
                pack_psi(i, m)
                start(i, m, 2)

        @pl.when(t == 2)
        def _():
            pack_c(i, 2, 1, (1, 5))
            start(i, C0 + 2, 1)
            pack_c(i, 0, 0, (0, 5), (1, 3))
            start(i, C0, 1)

    def receive(i, t):
        @pl.when(t == 0)
        def _():
            arrive(i, t)
            unpack_psi(i, 1)
            unpack_c(i, 1)

        @pl.when(t == 1)
        def _():
            arrive(i, t)
            unpack_c(i, 0)
            unpack_c(i, 2)

        @pl.when(t == 2)
        def _():
            arrive(i, t)
            unpack_psi(i, 0)
            unpack_psi(i, 2)

    def tell(i, t):
        def one_plane(n2):
            j = plane_of(t, n2)
            slot = 2 * t + n2
            fwd, bwd = zeros, zeros
            psi = [k.f[9 * i + j, c, pl.ds(R0, ROWS), :] for c in COMPS]
            chis = []
            for n, _ in STEPS:
                chis.append([jnp.zeros((ROWS, LANES), F32)] * 6)
                adj(chis[n], lambda c: k.lko[lo(2, n, i, j), c], psi)
            for c in COMPS:
                k.acc[j, c] = sum(rot(chis[n][c], off) for n, off in STEPS)
                for h in BLOCKS:
                    to = 4 * c + 24 * (h // BLK)
                    here = ylane // 4 == to // 4
                    fwd = jnp.where(here, rot(psi[c][h:h + BLK], to), fwd)
                    bwd = jnp.where(here, sum(rot(chis[n][c][h:h + BLK], to - YL + off) for n, off in STEPS), bwd)
            k.ysf[i, slot] = fwd
            k.ysc[i, slot] = bwd
            for h in range(2):
                acc = [zero8] * 6
                for n, first in ((0, R0 + 25), (1, R0 + 15 + 8 * h)):
                    if n or not h:
                        adj(acc, lambda c: k.lkt[lt(n, i, j), c, pl.ds(first, 8), :], [k.f[9 * i + j, c, pl.ds(first, 8), :] for c in COMPS])
                for c in COMPS:
                    k.tsc[i, slot, c, pl.ds(8 * h, 8), :] = acc[c]
                    k.tsf[i, slot, c, pl.ds(8 * h, 8), :] = k.f[9 * i + j, c, pl.ds(R0 + 8 * h, 8), :]

        for n2 in range(2):
            one_plane(n2)
        for cp in h_copies(i, t):
            cp.start()

    def post(i, t):
        o = 1 - i

        def one_plane(n2):
            j = plane_of(t, n2)
            for h in BLOCKS:
                psi = psi_of(i, j, h)
                for n, _ in STEPS:
                    chi = [zeros] * 6
                    adj(chi, lambda c: k.lko[lo(3, n, i, j), c, at(h), :], psi)
                    for c in COMPS:
                        k.xs[n, c, at(h, 8), :] = chi[c]
            for h in BLOCKS:
                x5 = lax.rem(row_b + h, XL)
                e = (((row_b + h) // XL + lane_b + (j + o)) & 1) == 1
                acc = [k.acc[j, c, at(h), :] for c in COMPS]
                for n, _ in STEPS:
                    for c in COMPS:
                        own = k.xs[n, c, at(h, 8), :]
                        far = jnp.where(x5 > 0, k.xs[n, c, at(h, 7), :], k.xs[n, c, at(h, 12), :])
                        close = rot(jnp.where(seg0, own, far), HALF)
                        acc[c] = acc[c] + (jnp.where(e, close, far) if n else jnp.where(e, own, close))
                for n, off in STEPS:
                    off *= XL
                    adj(acc, lambda c: k.lkt[lt(n, i, j), c, at(h, R0 - off), :], psi_of(i, j, h, -off))
                psi = psi_of(i, j, h)
                far = [jnp.where(x5 < 4, u, v) for u, v in zip(psi_of(i, j, h, 1), psi_of(i, j, h, -4))]
                close = [rot(jnp.where(seg0, far[c], psi[c]), HALF) for c in COMPS]
                mat(acc, lambda c: k.lko[lo(3, 0, o, j), c, at(h), :], [jnp.where(e, close[c], psi[c]) for c in COMPS])
                mat(acc, lambda c: k.lko[lo(3, 1, o, j), c, at(h), :], [jnp.where(e, far[c], close[c]) for c in COMPS])
                for c in COMPS:
                    k.acc[j, c, at(h), :] = acc[c]

        loop(0, 2, one_plane)

    m2 = mass[0] * mass[0]

    def store_odd(j, h, real, acc):
        for c in COMPS:
            k.f[9 + j, c, at(h, R0), :] = acc[c]

    def update_even(j, h, real, acc):
        cw, aw, ax, beta = (jnp.broadcast_to(k.cf[v, 0:1], (BLK, LANES)) for v in range(4))
        gg, dd = zeros, zeros
        for c in COMPS:
            sl, fl = (j, c, at(h), slice(None)), (j, c, at(h, R0), slice(None))
            w = jnp.where(real, k.f[fl], 0.0)
            n = m2 * w - acc[c]
            zv = n + beta * k.z[sl]
            sv = w + beta * k.s[sl]
            r = k.r[sl]
            pv = r + beta * k.p[sl]
            k.x[sl] = k.x[sl] + ax * pv
            r = r - ax * sv
            w = cw * w - aw * zv
            k.z[sl], k.s[sl], k.p[sl], k.r[sl], k.f[fl] = zv, sv, pv, r, w
            gg = gg + r * r
            dd = dd + w * r
        for v, t in enumerate((gg, dd)):
            k.gd[v] = k.gd[v] + fold(t)

    def finish(i, t, update):
        o = 1 - i
        for cp in h_waits(i, t, i, slice(4)):
            cp.wait_recv()

        def one_plane(n2):
            j = plane_of(t, n2)
            slot = 2 * t + n2
            for c in COMPS:
                k.f[9 * i + j, c, pl.ds(R0 + VALID, R0), :] = k.trf[i, slot, c]
            yf, yc = k.yrf[i, slot], k.yrc[i, slot]
            for h in BLOCKS:
                frm = [4 * c + 24 * (h // BLK) for c in COMPS]
                top = (ylane >= YL) & (ylane < YL + 3)
                psi = [jnp.where(top, rot(yf, YL - frm[c]), v) for c, v in enumerate(psi_of(i, j, h))]
                acc = [k.acc[j, c, at(h), :] + jnp.where(ylane < 3, rot(yc, -frm[c]), 0.0) for c in COMPS]
                if h == 0:
                    acc = [acc[c] + k.trc[i, slot, c] for c in COMPS]
                for n, off in STEPS:
                    mat(acc, lambda c: k.lkt[lt(n, o, j), c, at(h, R0), :], psi_of(i, j, h, XL * off))
                for n, off in STEPS:
                    mat(acc, lambda c: k.lko[lo(1, n, o, j), c, at(h), :], psi_of(i, j + off, h))
                    jb, on = jnp.maximum(j - off, 0), jnp.where(j >= off, 1.0, 0.0)
                    adj(acc, lambda c: k.lko[lo(1, n, i, jb), c, at(h), :], [on * v for v in psi_of(i, jb, h)])
                for n, off in STEPS:
                    mat(acc, lambda c: k.lko[lo(2, n, o, j), c, at(h), :], [rot(psi[c], -off) for c in COMPS])
                real = row_b + h < VALID
                good = real & (ylane < YL)
                update(j, h, real, [jnp.where(good, acc[c], 0.0) for c in COMPS])

        loop(0, 2, one_plane)

    def a_copy(b, stage, first, rows, dev):
        here = k.ra.at[b, pl.ds(first, rows)]
        return remote(here, here, k.a_ss.at[b, stage], k.a_rs.at[b, stage], dev)

    def sum_start(b, n, stage, me, to):
        mine = zeros[:1]
        for v in range(n):
            total = jnp.sum(jnp.sum(k.gd[v], axis=0, keepdims=True), axis=1, keepdims=True)
            mine = jnp.where(lane[:1] == v, total, mine)
        k.ra[b, pl.ds(me, 1), :] = mine
        for dev in to:
            a_copy(b, stage, me, 1, dev).start()

    def sum_next(b):
        a_copy(b, 0, 0, 1, at_z()).wait()
        me = R0 + 4 * iy + it
        k.ra[b, pl.ds(me, 1), :] = k.ra[b, 0:1, :] + k.ra[b, 1:2, :]
        for dev in slab:
            a_copy(b, 1, me, 1, dev).start()

    def sum_end(b, n, to, first):
        a_copy(b, 1, first, len(to), at_z()).wait()
        tile = jnp.sum(k.ra[b, first:], axis=0, keepdims=True)
        return [jnp.broadcast_to(tile[:, v:v + 1], (8, LANES)) for v in range(n)]

    def dots(q):
        j = plane_of(jnp.where(q < 2, 0, jnp.where(q < 4, 2, 1)), lax.rem(q, 2))
        sums = [jnp.zeros((ROWS, LANES), F32)] * 5
        for c in COMPS:
            w, r, s = k.f[j, c, pl.ds(R0, ROWS), :], k.r[j, c], k.s[j, c]
            sums = [t + u * v for t, (u, v) in zip(sums, ((w, r), (w, w), (r, s), (w, s), (s, s)))]
        for v, t in enumerate(sums):
            k.gd[2 + v] = k.gd[2 + v] + fold(t)

    CW, AW, AX, BETA, GAMMA, ALPHA, FIRST = range(7)
    one = jnp.ones((8, LANES), F32)
    for v, t in ((CW, zero8), (AW, -one), (AX, zero8), (BETA, zero8), (GAMMA, one), (ALPHA, one)):
        k.cf[v] = t

    def scalars(step, gamma, delta):
        @pl.when(step == 1)
        def _():
            k.cf[ALPHA] = gamma / delta
            k.cf[FIRST] = gamma

        @pl.when(step > 1)
        def _():
            beta = gamma / k.cf[GAMMA]
            k.cf[BETA] = beta
            k.cf[ALPHA] = gamma / (delta - beta * gamma / k.cf[ALPHA])
            res[step - 2] = (gamma / k.cf[FIRST])[0, 0]
        k.cf[CW], k.cf[AW], k.cf[AX], k.cf[GAMMA] = one, k.cf[ALPHA], k.cf[ALPHA], gamma

    def phase(u):
        begin = (u < 5) | (u == 6) | (u == 7) | (u == 9)
        v = jnp.where(u > 9, u - 8, jnp.where(u > 6, 1, 0))
        n, ph = v // 3, lax.rem(v, 3)
        i = lax.rem(n, 2)
        even, odd, starts, ends = i == 0, i == 1, ph == 0, ph == 2
        step = n // 2
        b = lax.rem(step, 2)
        t = jnp.where(starts, 0, jnp.where((ph == 1) == even, 1, 2))
        live = jnp.logical_not(begin)
        more = n < 2 * ITERS - 1

        @pl.when(begin)
        def _():
            loop(pick(PHASE_WORDS, jnp.minimum(u, 10)), pick(PHASE_WORDS, jnp.minimum(u + 1, 10)), load_step)

        @pl.when(u == 0)
        def _():
            all_rows = k.sst.at[:ZL * SITE]
            pltpu.make_async_copy(all_rows, all_rows, k.io_sem.at[0]).wait()
            loop(0, ZL, src_plane)
            pl.semaphore_wait(barrier, len(everyone))

        @pl.when(live & even & (ph == 1) & (step > 0))
        def _():
            sum_next(b)

        @pl.when(live & odd & starts)
        def _():
            @pl.when(step > 0)
            def _():
                scalars(step, *sum_end(b, 2, slab, R0))
            k.gd[0], k.gd[1] = zero8, zero8

        last = ends & jnp.logical_not(more)

        @pl.when(last)
        def _():
            loop(0, 4, dots)

        @pl.when(live & jnp.logical_not(last))
        def _():
            receive(i, t)

        @pl.when(live)
        def _():
            @pl.when(even)
            def _():
                finish(0, t, store_odd)

            @pl.when(odd)
            def _():
                finish(1, t, update_even)

        @pl.when(last)
        def _():
            arrive(i, t)
            loop(0, 2, lambda e: correct(2 * e))

        @pl.when(live & ends & odd & more)
        def _():
            sum_start(1 - b, 2, 0, iz, [at_z()])

        o = jnp.where(begin, 0, 1 - i)

        loop(0, jnp.where(begin, jnp.where(u < 2, u + 1, 0), more.astype(jnp.int32)), lambda e: send(o, jnp.where(begin, jnp.where(u == 0, 1, 2 * e), t)))

        tells = jnp.where(begin, (u == 2) | (u == 4) | (u == 6), more).astype(jnp.int32)
        tells = jnp.where(live & (n == 0), jnp.where(starts, 1, 2 * ends.astype(jnp.int32)), tells)
        loop(0, tells, lambda e: tell(o, jnp.where(begin, u // 2 - 1, t - e)))

        @pl.when(jnp.where(begin, (u == 3) | (u == 7) | (u == 9), jnp.where(ends, more, n > 0)))
        def _():
            post(jnp.where(begin | ends, o, i), jnp.where(begin, u // 3 - 1, jnp.where(ends, 0, jnp.where(starts == even, 1, 2))))

        @pl.when(live & ends)
        def _():
            sent(i)

    loop(0, 8 + 3 * 2 * ITERS, phase)

    loop(4, ZL, dots)
    sum_start(0, 7, 1, 8 * iy + 4 * iz + it, everyone)
    parts = (k.sst, k.stg.at[0], k.stg.at[1])

    def out_plane(j):
        for to, frm in zip(parts, (k.x, k.r, k.p)):
            for c in COMPS:
                for s in range(2):
                    to[pl.ds(j * SITE + 6 * s + c, VALID, 12), :] = rot(frm[j, c], HALF * s)[0:VALID, 0:YL]

    loop(0, ZL, out_plane)
    rr, _, wr, ww, rs, ws, ss = sum_end(0, 7, everyone, 0)
    beta = rr / k.cf[GAMMA]
    alpha = rr / (wr - beta * rr / k.cf[ALPHA])
    last = rr - 2.0 * alpha * (wr + beta * rs) + alpha * alpha * (ww + 2.0 * beta * ws + beta * beta * ss)
    for v, t in ((ITERS - 2, rr), (ITERS - 1, last)):
        res[v] = (t / k.cf[FIRST])[0, 0]
    alpha, beta = (jnp.broadcast_to(v[0:1, 0:YL], (SITE, YL)) for v in (alpha, beta))

    def out_rows(j):
        here = pl.ds(j * SITE, SITE)
        x, r, p = (ref[here, :] for ref in parts)
        v = x + alpha * (r + beta * p)
        for t in range(TL):
            out[t, pl.ds(j * 60, 60), :] = v[60 * t:60 * (t + 1)]

    loop(0, ZL, out_rows)


def solution(mesh):
    link_spec = P(None, 't', 'zz', 'yy')
    field_spec = P('t', 'zz', 'yy')

    def local_solve(fat_links, long_links, source, quark_mass):
        fat, lng = (jnp.moveaxis(v, 3, -1).reshape(4, TL, ZL, XL, QUAD, YL) for v in (fat_links, long_links))
        src = jnp.moveaxis(source, 2, -1).reshape(TL, SITE, YL)
        anywhere, local, scalar = (pl.BlockSpec(memory_space=space) for space in (pl.ANY, pltpu.VMEM, pltpu.SMEM))
        sol, res = pl.pallas_call(
            kernel,
            out_shape=(pltpu.VMEM((TL, SITE, YL), F32), pltpu.SMEM((8,), F32)),
            in_specs=[anywhere] * 3 + [scalar],
            out_specs=(local, scalar),
            scratch_shapes=list(SCRATCH.values()),
            compiler_params=pltpu.CompilerParams(collective_id=0, has_side_effects=True, vmem_limit_bytes=65000000),
            name='cg',
        )(fat, lng, src, quark_mass)
        return jnp.moveaxis(sol.reshape(TL, ZL, XH, 3, 2, YL), -1, 2), res

    return jax.shard_map(local_solve, mesh=mesh, in_specs=(link_spec, link_spec, field_spec, P()), out_specs=(field_spec, P()), check_vma=False)
```
